32 devices in a mesh: tm: 4 (over z), space: 8 (over y, x, core).
Axes of the slice: x: 2, y: 2, z: 4, core: 2. Of those that a mesh axis runs over, the one named last changes fastest.
Arguments:
- eigvecs: bfloat16 [4, 128, 2, 3, 32, 512], P('tm', None, None, None, 'space'), may hold values from -0.29882812 to 0.29882812
- gauge_links: float32 [4, 3, 2, 3, 3, 32, 512], P('tm', None, None, None, None, 'space'), may hold values from -1 to 1, as said below
- perambulator: bfloat16 [8, 4, 2, 128, 128], P('tm'), may hold values from -0.375 to 0.375
- job_owner: int32 [96, 1], replicated, may hold values from 0 to 3; in each aligned block of 24 rows (0 to 23, 24 to 47, ...) at most 18 rows name the same one
- job_elemental: int32 [96], replicated, may hold values from 0 to 3
- job_source: int32 [96], replicated, may hold values from 0 to 1
- job_spin: int32 [96], replicated, may hold values from 0 to 3
Outputs:
- dressed: bfloat16 [4, 4, 18, 2, 128, 128], P('tm', None, None, None, 'space')
The draws below stay inside these ranges and needn't reach their ends.
Inputs may be any that keep to these rules, and one draw needn't show every extreme that they name: `gauge_links`: each site's and direction's 3x3 complex matrix is special unitary. `job_owner`: jobs come in aligned blocks of 24 rows, block s holding the jobs of timeslice group s (timeslice s); within one block no owner is named by more than 18 rows, a bound that some block reaches. `job_elemental`: the job's timeslice within its group times 4 plus its operator (0 the momentum-projected plain elemental, 1 to 3 the derivatives along x1, x2, x3). `job_source`: the job's source time among its owner's 2 source times.
All inputs are finite; a program needn't handle non-finite values.
Results may differ from the reference program's by a relative error of at most 0.0057.
Values may be sent and summed in bfloat16 or wider, within the bound.
No kernel may reach another device: no remote copies, remote signals or barrier semaphores. Data moves between devices by JAX's collectives and lax.ppermute only.
A program may use at most 128 MiB of HBM per device.

```python
import math
import jax
import jax.numpy as jnp
import numpy as np
from jax import lax

NEV = 128
LX = 32
LY = 16
LZ = 32
OPS = 4
SPIN = 4
TS_DEV = 1
SRC_DEV = 2
JOB_DEV = 24
SITES = 512
SLICES = 4
SOURCES = 8
OWNERS = 4
JOBS = 96
CAP = 18


def complex_product(left_re, left_im, right_re, right_im):
    return (left_re * right_re - left_im * right_im, left_re * right_im + left_im * right_re)


def draw_gauge_links(key, part):
    gaussian = jax.random.normal(key, (2, 3, 3, SLICES, 3, LX, LY * LZ), jnp.float32)
    first_re = gaussian[0, 0]
    first_im = gaussian[1, 0]
    inverse_norm = lax.rsqrt(jnp.sum(first_re * first_re + first_im * first_im, axis=0))
    first_re = first_re * inverse_norm
    first_im = first_im * inverse_norm
    second_re = gaussian[0, 1]
    second_im = gaussian[1, 1]
    proj_re = jnp.sum(first_re * second_re + first_im * second_im, axis=0)
    proj_im = jnp.sum(first_re * second_im - first_im * second_re, axis=0)
    second_re = second_re - (proj_re * first_re - proj_im * first_im)
    second_im = second_im - (proj_re * first_im + proj_im * first_re)
    inverse_norm = lax.rsqrt(jnp.sum(second_re * second_re + second_im * second_im, axis=0))
    second_re = second_re * inverse_norm
    second_im = second_im * inverse_norm
    third_re = []
    third_im = []
    for colour in range(3):
        next_one = (colour + 1) % 3
        next_two = (colour + 2) % 3
        upper_re, upper_im = complex_product(first_re[next_one], first_im[next_one], second_re[next_two], second_im[next_two])
        lower_re, lower_im = complex_product(first_re[next_two], first_im[next_two], second_re[next_one], second_im[next_one])
        third_re.append(upper_re - lower_re)
        third_im.append(lower_im - upper_im)
    matrix_re = jnp.stack([first_re, second_re, jnp.stack(third_re, axis=0)], axis=0)
    matrix_im = jnp.stack([first_im, second_im, jnp.stack(third_im, axis=0)], axis=0)
    joined = jnp.stack([matrix_re, matrix_im], axis=0)
    return jnp.transpose(joined, (3, 4, 0, 1, 2, 5, 6)).astype(jnp.float32)


def touch_ends(drawn, key, smallest, top_value):
    dims = drawn.shape
    index_at = [jax.random.randint(jax.random.fold_in(key, axis), (), 0, dims[axis]) for axis in range(len(dims))]
    drawn = drawn.at[tuple(index_at)].set(smallest)
    longest = dims.index(max(dims))
    index_at[longest] = (index_at[longest] + 1) % dims[longest]
    return drawn.at[tuple(index_at)].set(top_value)


def block_levels(key, extent, pieces, least, top_value):
    def one(dim, parts):
        steps = jax.random.uniform(jax.random.fold_in(jax.random.fold_in(key, 6), dim), (parts,), jnp.float32, least / len(pieces), top_value / len(pieces))
        return jnp.repeat(jnp.exp(steps), extent[dim] // parts).reshape((-1,) + (1,) * (len(extent) - dim - 1))

    level = one(*pieces[0])
    for cut in pieces[1:]:
        level = level * one(*cut)
    return level


def deal_out(rng, own, number, rows, amount, top, most, lean):
    ranking = jax.random.permutation(rng, amount)
    crowded, usual = load_shares(amount, rows * top, most, lean, True), load_shares(amount, rows * top, most, lean, False)
    places = jnp.arange(amount)

    def named(sizes, turn):
        used = int((sizes > 0).sum())
        fixed = max(1, used // 4)
        shifted = fixed + (places - fixed + turn * (used - fixed)) % max(1, amount - fixed)
        return jnp.zeros((amount,), jnp.int32).at[ranking[jnp.where(places < fixed, places, shifted)]].set(jnp.asarray(sizes, jnp.int32))

    sizes = jnp.where(number % 4 == 0, named(crowded, number // 4), named(usual, number - number // 4 - 1))
    mixed = jax.random.permutation(jax.random.fold_in(own, 3), amount)
    donor, receiver = mixed[0:amount // 2 * 2:2], mixed[1:amount // 2 * 2:2]
    room = jnp.minimum(sizes[donor] - 1, most - sizes[receiver]) // 2
    room = jnp.where((donor == ranking[0]) | (receiver == ranking[0]) | (sizes[receiver] == 0), 0, jnp.maximum(room, 0))
    shifted = jax.random.randint(jax.random.fold_in(own, 4), (amount // 2,), 0, 1 << 20) % (room + 1)
    sizes = sizes.at[donor].add(-shifted).at[receiver].add(shifted)
    labels = jnp.searchsorted(jnp.cumsum(sizes), jnp.arange(rows * top), side="right").astype(jnp.int32)
    listing = labels.reshape(top, rows).T
    listing = listing[jax.random.permutation(jax.random.fold_in(own, 1), rows)]
    turn = jax.random.randint(jax.random.fold_in(own, 2), (rows, 1), 0, top)
    return jnp.take_along_axis(listing, (jnp.arange(top)[None, :] + turn) % top, axis=1)


def load_shares(amount, total, reach, skew, full):
    weights = [(1 << 20) // math.isqrt(rank ** skew) + 1 for rank in range(1, amount + 1)]
    largest = reach if full else min(reach, max(-(-total // amount), total * weights[0] // sum(weights)))
    least = 1 if total - largest >= amount - 1 else 0
    holding, rest = [largest] + [least] * (amount - 1), total - largest - least * (amount - 1)
    while rest > 0:
        free = [i for i in range(1, amount) if holding[i] < largest] or [i for i in range(1, amount) if holding[i] < reach]
        mass, budget = sum([weights[i] for i in free]), rest
        for i in free:
            extra = min(reach - holding[i], max(1, budget * weights[i] // mass), rest)
            holding[i] = holding[i] + extra
            rest = rest - extra
    return np.array(holding)


def centred(own_key, shape, scale, reach, pieces=(), kind=jnp.bfloat16):
    drawn = scale * jax.random.normal(own_key, shape, jnp.float32)
    if pieces:
        drawn = drawn * block_levels(own_key, shape, pieces, -0.22, 0.18)
    return jnp.clip(drawn, -reach, reach).astype(kind)


def setup_inputs(seed: int = 0) -> dict:
    keys = jax.random.split(jax.random.key(seed), 8)
    eigvecs = centred(keys[0], (SLICES, NEV, 2, 3, LX, SITES), 0.05, 0.29882812, ((0, 4), (4, 8)))
    gauge_links = draw_gauge_links(jax.random.fold_in(keys[7], 71), 0)
    perambulator = centred(keys[2], (SOURCES, SPIN, 2, NEV, NEV), (2 * NEV) ** -0.5, 0.375, ((0, 4),))
    job_owner_keys = jax.random.split(jax.random.fold_in(keys[3], 1), JOBS // JOB_DEV)
    job_owner_turns = jax.random.permutation(jax.random.fold_in(keys[3], 3), JOBS // JOB_DEV)
    job_owner = jax.vmap(lambda own, number: deal_out(jax.random.fold_in(keys[3], 2), own, number, JOB_DEV, OWNERS, 1, CAP, 2))(job_owner_keys, job_owner_turns).reshape((JOBS, 1))
    job_elemental = touch_ends(jax.random.randint(keys[4], (JOBS,), 0, TS_DEV * OPS), jax.random.fold_in(keys[4], 1), 0, (TS_DEV * OPS) - 1).astype(jnp.int32)
    job_source = touch_ends(jax.random.randint(keys[5], (JOBS,), 0, SRC_DEV), jax.random.fold_in(keys[5], 1), 0, SRC_DEV - 1).astype(jnp.int32)
    job_spin = touch_ends(jax.random.randint(keys[6], (JOBS,), 0, SPIN), jax.random.fold_in(keys[6], 1), 0, SPIN - 1).astype(jnp.int32)
    return {"eigvecs": eigvecs, "gauge_links": gauge_links, "perambulator": perambulator, "job_owner": job_owner, "job_elemental": job_elemental, "job_source": job_source, "job_spin": job_spin}


def shifted_sites(lattice_field, direction, offset):
    if direction == 1:
        return jnp.roll(lattice_field, -offset, axis=-2)
    shaped = lattice_field.reshape(lattice_field.shape[:-1] + (LY, LZ))
    rolled = jnp.roll(shaped, -offset, axis=direction - 4)
    return rolled.reshape(lattice_field.shape)


def apply_link(link_field, vectors):
    total_re = None
    total_im = None
    for colour in range(3):
        link_re = link_field[0, :, colour][None]
        link_im = link_field[1, :, colour][None]
        vector_re = vectors[:, 0, colour][:, None]
        vector_im = vectors[:, 1, colour][:, None]
        part_re = link_re * vector_re - link_im * vector_im
        part_im = link_re * vector_im + link_im * vector_re
        if colour == 0:
            total_re, total_im = part_re, part_im
        else:
            total_re = total_re + part_re
            total_im = total_im + part_im
    return jnp.stack([total_re, total_im], axis=1)


def stacked_form(vectors):
    vector_count = vectors.shape[0]
    swapped = jnp.concatenate([-vectors[:, 1:2], vectors[:, 0:1]], axis=1)
    return jnp.concatenate([vectors.reshape(vector_count, -1), swapped.reshape(vector_count, -1)], axis=0)


def paired_gram(stacked, lattice_field):
    vector_count = lattice_field.shape[0]
    flat_field = lattice_field.astype(jnp.bfloat16).reshape(vector_count, -1)
    product = lax.dot_general(stacked, flat_field, (((1,), (1,)), ((), ())), preferred_element_type=jnp.float32)
    return product.reshape(2, vector_count, vector_count)


def antihermitian(paired):
    return 0.5 * jnp.stack([paired[0] - paired[0].T, paired[1] + paired[1].T], axis=0)


def twisted_field(vectors, xcoord):
    phase_angle = (2.0 * math.pi / LX) * xcoord
    cosine = jnp.cos(phase_angle)[:, None]
    sine_part = jnp.sin(phase_angle)[:, None]
    real_part = cosine * vectors[:, 0] + sine_part * vectors[:, 1]
    imag_part = cosine * vectors[:, 1] - sine_part * vectors[:, 0]
    return jnp.stack([real_part, imag_part], axis=1)


def slice_elementals(inputs):
    low_vectors = inputs[0]
    vectors = low_vectors.astype(jnp.float32)
    link_all = inputs[1]
    xcoord = jnp.arange(LX, dtype=jnp.int32).astype(jnp.float32)
    stacked = stacked_form(low_vectors)
    results = [paired_gram(stacked, twisted_field(vectors, xcoord))]
    for direction in (1, 2, 3):
        forward = apply_link(link_all[direction - 1], shifted_sites(vectors, direction, 1))
        results.append(antihermitian(paired_gram(stacked, forward)))
    return jnp.stack(results, axis=0)


def reference(eigvecs, gauge_links, perambulator, job_owner, job_elemental, job_source, job_spin):
    elemental = lax.map(slice_elementals, (eigvecs, gauge_links)).astype(jnp.bfloat16)
    owners = job_owner[:, 0]
    grouped = owners.reshape(OWNERS, JOB_DEV)
    position = jnp.arange(JOB_DEV, dtype=jnp.int32)
    earlier = position[None, :] < position[:, None]
    same_owner = grouped[:, :, None] == grouped[:, None, :]
    slot_rank = jnp.sum(jnp.where(same_owner & earlier[None], 1, 0), axis=2).astype(jnp.int32).reshape(-1)
    group_index = jnp.arange(JOBS, dtype=jnp.int32) // JOB_DEV
    timeslice = group_index * TS_DEV + job_elemental // OPS
    operator_index = job_elemental % OPS
    left_side = elemental[timeslice, operator_index].astype(jnp.float32)
    right_side = perambulator[owners * SRC_DEV + job_source, job_spin].astype(jnp.float32)
    real_part = jnp.einsum("jab,jbc->jac", left_side[:, 0], right_side[:, 0]) - jnp.einsum("jab,jbc->jac", left_side[:, 1], right_side[:, 1])
    imag_part = jnp.einsum("jab,jbc->jac", left_side[:, 0], right_side[:, 1]) + jnp.einsum("jab,jbc->jac", left_side[:, 1], right_side[:, 0])
    result = jnp.stack([real_part, imag_part], axis=1).astype(jnp.bfloat16)
    dressed = jnp.zeros((OWNERS, OWNERS, CAP, 2, NEV, NEV), jnp.bfloat16)
    return dressed.at[owners, group_index, slot_rank].set(result)
```

```python
import math
from functools import partial

import numpy as np
import jax
import jax.numpy as jnp
from jax import lax
from jax.experimental import pallas as pl
from jax.experimental.pallas import tpu as pltpu
from jax.sharding import PartitionSpec as P

LY = 16
LZ = 32
OPS = 4
SPIN = 4
JOB_DEV = 24
LANES = 128
GROUP = 16
F32 = jnp.float32
BF16 = jnp.bfloat16
VMEM = pltpu.VMEM
SMEM = pltpu.SMEM


def vspec():
    return pl.BlockSpec(memory_space=VMEM)


def sspec():
    return pl.BlockSpec(memory_space=SMEM)


def cost(flops, moved):
    return pl.CostEstimate(flops=flops, bytes_accessed=moved, transcendentals=0)


def pick_matrix(rows, cols, source_of):
    row = lax.broadcasted_iota(jnp.int32, (rows, cols), 0)
    col = lax.broadcasted_iota(jnp.int32, (rows, cols), 1)
    return jnp.where(col == source_of(row), 1.0, 0.0).astype(BF16)


def nt_dot(left, right):
    return lax.dot_general(left, right, (((1,), (1,)), ((), ())), preferred_element_type=F32)


def rim_kernel(tiles, planes, x_ref, out_ref):
    spots = tiles * planes

    def source(row):
        return (row % GROUP) * spots + (row // GROUP) * planes

    chosen = pick_matrix(tiles * GROUP, GROUP * spots, source)
    block = x_ref[...].reshape(GROUP, 6, spots, LANES)
    for part in range(6):
        rows = block[:, part].reshape(GROUP * spots, LANES)
        taken = jnp.dot(chosen, rows, preferred_element_type=F32).astype(BF16)
        for tile in range(tiles):
            out_ref[part * tiles + tile] = taken[tile * GROUP : (tile + 1) * GROUP]


def rim_plane(x, count, tiles, planes):
    spots = tiles * planes
    return pl.pallas_call(
        partial(rim_kernel, tiles, planes),
        grid=(count // GROUP,),
        in_specs=[pl.BlockSpec((GROUP * 6 * spots, LANES), lambda g: (g, 0))],
        out_specs=pl.BlockSpec((6 * tiles, GROUP, LANES), lambda g: (0, g, 0)),
        out_shape=jax.ShapeDtypeStruct((6 * tiles, count, LANES), BF16),
        cost_estimate=cost(10**8, 4 * 10**6),
        name="rim",
    )(x)


def link_product(links, vec):
    outs_re, outs_im = [], []
    for row in range(3):
        total_re = None
        for col in range(3):
            link_re, link_im = links[0][row][col], links[1][row][col]
            part_re = link_re * vec[0][col] - link_im * vec[1][col]
            part_im = link_re * vec[1][col] + link_im * vec[0][col]
            if total_re is None:
                total_re, total_im = part_re, part_im
            else:
                total_re, total_im = total_re + part_re, total_im + part_im
        outs_re.append(total_re)
        outs_im.append(total_im)
    return outs_re, outs_im


def load_links(u_ref, direction, spot, spots):
    def one(part, row, col):
        at = (((direction * 2 + part) * 3 + row) * 3 + col) * spots + spot
        return jnp.broadcast_to(u_ref[pl.ds(at, 1), :], (8, LANES))

    return [[[one(part, row, col) for col in range(3)] for row in range(3)] for part in range(2)]


def paired(grid, count):
    real = grid[:count, :count] + grid[count:, count:]
    imag = grid[:count, count:] - grid[count:, :count]
    return real, imag


def anti(real, imag):
    return 0.5 * (real - real.T), 0.5 * (imag + imag.T)


def gram_kernel(
    count, tiles, planes, lx, x_ref, u_ref, phase_ref, sums_ref, rim_lhs_ref, v_ref, lhs_ref, op_ref, acc_ref, g_ref
):
    spots = tiles * planes
    groups = count // GROUP
    blocks = count // 8
    pair = 2
    steps = planes * (tiles // pair)

    def source(row):
        spot = row // GROUP
        return (row % GROUP) * spots + (spot % tiles) * planes + spot // tiles

    chosen = pick_matrix(GROUP * spots, GROUP * spots, source)

    def regroup(group, carry):
        start = pl.multiple_of(group * GROUP * 6 * spots, GROUP * 6 * spots)
        block = x_ref[pl.ds(start, GROUP * 6 * spots), :].reshape(GROUP, 6, spots, LANES)
        at = pl.multiple_of(group * GROUP, GROUP)
        for part in range(6):
            rows = block[:, part].reshape(GROUP * spots, LANES)
            taken = jnp.dot(chosen, rows, preferred_element_type=F32)
            half, colour = part // 3, part % 3
            for spot in range(spots):
                piece = taken[spot * GROUP : (spot + 1) * GROUP]
                v_ref[spot * 6 + part, pl.ds(at, GROUP), :] = piece
                plane, tile = spot // tiles, spot % tiles
                lhs_ref[
                    plane * (tiles // pair) + tile // pair,
                    pl.ds(half * count + at, GROUP),
                    ((tile % pair) * 3 + colour) * LANES : ((tile % pair) * 3 + colour + 1) * LANES,
                ] = piece.astype(BF16)
        return carry

    lax.fori_loop(0, groups, regroup, 0)
    for k in range(tiles * 6):
        v_ref[spots * 6 + k] = jnp.zeros((count, LANES), F32)
    acc_ref[...] = jnp.zeros_like(acc_ref)
    g_ref[...] = jnp.zeros_like(g_ref)

    lane = lax.broadcasted_iota(jnp.int32, (8, LANES), 1)
    wraps = (lane % LZ) == LZ - 1
    spills = lane < LZ

    def elementwise(step, slot):
        plane = step // (tiles // pair)
        half_tile = step % (tiles // pair)
        for sub in range(pair):
            tile = half_tile * pair + sub
            spot = plane * tiles + tile
            next_tile = plane * tiles + lax.rem(tile + 1, tiles)
            for direction in range(3):
                links = load_links(u_ref, direction, tile * planes + plane, spots)
                for block in range(blocks):
                    at = block * 8
                    if direction == 0:
                        base = (spot + tiles) * 6
                        parts = [v_ref[base + k, at : at + 8, :] for k in range(6)]
                    elif direction == 1:
                        parts = []
                        for k in range(6):
                            here = v_ref[spot * 6 + k, at : at + 8, :]
                            there = v_ref[next_tile * 6 + k, at : at + 8, :]
                            parts.append(pltpu.roll(jnp.where(spills, there, here), LANES - LZ, 1))
                    else:
                        parts = []
                        for k in range(6):
                            here = v_ref[spot * 6 + k, at : at + 8, :]
                            parts.append(
                                jnp.where(wraps, pltpu.roll(here, LZ - 1, 1), pltpu.roll(here, LANES - 1, 1))
                            )
                    outs = link_product(links, (parts[:3], parts[3:]))
                    for half in range(2):
                        for colour in range(3):
                            op_ref[
                                slot,
                                direction,
                                half * count + at : half * count + at + 8,
                                (sub * 3 + colour) * LANES : (sub * 3 + colour + 1) * LANES,
                            ] = outs[half][colour].astype(BF16)

    def multiply(step, slot):
        left = lhs_ref[step]
        plane = step // (tiles // pair)
        g_ref[plane] += nt_dot(left, left)
        for direction in range(3):
            acc_ref[direction] += nt_dot(left, op_ref[slot, direction])

    elementwise(0, 0)

    def body(step, carry):
        slot = lax.rem(step, 2)
        multiply(step - 1, 1 - slot)
        elementwise(step, slot)
        return carry

    lax.fori_loop(1, steps, body, 0)
    multiply(steps - 1, (steps - 1) % 2)

    first = lax.axis_index("space") * planes
    total_re = jnp.zeros((count, count), F32)
    total_im = jnp.zeros((count, count), F32)
    for plane in range(planes):
        real, imag = paired(g_ref[plane], count)
        cosine = phase_ref[first + plane]
        sine = phase_ref[lx + first + plane]
        total_re += cosine * real + sine * imag
        total_im += cosine * imag - sine * real
    sums_ref[0, 0] = total_re
    sums_ref[0, 1] = total_im
    for direction in range(3):
        real, imag = anti(*paired(acc_ref[direction], count))
        sums_ref[direction + 1, 0] = real
        sums_ref[direction + 1, 1] = imag
    for half in range(tiles // pair):
        rim_lhs_ref[half] = lhs_ref[(planes - 1) * (tiles // pair) + half]


def gram(x, u, phases, count, tiles, planes, lx):
    spots = tiles * planes
    pair = 2
    steps = planes * (tiles // pair)
    return pl.pallas_call(
        partial(gram_kernel, count, tiles, planes, lx),
        in_specs=[vspec(), vspec(), sspec()],
        out_specs=[vspec(), vspec()],
        out_shape=[
            jax.ShapeDtypeStruct((OPS, 2, count, count), F32),
            jax.ShapeDtypeStruct((tiles // pair, 2 * count, pair * 3 * LANES), BF16),
        ],
        scratch_shapes=[
            VMEM(((spots + tiles) * 6, count, LANES), F32),
            VMEM((steps, 2 * count, pair * 3 * LANES), BF16),
            VMEM((2, 3, 2 * count, pair * 3 * LANES), BF16),
            VMEM((3, 2 * count, 2 * count), F32),
            VMEM((planes, 2 * count, 2 * count), F32),
        ],
        compiler_params=pltpu.CompilerParams(vmem_limit_bytes=40 * 2**20),
        cost_estimate=cost(8 * 10**9, 5 * 10**6),
        name="gram",
    )(x, u, phases)


def edge_kernel(
    count, tiles, planes, rows, cores, halo_ref, lhs_ref, u_ref, sums_ref, keep_ref, send_ref, op_ref, tot_ref
):
    spots = tiles * planes
    blocks = count // GROUP
    pair = 2
    total = None
    for half_tile in range(tiles // pair):
        for sub in range(pair):
            tile = half_tile * pair + sub
            links = load_links(u_ref, 0, tile * planes + planes - 1, spots)

            for block in range(blocks):
                at = block * GROUP
                parts = [
                    halo_ref[k * tiles + tile, at : at + GROUP, :].astype(F32) for k in range(6)
                ]
                for eight in range(2):
                    vecs = [piece[eight * 8 : eight * 8 + 8] for piece in parts]
                    outs = link_product(links, (vecs[:3], vecs[3:]))
                    for half in range(2):
                        for colour in range(3):
                            start = half * count + at + eight * 8
                            op_ref[
                                half_tile,
                                start : start + 8,
                                (sub * 3 + colour) * LANES : (sub * 3 + colour + 1) * LANES,
                            ] = outs[half][colour].astype(BF16)
        got = nt_dot(lhs_ref[half_tile], op_ref[half_tile])
        total = got if total is None else total + got
    real, imag = anti(*paired(total, count))
    tot_ref[0] = real
    tot_ref[1] = imag
    mine = lax.rem(lax.axis_index("space"), cores)
    for chip in range(count // (rows * cores)):
        for which, ref in ((mine, keep_ref), (1 - mine, send_ref)):
            at = pl.multiple_of((chip * cores + which) * rows, rows)
            for op in range(OPS):
                for half in range(2):
                    piece = sums_ref[op, half, pl.ds(at, rows), :]
                    if op == 1:
                        piece = piece + tot_ref[half, pl.ds(at, rows), :]
                    ref[chip, op, half] = piece


def edge(halo, rim_lhs, u, sums, count, tiles, planes, rows, cores):
    pair = 2
    shape = jax.ShapeDtypeStruct((count // (rows * cores), OPS, 2, rows, count), F32)
    return pl.pallas_call(
        partial(edge_kernel, count, tiles, planes, rows, cores),
        in_specs=[vspec()] * 4,
        out_specs=[vspec(), vspec()],
        out_shape=[shape, shape],
        scratch_shapes=[
            VMEM((tiles // pair, 2 * count, pair * 3 * LANES), BF16),
            VMEM((2, count, count), F32),
        ],
        cost_estimate=cost(10**9, 3 * 10**6),
        name="edge",
    )(halo, rim_lhs, u, sums)


def fold_kernel(chips, keep_ref, got_ref, own_ref, *out_refs):
    me = lax.axis_index("space") // 2
    own_ref[...] = keep_ref[me] + got_ref[me]
    for step in range(1, chips):
        to = me ^ step
        out_refs[step - 1][...] = keep_ref[to] + got_ref[to]


def fold(keep, got):
    chips = keep.shape[0]
    shape = jax.ShapeDtypeStruct(keep.shape[1:], F32)
    return pl.pallas_call(
        partial(fold_kernel, chips),
        in_specs=[vspec()] * 2,
        out_specs=[vspec()] * chips,
        out_shape=[shape] * chips,
        cost_estimate=cost(10**6, 10**6),
        name="fold",
    )(keep, got)


def total_kernel(*refs):
    total = refs[0][...]
    for ref in refs[1:-1]:
        total = total + ref[...]
    refs[-1][...] = total.astype(BF16)


def total_rows(parts):
    return pl.pallas_call(
        total_kernel,
        in_specs=[vspec()] * len(parts),
        out_specs=vspec(),
        out_shape=jax.ShapeDtypeStruct(parts[0].shape, BF16),
        cost_estimate=cost(10**6, 10**6),
        name="total",
    )(*parts)


def table_kernel(groups, jobs, slots, empty, owner_ref, elem_ref, source_ref, spin_ref, out_ref):
    me = lax.axis_index("tm")

    def clear(at, carry):
        out_ref[at] = empty
        return carry

    lax.fori_loop(0, groups * slots + 1, clear, 0)
    for group in range(groups):

        def place(job, used):
            at = group * jobs + job
            mine = owner_ref[at] == me
            product = (source_ref[at] * SPIN + spin_ref[at]) * (groups * OPS) + group * OPS + elem_ref[at]
            spot = jnp.where(mine, group * slots + used, groups * slots)
            out_ref[spot] = product
            return used + mine.astype(jnp.int32)

        lax.fori_loop(0, jobs, place, jnp.int32(0))


def job_table(owner, elem, source, spin, groups, slots, empty):
    jobs = owner.shape[0] // groups
    return pl.pallas_call(
        partial(table_kernel, groups, jobs, slots, empty),
        in_specs=[sspec()] * 4,
        out_specs=sspec(),
        out_shape=jax.ShapeDtypeStruct((groups * slots + 1,), jnp.int32),
        cost_estimate=cost(10**5, 10**4),
        name="table",
    )(owner, elem, source, spin)


def dress_kernel(groups, slots, taus, rows, count, table_ref, per_ref, *refs):
    slab_refs = refs[:groups]
    out_ref, lhs_ref, prod_ref = refs[groups:]
    me = lax.axis_index("tm")
    for step in range(groups):
        group = me ^ step
        for op in range(OPS):
            at = pl.multiple_of((group * OPS + op) * rows, rows)
            lhs_ref[pl.ds(at, rows), 0:count] = slab_refs[step][op, 0]
            lhs_ref[pl.ds(at, rows), count : 2 * count] = slab_refs[step][op, 1]
    left = lhs_ref[...]
    for tau in range(taus):
        real, imag = per_ref[tau, 0], per_ref[tau, 1]
        right = jnp.concatenate(
            [jnp.concatenate([real, imag], axis=1), jnp.concatenate([-imag, real], axis=1)], axis=0
        )
        got = jnp.dot(left, right, preferred_element_type=F32).astype(BF16)
        for piece in range(groups * OPS):
            prod_ref[tau * groups * OPS + piece] = got[piece * rows : (piece + 1) * rows]
    prod_ref[taus * groups * OPS] = jnp.zeros((rows, 2 * count), BF16)
    for group in range(groups):
        for slot in range(slots):
            piece = prod_ref[table_ref[group * slots + slot]]
            out_ref[group, slot, 0] = piece[:, :count]
            out_ref[group, slot, 1] = piece[:, count:]


def dress(table, per, slabs, groups, slots, rows, count):
    taus = per.shape[0]
    return pl.pallas_call(
        partial(dress_kernel, groups, slots, taus, rows, count),
        in_specs=[sspec(), vspec()] + [vspec()] * groups,
        out_specs=vspec(),
        out_shape=jax.ShapeDtypeStruct((groups, slots, 2, rows, count), BF16),
        scratch_shapes=[
            VMEM((groups * OPS * rows, 2 * count), BF16),
            VMEM((taus * groups * OPS + 1, rows, 2 * count), BF16),
        ],
        cost_estimate=cost(10**9, 2 * 10**6),
        name="dress",
    )(table, per, *slabs)


def fast_shards(eigvecs, gauge_links, perambulator, job_owner, job_elemental, job_source, job_spin):
    count = eigvecs.shape[1]
    planes, sites = eigvecs.shape[4], eigvecs.shape[5]
    tiles = sites // LANES
    space_size = lax.axis_size("space")
    groups = lax.axis_size("tm")
    lx = planes * space_size
    rows = count // space_size
    slots = 3 * ((JOB_DEV + groups - 1) // groups)
    cores = 2

    def tiled(field):
        head = field.shape[:-2]
        order = tuple(range(len(head))) + (len(head) + 1, len(head), len(head) + 2)
        split = field.reshape(head + (planes, tiles, LANES))
        return split.transpose(order).reshape(-1, LANES)

    x = tiled(eigvecs)
    u = tiled(gauge_links)
    angle = 2.0 * math.pi / lx * np.arange(lx)
    phases = jnp.asarray(np.concatenate([np.cos(angle), np.sin(angle)]).astype(np.float32))

    rim = rim_plane(x, count, tiles, planes)
    halo = lax.ppermute(rim, "space", [(i, (i - 1) % space_size) for i in range(space_size)])
    sums, rim_lhs = gram(x, u, phases, count, tiles, planes, lx)
    per = perambulator.reshape(-1, 2, count, count)
    table = job_table(
        job_owner.reshape(-1), job_elemental, job_source, job_spin, groups, slots, per.shape[0] * groups * OPS
    )
    keep, send = edge(halo, rim_lhs, u, sums, count, tiles, planes, rows, cores)
    got = lax.ppermute(send, "space", [(i, i ^ 1) for i in range(space_size)])
    parts = fold(keep, got)
    summed = [parts[0]]
    for step in range(1, space_size // cores):
        summed.append(
            lax.ppermute(parts[step], "space", [(i, i ^ (step * cores)) for i in range(space_size)])
        )
    own = total_rows(summed)
    slabs = [own]
    for step in range(1, groups):
        slabs.append(lax.ppermute(own, "tm", [(i, i ^ step) for i in range(groups)]))
    return dress(table, per, slabs, groups, slots, rows, count)[None]


def passed_along(shard, axis, by):
    count = lax.axis_size(axis)
    return lax.ppermute(shard, axis, [(i, (i + by) % count) for i in range(count)])


def shifted_sites(lattice_field, direction, offset):
    shaped = lattice_field.reshape(lattice_field.shape[:-1] + (LY, LZ))
    rolled = jnp.roll(shaped, -offset, axis=direction - 4)
    return rolled.reshape(lattice_field.shape)


def apply_link(link_field, vectors):
    total_re = None
    total_im = None
    for colour in range(3):
        link_re = link_field[0, :, colour][None]
        link_im = link_field[1, :, colour][None]
        vector_re = vectors[:, 0, colour][:, None]
        vector_im = vectors[:, 1, colour][:, None]
        part_re = link_re * vector_re - link_im * vector_im
        part_im = link_re * vector_im + link_im * vector_re
        if colour == 0:
            total_re, total_im = (part_re, part_im)
        else:
            total_re = total_re + part_re
            total_im = total_im + part_im
    return jnp.stack([total_re, total_im], axis=1)


def stacked_form(vectors):
    vector_count = vectors.shape[0]
    swapped = jnp.concatenate([-vectors[:, 1:2], vectors[:, 0:1]], axis=1)
    return jnp.concatenate(
        [vectors.reshape(vector_count, -1), swapped.reshape(vector_count, -1)], axis=0
    )


def paired_gram(stacked, lattice_field):
    vector_count = lattice_field.shape[0]
    flat_field = lattice_field.astype(jnp.bfloat16).reshape(vector_count, -1)
    product = lax.dot_general(
        stacked, flat_field, (((1,), (1,)), ((), ())), preferred_element_type=jnp.float32
    )
    return product.reshape(2, vector_count, vector_count)


def twisted_field(vectors, xcoord):
    phase_angle = 2.0 * math.pi / (vectors.shape[3] * lax.axis_size("space")) * xcoord
    cosine = jnp.cos(phase_angle)[:, None]
    sine_part = jnp.sin(phase_angle)[:, None]
    real_part = cosine * vectors[:, 0] + sine_part * vectors[:, 1]
    imag_part = cosine * vectors[:, 1] - sine_part * vectors[:, 0]
    return jnp.stack([real_part, imag_part], axis=1)


def antihermitian(paired):
    return 0.5 * jnp.stack([paired[0] - paired[0].T, paired[1] + paired[1].T], axis=0)


def plain_shards(eigvecs, gauge_links, perambulator, job_owner, job_elemental, job_source, job_spin):
    slice_count = eigvecs.shape[0]
    vector_count = eigvecs.shape[1]
    planes = eigvecs.shape[4]
    space_size = lax.axis_size("space")
    group_count = lax.axis_size("tm")
    row_count = vector_count // space_size
    capacity = 3 * ((JOB_DEV + group_count - 1) // group_count)
    xcoord = (lax.axis_index("space") * planes + jnp.arange(planes, dtype=jnp.int32)).astype(
        jnp.float32
    )
    upper_plane = passed_along(eigvecs[:, :, :, :, 0:1], "space", -1)
    low_vectors = eigvecs[0]
    vectors = low_vectors.astype(jnp.float32)
    stacked = stacked_form(low_vectors)
    results = [paired_gram(stacked, twisted_field(vectors, xcoord))]
    for direction in (1, 2, 3):
        link_field = gauge_links[0, direction - 1]
        if direction == 1:
            upper_rim = upper_plane[0].astype(jnp.float32)
            above_field = jnp.concatenate([vectors[:, :, :, 1:], upper_rim], axis=3)
        else:
            above_field = shifted_sites(vectors, direction, 1)
        forward = apply_link(link_field, above_field)
        results.append(antihermitian(paired_gram(stacked, forward)))
    partial_list = [jnp.stack(results, axis=0)]
    partial_value = jnp.stack(partial_list, axis=0)
    summed = lax.psum(partial_value, "space")
    own_rows = lax.dynamic_slice_in_dim(summed, lax.axis_index("space") * row_count, row_count, 3)
    slab_table = own_rows.astype(jnp.bfloat16).reshape(
        slice_count * OPS, 2 * row_count * vector_count
    )
    owners = job_owner[:, 0].reshape(group_count, -1)
    elements = job_elemental.reshape(group_count, -1)
    position = jnp.arange(owners.shape[1], dtype=jnp.int32)
    earlier = position[None, :] < position[:, None]
    same_owner = owners[:, :, None] == owners[:, None, :]
    slot_rank = jnp.sum(jnp.where(same_owner & earlier[None], 1, 0), axis=2).astype(jnp.int32)
    own_group = lax.axis_index("tm")
    slot_count = group_count * capacity
    live_jobs = owners == own_group
    slot_match = live_jobs[:, None, :] & (
        slot_rank[:, None, :] == jnp.arange(capacity, dtype=jnp.int32)[None, :, None]
    )
    sender_owners = lax.dynamic_index_in_dim(owners, own_group, 0, keepdims=False)
    sender_ranks = lax.dynamic_index_in_dim(slot_rank, own_group, 0, keepdims=False)
    sender_elements = lax.dynamic_index_in_dim(elements, own_group, 0, keepdims=False)
    slot_ids = sender_owners * capacity + sender_ranks
    slot_hot = (jnp.arange(slot_count, dtype=jnp.int32)[:, None] == slot_ids[None, :]).astype(
        jnp.float32
    )
    elem_hot = (
        sender_elements[:, None] == jnp.arange(slice_count * OPS, dtype=jnp.int32)[None, :]
    ).astype(jnp.float32)
    picker = jnp.dot(slot_hot, elem_hot, precision=lax.Precision.HIGHEST).astype(jnp.bfloat16)
    outgoing = jnp.dot(picker, slab_table, preferred_element_type=jnp.float32).astype(jnp.bfloat16)
    outgoing = outgoing.reshape(group_count, capacity, 2, row_count, vector_count)
    received = lax.all_to_all(outgoing, "tm", split_axis=0, concat_axis=0, tiled=True)
    block_index = job_source.reshape(group_count, -1) * SPIN + job_spin.reshape(group_count, -1)
    tau_index = jnp.sum(jnp.where(slot_match, block_index[:, None, :], 0), axis=2)
    blocks = perambulator.reshape(-1, 2 * vector_count, vector_count)
    chosen = jnp.take(blocks, tau_index.reshape(-1), axis=0)
    slab_rows = received.reshape(slot_count, 2, row_count, vector_count)
    real_rows = jnp.concatenate([slab_rows[:, 0], -slab_rows[:, 1]], axis=-1)
    imag_rows = jnp.concatenate([slab_rows[:, 1], slab_rows[:, 0]], axis=-1)
    left_side = jnp.stack([real_rows, imag_rows], axis=1).reshape(
        slot_count, 2 * row_count, 2 * vector_count
    )
    dressed = lax.dot_general(
        left_side, chosen, (((2,), (1,)), ((0,), (0,))), preferred_element_type=jnp.float32
    )
    return dressed.astype(jnp.bfloat16).reshape(
        1, group_count, capacity, 2, row_count, vector_count
    )


def shards(*args):
    eigvecs = args[0]
    count, planes, sites = eigvecs.shape[1], eigvecs.shape[4], eigvecs.shape[5]
    space_size, groups = lax.axis_size("space"), lax.axis_size("tm")
    whole_tiles = sites % (2 * LANES) == 0 and count == LANES and planes * (sites // LANES) == GROUP
    powers = space_size & (space_size - 1) == 0 and groups & (groups - 1) == 0
    small = space_size * GROUP == count and groups <= 8
    if whole_tiles and powers and small and eigvecs.shape[0] == 1:
        return fast_shards(*args)
    return plain_shards(*args)


def solution(mesh):
    return jax.shard_map(
        shards,
        mesh=mesh,
        in_specs=(
            P("tm", None, None, None, "space", None),
            P("tm", None, None, None, None, "space", None),
            P("tm", None, None, None, None),
            P(),
            P(),
            P(),
            P(),
        ),
        out_specs=P("tm", None, None, None, "space", None),
        check_vma=False,
    )
```

```python
import math
from functools import partial

import numpy as np
import jax
import jax.numpy as jnp
from jax import lax
from jax.experimental import pallas as pl
from jax.experimental.pallas import tpu as pltpu
from jax.sharding import PartitionSpec as P

LY = 16
LZ = 32
OPS = 4
SPIN = 4
JOB_DEV = 24
LANES = 128
GROUP = 16
F32 = jnp.float32
BF16 = jnp.bfloat16
VMEM = pltpu.VMEM
SMEM = pltpu.SMEM


def vspec():
    return pl.BlockSpec(memory_space=VMEM)


def sspec():
    return pl.BlockSpec(memory_space=SMEM)


def cost(flops, moved):
    return pl.CostEstimate(flops=flops, bytes_accessed=moved, transcendentals=0)


def limit(mebibytes):
    return pltpu.CompilerParams(vmem_limit_bytes=mebibytes * 2**20)


def pick_matrix(rows, cols, source_of):
    row = lax.broadcasted_iota(jnp.int32, (rows, cols), 0)
    col = lax.broadcasted_iota(jnp.int32, (rows, cols), 1)
    return jnp.where(col == source_of(row), 1.0, 0.0).astype(BF16)


def nt_dot(left, right):
    return lax.dot_general(left, right, (((1,), (1,)), ((), ())), preferred_element_type=F32)


def rim_kernel(tiles, planes, x_hbm, u_hbm, out_ref, x_ref, u_ref, pick_ref, sems):
    spots = tiles * planes
    chunk = GROUP * 6 * spots
    chunks = x_hbm.shape[0] // chunk
    copies = []
    for g in range(chunks):
        rows = pl.ds(g * chunk, chunk)
        copies.append(pltpu.make_async_copy(x_hbm.at[rows], x_ref.at[rows], sems.at[g]))
    copies.append(pltpu.make_async_copy(u_hbm, u_ref, sems.at[chunks]))
    for copy in copies:
        copy.start()

    def source(row):
        return (row & (GROUP - 1)) * spots + (row // GROUP) * planes

    pick_ref[...] = pick_matrix(tiles * GROUP, GROUP * spots, source)
    chosen = pick_ref[...]
    for g in range(chunks):
        copies[g].wait()
        block = x_ref[g * chunk : (g + 1) * chunk, :].reshape(GROUP, 6, spots, LANES)
        for part in range(0, 6, 2):
            rows = jnp.concatenate(
                [block[:, part + k].reshape(GROUP * spots, LANES) for k in range(2)], axis=1
            )
            taken = jnp.dot(chosen, rows, preferred_element_type=F32).astype(BF16)
            for k in range(2):
                for tile in range(tiles):
                    out_ref[(part + k) * tiles + tile, g * GROUP : (g + 1) * GROUP] = taken[
                        tile * GROUP : (tile + 1) * GROUP, k * LANES : (k + 1) * LANES
                    ]
    copies[chunks].wait()


def rim_plane(x, u, count, tiles, planes):
    spots = tiles * planes
    return pl.pallas_call(
        partial(rim_kernel, tiles, planes),
        in_specs=[pl.BlockSpec(memory_space=pltpu.HBM)] * 2,
        out_specs=[vspec()] * 3,
        out_shape=[
            jax.ShapeDtypeStruct((6 * tiles, count, LANES), BF16),
            jax.ShapeDtypeStruct(x.shape, BF16),
            jax.ShapeDtypeStruct(u.shape, F32),
        ],
        scratch_shapes=[
            VMEM((tiles * GROUP, GROUP * spots), BF16),
            pltpu.SemaphoreType.DMA((count // GROUP + 1,)),
        ],
        compiler_params=limit(8),
        cost_estimate=cost(10**8, 4 * 10**6),
        name="rim",
    )(x, u)


def link_product(links, vec_re, vec_im):
    plus = [vec_re[c] + vec_im[c] for c in range(3)]
    minus = [vec_im[c] - vec_re[c] for c in range(3)]
    outs_re, outs_im = [], []
    for row in range(3):
        link_re, link_im, link_sum = links[0][row], links[1][row], links[2][row]
        one = link_sum[0] * vec_re[0] + link_sum[1] * vec_re[1] + link_sum[2] * vec_re[2]
        two = link_re[0] * minus[0] + link_re[1] * minus[1] + link_re[2] * minus[2]
        three = link_im[0] * plus[0] + link_im[1] * plus[1] + link_im[2] * plus[2]
        outs_re.append(one - three)
        outs_im.append(one + two)
    return outs_re, outs_im


def load_links(u_ref, direction, spot, spots):
    def one(part, row, col):
        at = (((direction * 2 + part) * 3 + row) * 3 + col) * spots + spot
        return jnp.broadcast_to(u_ref[pl.ds(at, 1), :], (8, LANES))

    grid = [[[one(part, row, col) for col in range(3)] for row in range(3)] for part in range(2)]
    total = [[grid[0][row][col] + grid[1][row][col] for col in range(3)] for row in range(3)]
    return grid + [total]


def paired(grid, count):
    real = grid[:count, :count] + grid[count:, count:]
    imag = grid[count:, :count] - grid[:count, count:]
    return real, imag


def anti(real, imag):
    return 0.5 * (real.T - real), 0.5 * (imag.T + imag)


def gram_kernel(
    count, tiles, planes, lx, groups, slots, empty,
    x_ref, u_ref, phase_ref, owner_ref, elem_ref, source_ref, spin_ref,
    sums_ref, rim_lhs_ref, table_ref,
    v_ref, lhs_ref, op_ref, acc_ref, g_ref, pick_ref,
):
    spots = tiles * planes
    pair = 2
    halves = tiles // pair
    steps = planes * halves
    total_jobs = owner_ref.shape[0]
    jobs = total_jobs // groups
    me = lax.axis_index("tm")

    def source(row):
        spot = row // GROUP
        return (row & (GROUP - 1)) * spots + (spot % tiles) * planes + spot // tiles

    pick_ref[...] = pick_matrix(GROUP * spots, GROUP * spots, source)
    acc_ref[...] = jnp.zeros_like(acc_ref)
    g_ref[...] = jnp.zeros_like(g_ref)
    for at in range(groups * slots):
        table_ref[at] = empty

    chosen = pick_ref[...]
    for at in range(0, count, GROUP):
        block = x_ref[at * 6 * spots : (at + GROUP) * 6 * spots, :].reshape(GROUP, 6, spots, LANES)
        for first in range(0, 6, 2):
            rows = jnp.concatenate(
                [block[:, first + k].reshape(GROUP * spots, LANES) for k in range(2)], axis=1
            )
            taken = jnp.dot(chosen, rows, preferred_element_type=F32)
            for k in range(2):
                part = first + k
                half, colour = part // 3, part % 3
                for spot in range(spots):
                    piece = taken[spot * GROUP : (spot + 1) * GROUP, k * LANES : (k + 1) * LANES]
                    v_ref[spot * 6 + part, at : at + GROUP, :] = piece
                    plane, tile = spot // tiles, spot % tiles
                    lhs_ref[
                        plane * halves + tile // pair,
                        half * count + at : half * count + at + GROUP,
                        ((tile % pair) * 3 + colour) * LANES : ((tile % pair) * 3 + colour + 1) * LANES,
                    ] = piece.astype(BF16)

    lane = lax.broadcasted_iota(jnp.int32, (8, LANES), 1)
    wraps = (lane & (LZ - 1)) == LZ - 1
    spills = lane < LZ

    def elementwise(step, slot, directions):
        plane = step // halves
        half_tile = step % halves
        for sub in range(pair):
            tile = half_tile * pair + sub
            spot = plane * tiles + tile
            next_tile = plane * tiles + (tile + 1) % tiles
            for direction in directions:
                links = load_links(u_ref, direction, tile * planes + plane, spots)
                for at in range(0, count, 8):

                    def part(where, k):
                        return v_ref[where * 6 + k, at : at + 8, :]

                    if direction == 0:
                        vec = [part(spot + tiles, k) for k in range(6)]
                    elif direction == 1:
                        vec = [
                            pltpu.roll(jnp.where(spills, part(next_tile, k), part(spot, k)), LANES - LZ, 1)
                            for k in range(6)
                        ]
                    else:
                        vec = [
                            jnp.where(
                                wraps,
                                pltpu.roll(part(spot, k), LZ - 1, 1),
                                pltpu.roll(part(spot, k), LANES - 1, 1),
                            )
                            for k in range(6)
                        ]
                    outs = link_product(links, vec[:3], vec[3:])
                    for half in range(2):
                        row = (direction * 2 + half) * count + at
                        for colour in range(3):
                            column = (sub * 3 + colour) * LANES
                            op_ref[slot, row : row + 8, column : column + LANES] = outs[half][colour].astype(
                                BF16
                            )

    def multiply(step, slot, directions):
        fixed = lhs_ref[step]
        g_ref[step // halves] += nt_dot(fixed, fixed)
        low = min(directions) * 2 * count
        high = (max(directions) + 1) * 2 * count
        acc_ref[low:high, :] += nt_dot(op_ref[slot, low:high, :], fixed)

    def place(group):
        used = jnp.int32(0)
        for at in range(group * jobs, (group + 1) * jobs):
            mine = owner_ref[at] == me
            product = source_ref[at] * (SPIN * groups * OPS) + spin_ref[at] * (groups * OPS) + elem_ref[at]
            table_ref[jnp.where(mine, group * slots + used, groups * slots)] = product + group * OPS
            used = used + jnp.where(mine, 1, 0)

    every, side = (0, 1, 2), (1, 2)
    inner = steps - halves
    elementwise(0, 0, every)

    def body(step, carry):
        slot = step & 1
        multiply(step - 1, 1 - slot, every)
        elementwise(step, slot, every)
        return carry

    lax.fori_loop(1, inner, body, 0)
    multiply(inner - 1, (inner - 1) & 1, every)
    for step in range(inner, steps):
        elementwise(step, step & 1, side)
        multiply(step, step & 1, side)
    for group in range(groups):
        place(group)

    first = lax.axis_index("space") * planes
    total_re = jnp.zeros((count, count), F32)
    total_im = jnp.zeros((count, count), F32)
    for plane in range(planes):
        real, imag = paired(g_ref[plane], count)
        cosine = phase_ref[first + plane]
        sine = phase_ref[lx + first + plane]
        total_re += cosine * real - sine * imag
        total_im += cosine * imag + sine * real
    sums_ref[0, 0] = total_re
    sums_ref[0, 1] = -total_im
    for direction in range(3):
        grid = acc_ref[direction * 2 * count : (direction + 1) * 2 * count, :]
        real, imag = anti(*paired(grid, count))
        sums_ref[direction + 1, 0] = real
        sums_ref[direction + 1, 1] = imag
    for half in range(halves):
        rim_lhs_ref[half] = lhs_ref[(planes - 1) * halves + half]


def gram(x, u, phases, tables, count, tiles, planes, lx, groups, slots, empty):
    spots = tiles * planes
    pair = 2
    steps = planes * (tiles // pair)
    wide = pair * 3 * LANES
    return pl.pallas_call(
        partial(gram_kernel, count, tiles, planes, lx, groups, slots, empty),
        in_specs=[vspec(), vspec()] + [sspec()] * 5,
        out_specs=[vspec(), vspec(), sspec()],
        out_shape=[
            jax.ShapeDtypeStruct((OPS, 2, count, count), F32),
            jax.ShapeDtypeStruct((tiles // pair, 2 * count, wide), BF16),
            jax.ShapeDtypeStruct((groups * slots + 1,), jnp.int32),
        ],
        scratch_shapes=[
            VMEM((spots * 6, count, LANES), F32),
            VMEM((steps, 2 * count, wide), BF16),
            VMEM((2, 6 * count, wide), BF16),
            VMEM((6 * count, 2 * count), F32),
            VMEM((planes, 2 * count, 2 * count), F32),
            VMEM((GROUP * spots, GROUP * spots), BF16),
        ],
        compiler_params=limit(26),
        cost_estimate=cost(8 * 10**9, 5 * 10**6),
        name="gram",
    )(x, u, phases, *tables)


def edge_kernel(
    count, tiles, planes, rows, cores, halo_ref, lhs_ref, u_ref, sums_ref, keep_ref, send_ref, op_ref, tot_ref
):
    spots = tiles * planes
    pair = 2
    total = None
    for half_tile in range(tiles // pair):
        for sub in range(pair):
            tile = half_tile * pair + sub
            links = load_links(u_ref, 0, tile * planes + planes - 1, spots)
            for at in range(0, count, GROUP):
                parts = [halo_ref[k * tiles + tile, at : at + GROUP, :].astype(F32) for k in range(6)]
                outs = [
                    link_product(
                        links,
                        [part[eight : eight + 8] for part in parts[:3]],
                        [part[eight : eight + 8] for part in parts[3:]],
                    )
                    for eight in (0, 8)
                ]
                for half in range(2):
                    for colour in range(3):
                        column = (sub * 3 + colour) * LANES
                        both = jnp.concatenate([outs[0][half][colour], outs[1][half][colour]], axis=0)
                        op_ref[
                            half_tile, half * count + at : half * count + at + GROUP, column : column + LANES
                        ] = both.astype(BF16)
        got = nt_dot(op_ref[half_tile], lhs_ref[half_tile])
        total = got if total is None else total + got
    real, imag = anti(*paired(total, count))
    tot_ref[0] = real
    tot_ref[1] = imag
    mine = lax.axis_index("space") & (cores - 1)
    for chip in range(count // (rows * cores)):
        for which, ref in ((mine, keep_ref), (1 - mine, send_ref)):
            at = pl.multiple_of((chip * cores + which) * rows, rows)
            for op in range(OPS):
                for half in range(2):
                    piece = sums_ref[op, half, pl.ds(at, rows), :]
                    if op == 1:
                        piece = piece + tot_ref[half, pl.ds(at, rows), :]
                    ref[chip, op, half] = piece


def edge(halo, rim_lhs, u, sums, count, tiles, planes, rows, cores):
    pair = 2
    shape = jax.ShapeDtypeStruct((count // (rows * cores), OPS, 2, rows, count), F32)
    return pl.pallas_call(
        partial(edge_kernel, count, tiles, planes, rows, cores),
        in_specs=[vspec()] * 4,
        out_specs=[vspec(), vspec()],
        out_shape=[shape, shape],
        scratch_shapes=[
            VMEM((tiles // pair, 2 * count, pair * 3 * LANES), BF16),
            VMEM((2, count, count), F32),
        ],
        compiler_params=limit(8),
        cost_estimate=cost(10**9, 3 * 10**6),
        name="edge",
    )(halo, rim_lhs, u, sums)


def fold_kernel(chips, keep_ref, got_ref, own_ref, *out_refs):
    me = lax.axis_index("space") // 2
    own_ref[...] = keep_ref[me] + got_ref[me]
    for step in range(1, chips):
        to = me ^ step
        out_refs[step - 1][...] = keep_ref[to] + got_ref[to]


def fold(keep, got):
    chips = keep.shape[0]
    shape = jax.ShapeDtypeStruct(keep.shape[1:], F32)
    return pl.pallas_call(
        partial(fold_kernel, chips),
        in_specs=[vspec()] * 2,
        out_specs=[vspec()] * chips,
        out_shape=[shape] * chips,
        compiler_params=limit(4),
        cost_estimate=cost(10**6, 10**6),
        name="fold",
    )(keep, got)


def total_kernel(*refs):
    total = refs[0][...]
    for ref in refs[1:-1]:
        total = total + ref[...]
    refs[-1][...] = total.astype(BF16)


def total_rows(parts):
    return pl.pallas_call(
        total_kernel,
        in_specs=[vspec()] * len(parts),
        out_specs=vspec(),
        out_shape=jax.ShapeDtypeStruct(parts[0].shape, BF16),
        compiler_params=limit(4),
        cost_estimate=cost(10**6, 10**6),
        name="total",
    )(*parts)


def dress_kernel(groups, slots, taus, rows, count, table_ref, per_ref, *refs):
    slab_refs = refs[:groups]
    out_ref, lhs_ref, prod_ref = refs[groups:]
    me = lax.axis_index("tm")
    for step in range(groups):
        group = me ^ step
        for op in range(OPS):
            at = pl.multiple_of((group * OPS + op) * rows, rows)
            lhs_ref[pl.ds(at, rows), 0:count] = slab_refs[step][op, 0]
            lhs_ref[pl.ds(at, rows), count : 2 * count] = slab_refs[step][op, 1]
    left = lhs_ref[...]
    for tau in range(taus):
        real, imag = per_ref[tau, 0], per_ref[tau, 1]
        right = jnp.concatenate(
            [jnp.concatenate([real, imag], axis=1), jnp.concatenate([-imag, real], axis=1)], axis=0
        )
        got = jnp.dot(left, right, preferred_element_type=F32).astype(BF16)
        for piece in range(groups * OPS):
            prod_ref[tau * groups * OPS + piece] = got[piece * rows : (piece + 1) * rows]
    prod_ref[taus * groups * OPS] = jnp.zeros((rows, 2 * count), BF16)
    for group in range(groups):
        for slot in range(slots):
            piece = prod_ref[table_ref[group * slots + slot]]
            out_ref[group, slot, 0] = piece[:, :count]
            out_ref[group, slot, 1] = piece[:, count:]


def dress(table, per, slabs, groups, slots, rows, count):
    taus = per.shape[0]
    return pl.pallas_call(
        partial(dress_kernel, groups, slots, taus, rows, count),
        in_specs=[sspec(), vspec()] + [vspec()] * groups,
        out_specs=vspec(),
        out_shape=jax.ShapeDtypeStruct((groups, slots, 2, rows, count), BF16),
        scratch_shapes=[
            VMEM((groups * OPS * rows, 2 * count), BF16),
            VMEM((taus * groups * OPS + 1, rows, 2 * count), BF16),
        ],
        compiler_params=limit(8),
        cost_estimate=cost(10**9, 2 * 10**6),
        name="dress",
    )(table, per, *slabs)


def fast_shards(eigvecs, gauge_links, perambulator, job_owner, job_elemental, job_source, job_spin):
    count = eigvecs.shape[1]
    planes, sites = eigvecs.shape[4], eigvecs.shape[5]
    tiles = sites // LANES
    space_size = lax.axis_size("space")
    groups = lax.axis_size("tm")
    lx = planes * space_size
    rows = count // space_size
    slots = 3 * ((JOB_DEV + groups - 1) // groups)
    cores = 2

    def tiled(field):
        head = field.shape[:-2]
        order = tuple(range(len(head))) + (len(head) + 1, len(head), len(head) + 2)
        split = field.reshape(head + (planes, tiles, LANES))
        return split.transpose(order).reshape(-1, LANES)

    x = tiled(eigvecs)
    u = tiled(gauge_links)
    angle = 2.0 * math.pi / lx * np.arange(lx)
    phases = jnp.asarray(np.concatenate([np.cos(angle), np.sin(angle)]).astype(np.float32))

    per = perambulator.reshape(-1, 2, count, count)
    empty = per.shape[0] * groups * OPS
    rim, x, u = rim_plane(x, u, count, tiles, planes)
    halo = lax.ppermute(rim, "space", [(i, (i - 1) % space_size) for i in range(space_size)])
    tables = (job_owner.reshape(-1), job_elemental, job_source, job_spin)
    sums, rim_lhs, table = gram(
        x, u, phases, tables, count, tiles, planes, lx, groups, slots, empty
    )
    keep, send = edge(halo, rim_lhs, u, sums, count, tiles, planes, rows, cores)
    got = lax.ppermute(send, "space", [(i, i ^ 1) for i in range(space_size)])
    parts = fold(keep, got)
    summed = [parts[0]]
    for step in range(1, space_size // cores):
        summed.append(
            lax.ppermute(parts[step], "space", [(i, i ^ (step * cores)) for i in range(space_size)])
        )
    own = total_rows(summed)
    slabs = [own]
    for step in range(1, groups):
        slabs.append(lax.ppermute(own, "tm", [(i, i ^ step) for i in range(groups)]))
    return dress(table, per, slabs, groups, slots, rows, count)[None]


def passed_along(shard, axis, by):
    count = lax.axis_size(axis)
    return lax.ppermute(shard, axis, [(i, (i + by) % count) for i in range(count)])


def shifted_sites(lattice_field, direction, offset):
    shaped = lattice_field.reshape(lattice_field.shape[:-1] + (LY, LZ))
    rolled = jnp.roll(shaped, -offset, axis=direction - 4)
    return rolled.reshape(lattice_field.shape)


def apply_link(link_field, vectors):
    total_re = None
    total_im = None
    for colour in range(3):
        link_re = link_field[0, :, colour][None]
        link_im = link_field[1, :, colour][None]
        vector_re = vectors[:, 0, colour][:, None]
        vector_im = vectors[:, 1, colour][:, None]
        part_re = link_re * vector_re - link_im * vector_im
        part_im = link_re * vector_im + link_im * vector_re
        if colour == 0:
            total_re, total_im = (part_re, part_im)
        else:
            total_re = total_re + part_re
            total_im = total_im + part_im
    return jnp.stack([total_re, total_im], axis=1)


def stacked_form(vectors):
    vector_count = vectors.shape[0]
    swapped = jnp.concatenate([-vectors[:, 1:2], vectors[:, 0:1]], axis=1)
    return jnp.concatenate(
        [vectors.reshape(vector_count, -1), swapped.reshape(vector_count, -1)], axis=0
    )


def paired_gram(stacked, lattice_field):
    vector_count = lattice_field.shape[0]
    flat_field = lattice_field.astype(jnp.bfloat16).reshape(vector_count, -1)
    product = lax.dot_general(
        stacked, flat_field, (((1,), (1,)), ((), ())), preferred_element_type=jnp.float32
    )
    return product.reshape(2, vector_count, vector_count)


def twisted_field(vectors, xcoord):
    phase_angle = 2.0 * math.pi / (vectors.shape[3] * lax.axis_size("space")) * xcoord
    cosine = jnp.cos(phase_angle)[:, None]
    sine_part = jnp.sin(phase_angle)[:, None]
    real_part = cosine * vectors[:, 0] + sine_part * vectors[:, 1]
    imag_part = cosine * vectors[:, 1] - sine_part * vectors[:, 0]
    return jnp.stack([real_part, imag_part], axis=1)


def antihermitian(paired):
    return 0.5 * jnp.stack([paired[0] - paired[0].T, paired[1] + paired[1].T], axis=0)


def plain_shards(eigvecs, gauge_links, perambulator, job_owner, job_elemental, job_source, job_spin):
    slice_count = eigvecs.shape[0]
    vector_count = eigvecs.shape[1]
    planes = eigvecs.shape[4]
    space_size = lax.axis_size("space")
    group_count = lax.axis_size("tm")
    row_count = vector_count // space_size
    capacity = 3 * ((JOB_DEV + group_count - 1) // group_count)
    xcoord = (lax.axis_index("space") * planes + jnp.arange(planes, dtype=jnp.int32)).astype(
        jnp.float32
    )
    upper_plane = passed_along(eigvecs[:, :, :, :, 0:1], "space", -1)
    low_vectors = eigvecs[0]
    vectors = low_vectors.astype(jnp.float32)
    stacked = stacked_form(low_vectors)
    results = [paired_gram(stacked, twisted_field(vectors, xcoord))]
    for direction in (1, 2, 3):
        link_field = gauge_links[0, direction - 1]
        if direction == 1:
            upper_rim = upper_plane[0].astype(jnp.float32)
            above_field = jnp.concatenate([vectors[:, :, :, 1:], upper_rim], axis=3)
        else:
            above_field = shifted_sites(vectors, direction, 1)
        forward = apply_link(link_field, above_field)
        results.append(antihermitian(paired_gram(stacked, forward)))
    partial_list = [jnp.stack(results, axis=0)]
    partial_value = jnp.stack(partial_list, axis=0)
    summed = lax.psum(partial_value, "space")
    own_rows = lax.dynamic_slice_in_dim(summed, lax.axis_index("space") * row_count, row_count, 3)
    slab_table = own_rows.astype(jnp.bfloat16).reshape(
        slice_count * OPS, 2 * row_count * vector_count
    )
    owners = job_owner[:, 0].reshape(group_count, -1)
    elements = job_elemental.reshape(group_count, -1)
    position = jnp.arange(owners.shape[1], dtype=jnp.int32)
    earlier = position[None, :] < position[:, None]
    same_owner = owners[:, :, None] == owners[:, None, :]
    slot_rank = jnp.sum(jnp.where(same_owner & earlier[None], 1, 0), axis=2).astype(jnp.int32)
    own_group = lax.axis_index("tm")
    slot_count = group_count * capacity
    live_jobs = owners == own_group
    slot_match = live_jobs[:, None, :] & (
        slot_rank[:, None, :] == jnp.arange(capacity, dtype=jnp.int32)[None, :, None]
    )
    sender_owners = lax.dynamic_index_in_dim(owners, own_group, 0, keepdims=False)
    sender_ranks = lax.dynamic_index_in_dim(slot_rank, own_group, 0, keepdims=False)
    sender_elements = lax.dynamic_index_in_dim(elements, own_group, 0, keepdims=False)
    slot_ids = sender_owners * capacity + sender_ranks
    slot_hot = (jnp.arange(slot_count, dtype=jnp.int32)[:, None] == slot_ids[None, :]).astype(
        jnp.float32
    )
    elem_hot = (
        sender_elements[:, None] == jnp.arange(slice_count * OPS, dtype=jnp.int32)[None, :]
    ).astype(jnp.float32)
    picker = jnp.dot(slot_hot, elem_hot, precision=lax.Precision.HIGHEST).astype(jnp.bfloat16)
    outgoing = jnp.dot(picker, slab_table, preferred_element_type=jnp.float32).astype(jnp.bfloat16)
    outgoing = outgoing.reshape(group_count, capacity, 2, row_count, vector_count)
    received = lax.all_to_all(outgoing, "tm", split_axis=0, concat_axis=0, tiled=True)
    block_index = job_source.reshape(group_count, -1) * SPIN + job_spin.reshape(group_count, -1)
    tau_index = jnp.sum(jnp.where(slot_match, block_index[:, None, :], 0), axis=2)
    blocks = perambulator.reshape(-1, 2 * vector_count, vector_count)
    chosen = jnp.take(blocks, tau_index.reshape(-1), axis=0)
    slab_rows = received.reshape(slot_count, 2, row_count, vector_count)
    real_rows = jnp.concatenate([slab_rows[:, 0], -slab_rows[:, 1]], axis=-1)
    imag_rows = jnp.concatenate([slab_rows[:, 1], slab_rows[:, 0]], axis=-1)
    left_side = jnp.stack([real_rows, imag_rows], axis=1).reshape(
        slot_count, 2 * row_count, 2 * vector_count
    )
    dressed = lax.dot_general(
        left_side, chosen, (((2,), (1,)), ((0,), (0,))), preferred_element_type=jnp.float32
    )
    return dressed.astype(jnp.bfloat16).reshape(
        1, group_count, capacity, 2, row_count, vector_count
    )


def shards(*args):
    eigvecs = args[0]
    count, planes, sites = eigvecs.shape[1], eigvecs.shape[4], eigvecs.shape[5]
    space_size, groups = lax.axis_size("space"), lax.axis_size("tm")
    whole_tiles = sites % (2 * LANES) == 0 and count == LANES and planes * (sites // LANES) == GROUP
    powers = space_size & (space_size - 1) == 0 and groups & (groups - 1) == 0
    small = space_size * GROUP == count and groups <= 8
    if whole_tiles and powers and small and eigvecs.shape[0] == 1:
        return fast_shards(*args)
    return plain_shards(*args)


def solution(mesh):
    return jax.shard_map(
        shards,
        mesh=mesh,
        in_specs=(
            P("tm", None, None, None, "space", None),
            P("tm", None, None, None, None, "space", None),
            P("tm", None, None, None, None),
            P(),
            P(),
            P(),
            P(),
        ),
        out_specs=P("tm", None, None, None, "space", None),
        check_vma=False,
    )
```

```python
import math
from functools import partial

import numpy as np
import jax
import jax.numpy as jnp
from jax import lax
from jax.experimental import pallas as pl
from jax.experimental.pallas import tpu as pltpu
from jax.sharding import PartitionSpec as P

LY = 16
LZ = 32
OPS = 4
SPIN = 4
JOB_DEV = 24
LANES = 128
GROUP = 16
F32 = jnp.float32
BF16 = jnp.bfloat16
VMEM = pltpu.VMEM
SMEM = pltpu.SMEM


def vspec():
    return pl.BlockSpec(memory_space=VMEM)


def sspec():
    return pl.BlockSpec(memory_space=SMEM)


def cost(flops, moved):
    return pl.CostEstimate(flops=flops, bytes_accessed=moved, transcendentals=0)


def limit(mebibytes):
    return pltpu.CompilerParams(vmem_limit_bytes=mebibytes * 2**20)


def pick_matrix(rows, cols, source_of):
    row = lax.broadcasted_iota(jnp.int32, (rows, cols), 0)
    col = lax.broadcasted_iota(jnp.int32, (rows, cols), 1)
    return jnp.where(col == source_of(row), 1.0, 0.0).astype(BF16)


def nt_dot(left, right):
    return lax.dot_general(left, right, (((1,), (1,)), ((), ())), preferred_element_type=F32)


def rim_kernel(tiles, planes, x_hbm, u_hbm, out_ref, x_ref, u_ref, pick_ref, sems):
    spots = tiles * planes
    chunk = GROUP * 6 * spots
    chunks = x_hbm.shape[0] // chunk
    copies = []
    for g in range(chunks):
        rows = pl.ds(g * chunk, chunk)
        copies.append(pltpu.make_async_copy(x_hbm.at[rows], x_ref.at[rows], sems.at[g]))
    copies.append(pltpu.make_async_copy(u_hbm, u_ref, sems.at[chunks]))
    for copy in copies:
        copy.start()

    def source(row):
        return (row & (GROUP - 1)) * spots + (row // GROUP) * planes

    pick_ref[...] = pick_matrix(tiles * GROUP, GROUP * spots, source)
    chosen = pick_ref[...]
    for g in range(chunks):
        copies[g].wait()
        block = x_ref[g * chunk : (g + 1) * chunk, :].reshape(GROUP, 6, spots, LANES)
        for part in range(0, 6, 2):
            rows = jnp.concatenate(
                [block[:, part + k].reshape(GROUP * spots, LANES) for k in range(2)], axis=1
            )
            taken = jnp.dot(chosen, rows, preferred_element_type=F32).astype(BF16)
            for k in range(2):
                for tile in range(tiles):
                    out_ref[(part + k) * tiles + tile, g * GROUP : (g + 1) * GROUP] = taken[
                        tile * GROUP : (tile + 1) * GROUP, k * LANES : (k + 1) * LANES
                    ]
    copies[chunks].wait()


def rim_plane(x, u, count, tiles, planes):
    spots = tiles * planes
    return pl.pallas_call(
        partial(rim_kernel, tiles, planes),
        in_specs=[pl.BlockSpec(memory_space=pltpu.HBM)] * 2,
        out_specs=[vspec()] * 3,
        out_shape=[
            jax.ShapeDtypeStruct((6 * tiles, count, LANES), BF16),
            jax.ShapeDtypeStruct(x.shape, BF16),
            jax.ShapeDtypeStruct(u.shape, F32),
        ],
        scratch_shapes=[
            VMEM((tiles * GROUP, GROUP * spots), BF16),
            pltpu.SemaphoreType.DMA((count // GROUP + 1,)),
        ],
        compiler_params=limit(8),
        cost_estimate=cost(10**8, 4 * 10**6),
        name="rim",
    )(x, u)


def link_product(links, vec_re, vec_im):
    plus = [vec_re[c] + vec_im[c] for c in range(3)]
    outs_re, outs_im = [], []
    for row in range(3):
        link_re, link_less, link_more = links[0][row], links[1][row], links[2][row]
        one = link_re[0] * plus[0] + link_re[1] * plus[1] + link_re[2] * plus[2]
        two = link_less[0] * vec_re[0] + link_less[1] * vec_re[1] + link_less[2] * vec_re[2]
        three = link_more[0] * vec_im[0] + link_more[1] * vec_im[1] + link_more[2] * vec_im[2]
        outs_re.append(one - three)
        outs_im.append(one + two)
    return outs_re, outs_im


def load_links(u_ref, direction, spot, spots):
    def one(part, row, col):
        at = (((direction * 2 + part) * 3 + row) * 3 + col) * spots + spot
        return jnp.broadcast_to(u_ref[pl.ds(at, 1), :], (8, LANES))

    grid = [[[one(part, row, col) for col in range(3)] for row in range(3)] for part in range(2)]
    less = [[grid[1][row][col] - grid[0][row][col] for col in range(3)] for row in range(3)]
    more = [[grid[1][row][col] + grid[0][row][col] for col in range(3)] for row in range(3)]
    return grid[0], less, more


def paired(grid, count):
    real = grid[:count, :count] + grid[count:, count:]
    imag = grid[count:, :count] - grid[:count, count:]
    return real, imag


def anti(real, imag):
    return 0.5 * (real.T - real), 0.5 * (imag.T + imag)


def gram_kernel(
    count, tiles, planes, lx,
    x_ref, u_ref, phase_ref, sums_ref, rim_lhs_ref,
    v_ref, lhs_ref, op_ref, acc_ref, g_ref, pick_ref,
):
    spots = tiles * planes
    pair = 2
    halves = tiles // pair
    steps = planes * halves

    def source(row):
        spot = row // GROUP
        return (row & (GROUP - 1)) * spots + (spot % tiles) * planes + spot // tiles

    pick_ref[...] = pick_matrix(GROUP * spots, GROUP * spots, source)
    acc_ref[...] = jnp.zeros_like(acc_ref)
    g_ref[...] = jnp.zeros_like(g_ref)

    chosen = pick_ref[...]
    for at in range(0, count, GROUP):
        block = x_ref[at * 6 * spots : (at + GROUP) * 6 * spots, :].reshape(GROUP, 6, spots, LANES)
        for first in range(0, 6, 2):
            rows = jnp.concatenate(
                [block[:, first + k].reshape(GROUP * spots, LANES) for k in range(2)], axis=1
            )
            taken = jnp.dot(chosen, rows, preferred_element_type=F32)
            for k in range(2):
                part = first + k
                half, colour = part // 3, part % 3
                for spot in range(spots):
                    piece = taken[spot * GROUP : (spot + 1) * GROUP, k * LANES : (k + 1) * LANES]
                    v_ref[spot * 6 + part, at : at + GROUP, :] = piece
                    plane, tile = spot // tiles, spot % tiles
                    lhs_ref[
                        plane * halves + tile // pair,
                        half * count + at : half * count + at + GROUP,
                        ((tile % pair) * 3 + colour) * LANES : ((tile % pair) * 3 + colour + 1) * LANES,
                    ] = piece.astype(BF16)

    lane = lax.broadcasted_iota(jnp.int32, (8, LANES), 1)
    wraps = (lane & (LZ - 1)) == LZ - 1
    spills = lane < LZ

    def elementwise(step, slot, directions):
        plane = step // halves
        half_tile = step % halves
        for sub in range(pair):
            tile = half_tile * pair + sub
            spot = plane * tiles + tile
            next_tile = plane * tiles + (tile + 1) % tiles
            for direction in directions:
                links = load_links(u_ref, direction, tile * planes + plane, spots)
                for at in range(0, count, 8):

                    def part(where, k):
                        return v_ref[where * 6 + k, at : at + 8, :]

                    if direction == 0:
                        vec = [part(spot + tiles, k) for k in range(6)]
                    elif direction == 1:
                        vec = [
                            pltpu.roll(jnp.where(spills, part(next_tile, k), part(spot, k)), LANES - LZ, 1)
                            for k in range(6)
                        ]
                    else:
                        vec = [
                            jnp.where(
                                wraps,
                                pltpu.roll(part(spot, k), LZ - 1, 1),
                                pltpu.roll(part(spot, k), LANES - 1, 1),
                            )
                            for k in range(6)
                        ]
                    outs = link_product(links, vec[:3], vec[3:])
                    for half in range(2):
                        row = (direction * 2 + half) * count + at
                        for colour in range(3):
                            column = (sub * 3 + colour) * LANES
                            op_ref[slot, row : row + 8, column : column + LANES] = outs[half][colour].astype(
                                BF16
                            )

    def multiply(step, slot, directions):
        fixed = lhs_ref[step]
        g_ref[step // halves] += nt_dot(fixed, fixed)
        low = min(directions) * 2 * count
        high = (max(directions) + 1) * 2 * count
        acc_ref[low:high, :] += nt_dot(op_ref[slot, low:high, :], fixed)

    every, side = (0, 1, 2), (1, 2)
    inner = steps - halves
    elementwise(0, 0, every)

    def body(step, carry):
        slot = step & 1
        multiply(step - 1, 1 - slot, every)
        elementwise(step, slot, every)
        return carry

    lax.fori_loop(1, inner, body, 0)
    multiply(inner - 1, (inner - 1) & 1, every)
    for step in range(inner, steps):
        elementwise(step, step & 1, side)
        multiply(step, step & 1, side)

    first = lax.axis_index("space") * planes
    total_re = jnp.zeros((count, count), F32)
    total_im = jnp.zeros((count, count), F32)
    for plane in range(planes):
        real, imag = paired(g_ref[plane], count)
        cosine = phase_ref[first + plane]
        sine = phase_ref[lx + first + plane]
        total_re += cosine * real - sine * imag
        total_im += cosine * imag + sine * real
    sums_ref[0, 0] = total_re
    sums_ref[0, 1] = -total_im
    for direction in range(3):
        grid = acc_ref[direction * 2 * count : (direction + 1) * 2 * count, :]
        real, imag = anti(*paired(grid, count))
        sums_ref[direction + 1, 0] = real
        sums_ref[direction + 1, 1] = imag
    for half in range(halves):
        rim_lhs_ref[half] = lhs_ref[(planes - 1) * halves + half]


def gram(x, u, phases, count, tiles, planes, lx):
    spots = tiles * planes
    pair = 2
    steps = planes * (tiles // pair)
    wide = pair * 3 * LANES
    return pl.pallas_call(
        partial(gram_kernel, count, tiles, planes, lx),
        in_specs=[vspec(), vspec(), sspec()],
        out_specs=[vspec(), vspec()],
        out_shape=[
            jax.ShapeDtypeStruct((OPS, 2, count, count), F32),
            jax.ShapeDtypeStruct((tiles // pair, 2 * count, wide), BF16),
        ],
        scratch_shapes=[
            VMEM((spots * 6, count, LANES), F32),
            VMEM((steps, 2 * count, wide), BF16),
            VMEM((2, 6 * count, wide), BF16),
            VMEM((6 * count, 2 * count), F32),
            VMEM((planes, 2 * count, 2 * count), F32),
            VMEM((GROUP * spots, GROUP * spots), BF16),
        ],
        compiler_params=limit(26),
        cost_estimate=cost(8 * 10**9, 5 * 10**6),
        name="gram",
    )(x, u, phases)


def edge_kernel(
    count, tiles, planes, rows, cores, halo_ref, lhs_ref, u_ref, sums_ref, keep_ref, send_ref, op_ref, tot_ref
):
    spots = tiles * planes
    pair = 2
    total = None
    for half_tile in range(tiles // pair):
        for sub in range(pair):
            tile = half_tile * pair + sub
            links = load_links(u_ref, 0, tile * planes + planes - 1, spots)
            for at in range(0, count, GROUP):
                parts = [halo_ref[k * tiles + tile, at : at + GROUP, :].astype(F32) for k in range(6)]
                outs = [
                    link_product(
                        links,
                        [part[eight : eight + 8] for part in parts[:3]],
                        [part[eight : eight + 8] for part in parts[3:]],
                    )
                    for eight in (0, 8)
                ]
                for half in range(2):
                    for colour in range(3):
                        column = (sub * 3 + colour) * LANES
                        both = jnp.concatenate([outs[0][half][colour], outs[1][half][colour]], axis=0)
                        op_ref[
                            half_tile, half * count + at : half * count + at + GROUP, column : column + LANES
                        ] = both.astype(BF16)
        got = nt_dot(op_ref[half_tile], lhs_ref[half_tile])
        total = got if total is None else total + got
    real, imag = anti(*paired(total, count))
    tot_ref[0] = real
    tot_ref[1] = imag
    mine = lax.axis_index("space") & (cores - 1)
    for chip in range(count // (rows * cores)):
        for which, ref in ((mine, keep_ref), (1 - mine, send_ref)):
            at = pl.multiple_of((chip * cores + which) * rows, rows)
            for op in range(OPS):
                for half in range(2):
                    piece = sums_ref[op, half, pl.ds(at, rows), :]
                    if op == 1:
                        piece = piece + tot_ref[half, pl.ds(at, rows), :]
                    ref[chip, op, half] = piece


def edge(halo, rim_lhs, u, sums, count, tiles, planes, rows, cores):
    pair = 2
    shape = jax.ShapeDtypeStruct((count // (rows * cores), OPS, 2, rows, count), F32)
    return pl.pallas_call(
        partial(edge_kernel, count, tiles, planes, rows, cores),
        in_specs=[vspec()] * 4,
        out_specs=[vspec(), vspec()],
        out_shape=[shape, shape],
        scratch_shapes=[
            VMEM((tiles // pair, 2 * count, pair * 3 * LANES), BF16),
            VMEM((2, count, count), F32),
        ],
        compiler_params=limit(8),
        cost_estimate=cost(10**9, 3 * 10**6),
        name="edge",
    )(halo, rim_lhs, u, sums)


def fold_kernel(chips, keep_ref, got_ref, own_ref, *out_refs):
    me = lax.axis_index("space") // 2
    own_ref[...] = keep_ref[me] + got_ref[me]
    for step in range(1, chips):
        to = me ^ step
        out_refs[step - 1][...] = keep_ref[to] + got_ref[to]


def fold(keep, got):
    chips = keep.shape[0]
    shape = jax.ShapeDtypeStruct(keep.shape[1:], F32)
    return pl.pallas_call(
        partial(fold_kernel, chips),
        in_specs=[vspec()] * 2,
        out_specs=[vspec()] * chips,
        out_shape=[shape] * chips,
        compiler_params=limit(4),
        cost_estimate=cost(10**6, 10**6),
        name="fold",
    )(keep, got)


def total_kernel(*refs):
    total = refs[0][...]
    for ref in refs[1:-1]:
        total = total + ref[...]
    refs[-1][...] = total.astype(BF16)


def total_rows(parts):
    return pl.pallas_call(
        total_kernel,
        in_specs=[vspec()] * len(parts),
        out_specs=vspec(),
        out_shape=jax.ShapeDtypeStruct(parts[0].shape, BF16),
        compiler_params=limit(4),
        cost_estimate=cost(10**6, 10**6),
        name="total",
    )(*parts)


def table_kernel(groups, slots, empty, owner_ref, elem_ref, source_ref, spin_ref, table_ref):
    me = lax.axis_index("tm")
    jobs = owner_ref.shape[0] // groups
    for at in range(groups * slots):
        table_ref[at] = empty
    for group in range(groups):
        used = jnp.int32(0)
        for at in range(group * jobs, (group + 1) * jobs):
            mine = owner_ref[at] == me
            product = source_ref[at] * (SPIN * groups * OPS) + spin_ref[at] * (groups * OPS) + elem_ref[at]
            table_ref[jnp.where(mine, group * slots + used, groups * slots)] = product + group * OPS
            used = used + jnp.where(mine, 1, 0)


def job_table(tables, groups, slots, empty):
    return pl.pallas_call(
        partial(table_kernel, groups, slots, empty),
        in_specs=[sspec()] * 4,
        out_specs=sspec(),
        out_shape=jax.ShapeDtypeStruct((groups * slots + 1,), jnp.int32),
        compiler_params=limit(1),
        cost_estimate=cost(10**5, 10**4),
        name="table",
    )(*tables)


def dress_kernel(groups, slots, taus, rows, count, table_ref, per_ref, *refs):
    slab_refs = refs[:groups]
    out_ref, lhs_ref, prod_ref = refs[groups:]
    me = lax.axis_index("tm")
    for step in range(groups):
        group = me ^ step
        for op in range(OPS):
            at = pl.multiple_of((group * OPS + op) * rows, rows)
            lhs_ref[pl.ds(at, rows), 0:count] = slab_refs[step][op, 0]
            lhs_ref[pl.ds(at, rows), count : 2 * count] = slab_refs[step][op, 1]
    left = lhs_ref[...]
    for tau in range(taus):
        real, imag = per_ref[tau, 0], per_ref[tau, 1]
        right = jnp.concatenate(
            [jnp.concatenate([real, imag], axis=1), jnp.concatenate([-imag, real], axis=1)], axis=0
        )
        got = jnp.dot(left, right, preferred_element_type=F32).astype(BF16)
        for piece in range(groups * OPS):
            prod_ref[tau * groups * OPS + piece] = got[piece * rows : (piece + 1) * rows]
    prod_ref[taus * groups * OPS] = jnp.zeros((rows, 2 * count), BF16)
    for group in range(groups):
        for slot in range(slots):
            piece = prod_ref[table_ref[group * slots + slot]]
            out_ref[group, slot, 0] = piece[:, :count]
            out_ref[group, slot, 1] = piece[:, count:]


def dress(table, per, slabs, groups, slots, rows, count):
    taus = per.shape[0]
    return pl.pallas_call(
        partial(dress_kernel, groups, slots, taus, rows, count),
        in_specs=[sspec(), vspec()] + [vspec()] * groups,
        out_specs=vspec(),
        out_shape=jax.ShapeDtypeStruct((groups, slots, 2, rows, count), BF16),
        scratch_shapes=[
            VMEM((groups * OPS * rows, 2 * count), BF16),
            VMEM((taus * groups * OPS + 1, rows, 2 * count), BF16),
        ],
        compiler_params=limit(8),
        cost_estimate=cost(10**9, 2 * 10**6),
        name="dress",
    )(table, per, *slabs)


def fast_shards(eigvecs, gauge_links, perambulator, job_owner, job_elemental, job_source, job_spin):
    count = eigvecs.shape[1]
    planes, sites = eigvecs.shape[4], eigvecs.shape[5]
    tiles = sites // LANES
    space_size = lax.axis_size("space")
    groups = lax.axis_size("tm")
    lx = planes * space_size
    rows = count // space_size
    slots = 3 * ((JOB_DEV + groups - 1) // groups)
    cores = 2

    def tiled(field):
        head = field.shape[:-2]
        order = tuple(range(len(head))) + (len(head) + 1, len(head), len(head) + 2)
        split = field.reshape(head + (planes, tiles, LANES))
        return split.transpose(order).reshape(-1, LANES)

    x = tiled(eigvecs)
    u = tiled(gauge_links)
    angle = 2.0 * math.pi / lx * np.arange(lx)
    phases = jnp.asarray(np.concatenate([np.cos(angle), np.sin(angle)]).astype(np.float32))

    per = perambulator.reshape(-1, 2, count, count)
    empty = per.shape[0] * groups * OPS
    x = pltpu.with_memory_space_constraint(x, pltpu.HBM)
    u = pltpu.with_memory_space_constraint(u, pltpu.HBM)
    rim, x, u = rim_plane(x, u, count, tiles, planes)
    halo = lax.ppermute(rim, "space", [(i, (i - 1) % space_size) for i in range(space_size)])
    tables = (job_owner.reshape(-1), job_elemental, job_source, job_spin)
    table = job_table(tables, groups, slots, empty)
    sums, rim_lhs = gram(x, u, phases, count, tiles, planes, lx)
    keep, send = edge(halo, rim_lhs, u, sums, count, tiles, planes, rows, cores)
    got = lax.ppermute(send, "space", [(i, i ^ 1) for i in range(space_size)])
    parts = fold(keep, got)
    summed = [parts[0]]
    for step in range(1, space_size // cores):
        summed.append(
            lax.ppermute(parts[step], "space", [(i, i ^ (step * cores)) for i in range(space_size)])
        )
    own = total_rows(summed)
    slabs = [own]
    for step in range(1, groups):
        slabs.append(lax.ppermute(own, "tm", [(i, i ^ step) for i in range(groups)]))
    return dress(table, per, slabs, groups, slots, rows, count)[None]


def passed_along(shard, axis, by):
    count = lax.axis_size(axis)
    return lax.ppermute(shard, axis, [(i, (i + by) % count) for i in range(count)])


def shifted_sites(lattice_field, direction, offset):
    shaped = lattice_field.reshape(lattice_field.shape[:-1] + (LY, LZ))
    rolled = jnp.roll(shaped, -offset, axis=direction - 4)
    return rolled.reshape(lattice_field.shape)


def apply_link(link_field, vectors):
    total_re = None
    total_im = None
    for colour in range(3):
        link_re = link_field[0, :, colour][None]
        link_im = link_field[1, :, colour][None]
        vector_re = vectors[:, 0, colour][:, None]
        vector_im = vectors[:, 1, colour][:, None]
        part_re = link_re * vector_re - link_im * vector_im
        part_im = link_re * vector_im + link_im * vector_re
        if colour == 0:
            total_re, total_im = (part_re, part_im)
        else:
            total_re = total_re + part_re
            total_im = total_im + part_im
    return jnp.stack([total_re, total_im], axis=1)


def stacked_form(vectors):
    vector_count = vectors.shape[0]
    swapped = jnp.concatenate([-vectors[:, 1:2], vectors[:, 0:1]], axis=1)
    return jnp.concatenate(
        [vectors.reshape(vector_count, -1), swapped.reshape(vector_count, -1)], axis=0
    )


def paired_gram(stacked, lattice_field):
    vector_count = lattice_field.shape[0]
    flat_field = lattice_field.astype(jnp.bfloat16).reshape(vector_count, -1)
    product = lax.dot_general(
        stacked, flat_field, (((1,), (1,)), ((), ())), preferred_element_type=jnp.float32
    )
    return product.reshape(2, vector_count, vector_count)


def twisted_field(vectors, xcoord):
    phase_angle = 2.0 * math.pi / (vectors.shape[3] * lax.axis_size("space")) * xcoord
    cosine = jnp.cos(phase_angle)[:, None]
    sine_part = jnp.sin(phase_angle)[:, None]
    real_part = cosine * vectors[:, 0] + sine_part * vectors[:, 1]
    imag_part = cosine * vectors[:, 1] - sine_part * vectors[:, 0]
    return jnp.stack([real_part, imag_part], axis=1)


def antihermitian(paired):
    return 0.5 * jnp.stack([paired[0] - paired[0].T, paired[1] + paired[1].T], axis=0)


def plain_shards(eigvecs, gauge_links, perambulator, job_owner, job_elemental, job_source, job_spin):
    slice_count = eigvecs.shape[0]
    vector_count = eigvecs.shape[1]
    planes = eigvecs.shape[4]
    space_size = lax.axis_size("space")
    group_count = lax.axis_size("tm")
    row_count = vector_count // space_size
    capacity = 3 * ((JOB_DEV + group_count - 1) // group_count)
    xcoord = (lax.axis_index("space") * planes + jnp.arange(planes, dtype=jnp.int32)).astype(
        jnp.float32
    )
    upper_plane = passed_along(eigvecs[:, :, :, :, 0:1], "space", -1)
    low_vectors = eigvecs[0]
    vectors = low_vectors.astype(jnp.float32)
    stacked = stacked_form(low_vectors)
    results = [paired_gram(stacked, twisted_field(vectors, xcoord))]
    for direction in (1, 2, 3):
        link_field = gauge_links[0, direction - 1]
        if direction == 1:
            upper_rim = upper_plane[0].astype(jnp.float32)
            above_field = jnp.concatenate([vectors[:, :, :, 1:], upper_rim], axis=3)
        else:
            above_field = shifted_sites(vectors, direction, 1)
        forward = apply_link(link_field, above_field)
        results.append(antihermitian(paired_gram(stacked, forward)))
    partial_list = [jnp.stack(results, axis=0)]
    partial_value = jnp.stack(partial_list, axis=0)
    summed = lax.psum(partial_value, "space")
    own_rows = lax.dynamic_slice_in_dim(summed, lax.axis_index("space") * row_count, row_count, 3)
    slab_table = own_rows.astype(jnp.bfloat16).reshape(
        slice_count * OPS, 2 * row_count * vector_count
    )
    owners = job_owner[:, 0].reshape(group_count, -1)
    elements = job_elemental.reshape(group_count, -1)
    position = jnp.arange(owners.shape[1], dtype=jnp.int32)
    earlier = position[None, :] < position[:, None]
    same_owner = owners[:, :, None] == owners[:, None, :]
    slot_rank = jnp.sum(jnp.where(same_owner & earlier[None], 1, 0), axis=2).astype(jnp.int32)
    own_group = lax.axis_index("tm")
    slot_count = group_count * capacity
    live_jobs = owners == own_group
    slot_match = live_jobs[:, None, :] & (
        slot_rank[:, None, :] == jnp.arange(capacity, dtype=jnp.int32)[None, :, None]
    )
    sender_owners = lax.dynamic_index_in_dim(owners, own_group, 0, keepdims=False)
    sender_ranks = lax.dynamic_index_in_dim(slot_rank, own_group, 0, keepdims=False)
    sender_elements = lax.dynamic_index_in_dim(elements, own_group, 0, keepdims=False)
    slot_ids = sender_owners * capacity + sender_ranks
    slot_hot = (jnp.arange(slot_count, dtype=jnp.int32)[:, None] == slot_ids[None, :]).astype(
        jnp.float32
    )
    elem_hot = (
        sender_elements[:, None] == jnp.arange(slice_count * OPS, dtype=jnp.int32)[None, :]
    ).astype(jnp.float32)
    picker = jnp.dot(slot_hot, elem_hot, precision=lax.Precision.HIGHEST).astype(jnp.bfloat16)
    outgoing = jnp.dot(picker, slab_table, preferred_element_type=jnp.float32).astype(jnp.bfloat16)
    outgoing = outgoing.reshape(group_count, capacity, 2, row_count, vector_count)
    received = lax.all_to_all(outgoing, "tm", split_axis=0, concat_axis=0, tiled=True)
    block_index = job_source.reshape(group_count, -1) * SPIN + job_spin.reshape(group_count, -1)
    tau_index = jnp.sum(jnp.where(slot_match, block_index[:, None, :], 0), axis=2)
    blocks = perambulator.reshape(-1, 2 * vector_count, vector_count)
    chosen = jnp.take(blocks, tau_index.reshape(-1), axis=0)
    slab_rows = received.reshape(slot_count, 2, row_count, vector_count)
    real_rows = jnp.concatenate([slab_rows[:, 0], -slab_rows[:, 1]], axis=-1)
    imag_rows = jnp.concatenate([slab_rows[:, 1], slab_rows[:, 0]], axis=-1)
    left_side = jnp.stack([real_rows, imag_rows], axis=1).reshape(
        slot_count, 2 * row_count, 2 * vector_count
    )
    dressed = lax.dot_general(
        left_side, chosen, (((2,), (1,)), ((0,), (0,))), preferred_element_type=jnp.float32
    )
    return dressed.astype(jnp.bfloat16).reshape(
        1, group_count, capacity, 2, row_count, vector_count
    )


def shards(*args):
    eigvecs = args[0]
    count, planes, sites = eigvecs.shape[1], eigvecs.shape[4], eigvecs.shape[5]
    space_size, groups = lax.axis_size("space"), lax.axis_size("tm")
    whole_tiles = sites % (2 * LANES) == 0 and count == LANES and planes * (sites // LANES) == GROUP
    powers = space_size & (space_size - 1) == 0 and groups & (groups - 1) == 0
    small = space_size * GROUP == count and groups <= 8
    if whole_tiles and powers and small and eigvecs.shape[0] == 1:
        return fast_shards(*args)
    return plain_shards(*args)


def solution(mesh):
    return jax.shard_map(
        shards,
        mesh=mesh,
        in_specs=(
            P("tm", None, None, None, "space", None),
            P("tm", None, None, None, None, "space", None),
            P("tm", None, None, None, None),
            P(),
            P(),
            P(),
            P(),
        ),
        out_specs=P("tm", None, None, None, "space", None),
        check_vma=False,
    )
```

```python
import math
from functools import partial

import numpy as np
import jax
import jax.numpy as jnp
from jax import lax
from jax.experimental import pallas as pl
from jax.experimental.pallas import tpu as pltpu
from jax.sharding import PartitionSpec as P

LY = 16
LZ = 32
OPS = 4
SPIN = 4
JOB_DEV = 24
LANES = 128
GROUP = 16
F32 = jnp.float32
BF16 = jnp.bfloat16
VMEM = pltpu.VMEM
SMEM = pltpu.SMEM


def vspec():
    return pl.BlockSpec(memory_space=VMEM)


def sspec():
    return pl.BlockSpec(memory_space=SMEM)


def cost(flops, moved):
    return pl.CostEstimate(flops=flops, bytes_accessed=moved, transcendentals=0)


def limit(mebibytes):
    return pltpu.CompilerParams(vmem_limit_bytes=mebibytes * 2**20)


def pick_matrix(rows, cols, source_of):
    row = lax.broadcasted_iota(jnp.int32, (rows, cols), 0)
    col = lax.broadcasted_iota(jnp.int32, (rows, cols), 1)
    return jnp.where(col == source_of(row), 1.0, 0.0).astype(BF16)


def nt_dot(left, right):
    return lax.dot_general(left, right, (((1,), (1,)), ((), ())), preferred_element_type=F32)


def rim_kernel(tiles, planes, x_hbm, u_hbm, out_ref, x_ref, u_ref, pick_ref, sems):
    spots = tiles * planes
    chunk = GROUP * 6 * spots
    chunks = x_hbm.shape[0] // chunk
    copies = []
    for g in range(chunks):
        rows = pl.ds(g * chunk, chunk)
        copies.append(pltpu.make_async_copy(x_hbm.at[rows], x_ref.at[rows], sems.at[g]))
    copies.append(pltpu.make_async_copy(u_hbm, u_ref, sems.at[chunks]))
    for copy in copies:
        copy.start()

    def source(row):
        return (row & (GROUP - 1)) * spots + (row // GROUP) * planes

    pick_ref[...] = pick_matrix(tiles * GROUP, GROUP * spots, source)
    chosen = pick_ref[...]
    for g in range(chunks):
        copies[g].wait()
        block = x_ref[g * chunk : (g + 1) * chunk, :].reshape(GROUP, 6, spots, LANES)
        for part in range(0, 6, 2):
            rows = jnp.concatenate(
                [block[:, part + k].reshape(GROUP * spots, LANES) for k in range(2)], axis=1
            )
            taken = jnp.dot(chosen, rows, preferred_element_type=F32).astype(BF16)
            for k in range(2):
                for tile in range(tiles):
                    out_ref[(part + k) * tiles + tile, g * GROUP : (g + 1) * GROUP] = taken[
                        tile * GROUP : (tile + 1) * GROUP, k * LANES : (k + 1) * LANES
                    ]
    copies[chunks].wait()


def rim_plane(x, u, count, tiles, planes):
    spots = tiles * planes
    return pl.pallas_call(
        partial(rim_kernel, tiles, planes),
        in_specs=[pl.BlockSpec(memory_space=pltpu.HBM)] * 2,
        out_specs=[vspec()] * 3,
        out_shape=[
            jax.ShapeDtypeStruct((6 * tiles, count, LANES), BF16),
            jax.ShapeDtypeStruct(x.shape, BF16),
            jax.ShapeDtypeStruct(u.shape, F32),
        ],
        scratch_shapes=[
            VMEM((tiles * GROUP, GROUP * spots), BF16),
            pltpu.SemaphoreType.DMA((count // GROUP + 1,)),
        ],
        compiler_params=limit(8),
        cost_estimate=cost(10**8, 4 * 10**6),
        name="rim",
    )(x, u)


def link_product(links, vec_re, vec_im):
    plus = [vec_re[c] + vec_im[c] for c in range(3)]
    outs_re, outs_im = [], []
    for row in range(3):
        link_re, link_less, link_more = links[0][row], links[1][row], links[2][row]
        one = link_re[0] * plus[0] + link_re[1] * plus[1] + link_re[2] * plus[2]
        two = link_less[0] * vec_re[0] + link_less[1] * vec_re[1] + link_less[2] * vec_re[2]
        three = link_more[0] * vec_im[0] + link_more[1] * vec_im[1] + link_more[2] * vec_im[2]
        outs_re.append(one - three)
        outs_im.append(one + two)
    return outs_re, outs_im


def load_links(u_ref, direction, spot, spots):
    def one(part, row, col):
        at = (((direction * 2 + part) * 3 + row) * 3 + col) * spots + spot
        return jnp.broadcast_to(u_ref[pl.ds(at, 1), :], (8, LANES))

    grid = [[[one(part, row, col) for col in range(3)] for row in range(3)] for part in range(2)]
    less = [[grid[1][row][col] - grid[0][row][col] for col in range(3)] for row in range(3)]
    more = [[grid[1][row][col] + grid[0][row][col] for col in range(3)] for row in range(3)]
    return grid[0], less, more


def fill_table(groups, slots, empty, owner_ref, elem_ref, source_ref, spin_ref, table_ref):
    total = owner_ref.shape[1]
    jobs = total // groups
    row = lax.broadcasted_iota(jnp.int32, (total, total), 0)
    col = lax.broadcasted_iota(jnp.int32, (total, total), 1)

    def group_of(index):
        return sum((index >= group * jobs).astype(jnp.int32) for group in range(1, groups))

    live = jnp.where(owner_ref[...] == lax.axis_index("tm"), 1.0, 0.0)
    product = source_ref[...] * (SPIN * groups * OPS) + spin_ref[...] * (groups * OPS) + elem_ref[...]

    def column(mask, values):
        wide = jnp.broadcast_to(values.astype(F32), (total, total))
        return jnp.sum(jnp.where(mask, wide, 0.0), axis=1, keepdims=True)

    rank = column((col < row) & (group_of(col) == group_of(row)), live)
    alive = column(col == row, live)
    value = column(col == row, product)
    at_row = lax.broadcasted_iota(jnp.int32, (total, LANES), 0)
    at_col = lax.broadcasted_iota(jnp.int32, (total, LANES), 1)
    group = group_of(at_row).astype(F32)
    place = jnp.where(alive > 0.5, group * slots + rank, -1.0)
    found = at_col.astype(F32) == place
    picked = jnp.sum(jnp.where(found, value + group * OPS - empty, 0.0), axis=0, keepdims=True)
    table_ref[...] = (picked + empty).astype(jnp.int32)


def paired(grid, count):
    real = grid[:count, :count] + grid[count:, count:]
    imag = grid[count:, :count] - grid[:count, count:]
    return real, imag


def anti(real, imag):
    return 0.5 * (real.T - real), 0.5 * (imag.T + imag)


def gram_kernel(
    count, tiles, planes, lx, groups, slots, empty,
    x_ref, u_ref, phase_ref, owner_ref, elem_ref, source_ref, spin_ref,
    sums_ref, rim_lhs_ref, table_ref,
    v_ref, lhs_ref, op_ref, acc_ref, g_ref, pick_ref,
):
    spots = tiles * planes
    pair = 2
    halves = tiles // pair
    steps = planes * halves

    def source(row):
        spot = row // GROUP
        return (row & (GROUP - 1)) * spots + (spot % tiles) * planes + spot // tiles

    pick_ref[...] = pick_matrix(GROUP * spots, GROUP * spots, source)
    acc_ref[...] = jnp.zeros_like(acc_ref)
    g_ref[...] = jnp.zeros_like(g_ref)

    chosen = pick_ref[...]
    for at in range(0, count, GROUP):
        block = x_ref[at * 6 * spots : (at + GROUP) * 6 * spots, :].reshape(GROUP, 6, spots, LANES)
        for first in range(0, 6, 2):
            rows = jnp.concatenate(
                [block[:, first + k].reshape(GROUP * spots, LANES) for k in range(2)], axis=1
            )
            taken = jnp.dot(chosen, rows, preferred_element_type=F32)
            for k in range(2):
                part = first + k
                half, colour = part // 3, part % 3
                for spot in range(spots):
                    piece = taken[spot * GROUP : (spot + 1) * GROUP, k * LANES : (k + 1) * LANES]
                    v_ref[spot * 6 + part, at : at + GROUP, :] = piece
                    plane, tile = spot // tiles, spot % tiles
                    lhs_ref[
                        plane * halves + tile // pair,
                        half * count + at : half * count + at + GROUP,
                        ((tile % pair) * 3 + colour) * LANES : ((tile % pair) * 3 + colour + 1) * LANES,
                    ] = piece.astype(BF16)

    lane = lax.broadcasted_iota(jnp.int32, (8, LANES), 1)
    wraps = (lane & (LZ - 1)) == LZ - 1
    spills = lane < LZ

    def elementwise(step, slot, directions):
        plane = step // halves
        half_tile = step % halves
        for sub in range(pair):
            tile = half_tile * pair + sub
            spot = plane * tiles + tile
            next_tile = plane * tiles + (tile + 1) % tiles
            for direction in directions:
                links = load_links(u_ref, direction, tile * planes + plane, spots)
                for at in range(0, count, 8):

                    def part(where, k):
                        return v_ref[where * 6 + k, at : at + 8, :]

                    if direction == 0:
                        vec = [part(spot + tiles, k) for k in range(6)]
                    elif direction == 1:
                        vec = [
                            pltpu.roll(jnp.where(spills, part(next_tile, k), part(spot, k)), LANES - LZ, 1)
                            for k in range(6)
                        ]
                    else:
                        vec = [
                            jnp.where(
                                wraps,
                                pltpu.roll(part(spot, k), LZ - 1, 1),
                                pltpu.roll(part(spot, k), LANES - 1, 1),
                            )
                            for k in range(6)
                        ]
                    outs = link_product(links, vec[:3], vec[3:])
                    for half in range(2):
                        row = (direction * 2 + half) * count + at
                        for colour in range(3):
                            column = (sub * 3 + colour) * LANES
                            op_ref[slot, row : row + 8, column : column + LANES] = outs[half][colour].astype(
                                BF16
                            )

    def multiply(step, slot, directions):
        fixed = lhs_ref[step]
        low = min(directions) * 2 * count
        high = (max(directions) + 1) * 2 * count
        got = nt_dot(jnp.concatenate([fixed, op_ref[slot, low:high, :]], axis=0), fixed)
        g_ref[step // halves] += got[: 2 * count]
        acc_ref[low:high, :] += got[2 * count :]

    every, side = (0, 1, 2), (1, 2)
    inner = steps - halves
    elementwise(0, 0, every)

    def body(step, carry):
        slot = step & 1
        multiply(step - 1, 1 - slot, every)
        elementwise(step, slot, every)
        return carry

    lax.fori_loop(1, inner, body, 0)
    multiply(inner - 1, (inner - 1) & 1, every)
    for step in range(inner, steps):
        elementwise(step, step & 1, side)
        multiply(step, step & 1, side)
    fill_table(groups, slots, empty, owner_ref, elem_ref, source_ref, spin_ref, table_ref)

    first = lax.axis_index("space") * planes
    total_re = jnp.zeros((count, count), F32)
    total_im = jnp.zeros((count, count), F32)
    for plane in range(planes):
        real, imag = paired(g_ref[plane], count)
        cosine = phase_ref[first + plane]
        sine = phase_ref[lx + first + plane]
        total_re += cosine * real - sine * imag
        total_im += cosine * imag + sine * real
    sums_ref[0, 0] = total_re
    sums_ref[0, 1] = -total_im
    for direction in range(3):
        grid = acc_ref[direction * 2 * count : (direction + 1) * 2 * count, :]
        real, imag = anti(*paired(grid, count))
        sums_ref[direction + 1, 0] = real
        sums_ref[direction + 1, 1] = imag
    for half in range(halves):
        rim_lhs_ref[half] = lhs_ref[(planes - 1) * halves + half]


def gram(x, u, phases, tables, count, tiles, planes, lx, groups, slots, empty):
    spots = tiles * planes
    pair = 2
    steps = planes * (tiles // pair)
    wide = pair * 3 * LANES
    return pl.pallas_call(
        partial(gram_kernel, count, tiles, planes, lx, groups, slots, empty),
        in_specs=[vspec()] * 2 + [sspec()] + [vspec()] * 4,
        out_specs=[vspec()] * 3,
        out_shape=[
            jax.ShapeDtypeStruct((OPS, 2, count, count), F32),
            jax.ShapeDtypeStruct((tiles // pair, 2 * count, wide), BF16),
            jax.ShapeDtypeStruct((1, LANES), jnp.int32),
        ],
        scratch_shapes=[
            VMEM((spots * 6, count, LANES), F32),
            VMEM((steps, 2 * count, wide), BF16),
            VMEM((2, 6 * count, wide), BF16),
            VMEM((6 * count, 2 * count), F32),
            VMEM((planes, 2 * count, 2 * count), F32),
            VMEM((GROUP * spots, GROUP * spots), BF16),
        ],
        compiler_params=limit(26),
        cost_estimate=cost(8 * 10**9, 5 * 10**6),
        name="gram",
    )(x, u, phases, *tables)


def edge_kernel(
    count, tiles, planes, rows, cores, halo_ref, lhs_ref, u_ref, sums_ref, keep_ref, send_ref, op_ref, tot_ref
):
    spots = tiles * planes
    pair = 2
    total = None
    for half_tile in range(tiles // pair):
        for sub in range(pair):
            tile = half_tile * pair + sub
            links = load_links(u_ref, 0, tile * planes + planes - 1, spots)
            for at in range(0, count, GROUP):
                parts = [halo_ref[k * tiles + tile, at : at + GROUP, :].astype(F32) for k in range(6)]
                outs = [
                    link_product(
                        links,
                        [part[eight : eight + 8] for part in parts[:3]],
                        [part[eight : eight + 8] for part in parts[3:]],
                    )
                    for eight in (0, 8)
                ]
                for half in range(2):
                    for colour in range(3):
                        column = (sub * 3 + colour) * LANES
                        both = jnp.concatenate([outs[0][half][colour], outs[1][half][colour]], axis=0)
                        op_ref[
                            half_tile, half * count + at : half * count + at + GROUP, column : column + LANES
                        ] = both.astype(BF16)
        got = nt_dot(op_ref[half_tile], lhs_ref[half_tile])
        total = got if total is None else total + got
    real, imag = anti(*paired(total, count))
    tot_ref[0] = real
    tot_ref[1] = imag
    mine = lax.axis_index("space") & (cores - 1)
    for chip in range(count // (rows * cores)):
        for which, ref in ((mine, keep_ref), (1 - mine, send_ref)):
            at = pl.multiple_of((chip * cores + which) * rows, rows)
            for op in range(OPS):
                for half in range(2):
                    piece = sums_ref[op, half, pl.ds(at, rows), :]
                    if op == 1:
                        piece = piece + tot_ref[half, pl.ds(at, rows), :]
                    ref[chip, op, half] = piece


def edge(halo, rim_lhs, u, sums, count, tiles, planes, rows, cores):
    pair = 2
    shape = jax.ShapeDtypeStruct((count // (rows * cores), OPS, 2, rows, count), F32)
    return pl.pallas_call(
        partial(edge_kernel, count, tiles, planes, rows, cores),
        in_specs=[vspec()] * 4,
        out_specs=[vspec(), vspec()],
        out_shape=[shape, shape],
        scratch_shapes=[
            VMEM((tiles // pair, 2 * count, pair * 3 * LANES), BF16),
            VMEM((2, count, count), F32),
        ],
        compiler_params=limit(8),
        cost_estimate=cost(10**9, 3 * 10**6),
        name="edge",
    )(halo, rim_lhs, u, sums)


def split_sum(block):
    high = block[0:1].astype(BF16)
    low = (block[0:1] - high.astype(F32)).astype(BF16)
    return jnp.concatenate([high, low, block[1:].astype(BF16)], axis=0)


def fold_kernel(chips, cores, keep_ref, got_ref, own_ref, *out_refs):
    me = lax.axis_index("space") // cores
    own_ref[...] = keep_ref[me] + got_ref[me]
    for step in range(1, chips):
        to = me ^ step
        out_refs[step - 1][...] = split_sum(keep_ref[to] + got_ref[to])


def fold(keep, got, cores):
    chips = keep.shape[0]
    shape = keep.shape[1:]
    sent = jax.ShapeDtypeStruct((shape[0] + 1,) + shape[1:], BF16)
    return pl.pallas_call(
        partial(fold_kernel, chips, cores),
        in_specs=[vspec()] * 2,
        out_specs=[vspec()] * chips,
        out_shape=[jax.ShapeDtypeStruct(shape, F32)] + [sent] * (chips - 1),
        compiler_params=limit(4),
        cost_estimate=cost(10**6, 10**6),
        name="fold",
    )(keep, got)


def total_kernel(own_ref, *refs):
    total_ref = refs[-1]
    first = own_ref[0:1]
    rest = own_ref[1:]
    for ref in refs[:-1]:
        first = first + (ref[0:1].astype(F32) + ref[1:2].astype(F32))
        rest = rest + ref[2:].astype(F32)
    total_ref[0:1] = first.astype(BF16)
    total_ref[1:] = rest.astype(BF16)


def total_rows(parts):
    return pl.pallas_call(
        total_kernel,
        in_specs=[vspec()] * len(parts),
        out_specs=vspec(),
        out_shape=jax.ShapeDtypeStruct(parts[0].shape, BF16),
        compiler_params=limit(4),
        cost_estimate=cost(10**6, 10**6),
        name="total",
    )(*parts)


def dress_kernel(groups, slots, taus, rows, count, table_ref, per_ref, *refs):
    slab_refs = refs[:groups]
    out_ref, lhs_ref, prod_ref = refs[groups:]
    me = lax.axis_index("tm")
    for step in range(groups):
        group = me ^ step
        for op in range(OPS):
            at = pl.multiple_of((group * OPS + op) * rows, rows)
            lhs_ref[pl.ds(at, rows), 0:count] = slab_refs[step][op, 0]
            lhs_ref[pl.ds(at, rows), count : 2 * count] = slab_refs[step][op, 1]
    left = lhs_ref[...]
    for tau in range(taus):
        real, imag = per_ref[tau, 0], per_ref[tau, 1]
        right = jnp.concatenate(
            [jnp.concatenate([real, imag], axis=1), jnp.concatenate([-imag, real], axis=1)], axis=0
        )
        got = jnp.dot(left, right, preferred_element_type=F32).astype(BF16)
        for piece in range(groups * OPS):
            prod_ref[tau * groups * OPS + piece] = got[piece * rows : (piece + 1) * rows]
    prod_ref[taus * groups * OPS] = jnp.zeros((rows, 2 * count), BF16)
    for group in range(groups):
        for slot in range(slots):
            piece = prod_ref[table_ref[0, group * slots + slot]]
            out_ref[group, slot, 0] = piece[:, :count]
            out_ref[group, slot, 1] = piece[:, count:]


def dress(table, per, slabs, groups, slots, rows, count):
    taus = per.shape[0]
    return pl.pallas_call(
        partial(dress_kernel, groups, slots, taus, rows, count),
        in_specs=[sspec(), vspec()] + [vspec()] * groups,
        out_specs=vspec(),
        out_shape=jax.ShapeDtypeStruct((groups, slots, 2, rows, count), BF16),
        scratch_shapes=[
            VMEM((groups * OPS * rows, 2 * count), BF16),
            VMEM((taus * groups * OPS + 1, rows, 2 * count), BF16),
        ],
        compiler_params=limit(8),
        cost_estimate=cost(10**9, 2 * 10**6),
        name="dress",
    )(table, per, *slabs)


def fast_shards(eigvecs, gauge_links, perambulator, job_owner, job_elemental, job_source, job_spin):
    count = eigvecs.shape[1]
    planes, sites = eigvecs.shape[4], eigvecs.shape[5]
    tiles = sites // LANES
    space_size = lax.axis_size("space")
    groups = lax.axis_size("tm")
    lx = planes * space_size
    rows = count // space_size
    slots = 3 * ((JOB_DEV + groups - 1) // groups)
    cores = 2

    def tiled(field):
        head = field.shape[:-2]
        order = tuple(range(len(head))) + (len(head) + 1, len(head), len(head) + 2)
        split = field.reshape(head + (planes, tiles, LANES))
        return split.transpose(order).reshape(-1, LANES)

    x = tiled(eigvecs)
    u = tiled(gauge_links)
    angle = 2.0 * math.pi / lx * np.arange(lx)
    phases = jnp.asarray(np.concatenate([np.cos(angle), np.sin(angle)]).astype(np.float32))

    per = perambulator.reshape(-1, 2, count, count)
    empty = per.shape[0] * groups * OPS
    x = pltpu.with_memory_space_constraint(x, pltpu.HBM)
    u = pltpu.with_memory_space_constraint(u, pltpu.HBM)
    rim, x, u = rim_plane(x, u, count, tiles, planes)
    halo = lax.ppermute(rim, "space", [(i, (i - 1) % space_size) for i in range(space_size)])
    tables = [job.reshape(1, -1) for job in (job_owner, job_elemental, job_source, job_spin)]
    sums, rim_lhs, table = gram(
        x, u, phases, tables, count, tiles, planes, lx, groups, slots, empty
    )
    keep, send = edge(halo, rim_lhs, u, sums, count, tiles, planes, rows, cores)
    got = lax.ppermute(send, "space", [(i, i ^ 1) for i in range(space_size)])
    parts = fold(keep, got, cores)
    summed = [parts[0]]
    for step in range(1, space_size // cores):
        summed.append(
            lax.ppermute(parts[step], "space", [(i, i ^ (step * cores)) for i in range(space_size)])
        )
    own = total_rows(summed)
    slabs = [own]
    for step in range(1, groups):
        slabs.append(lax.ppermute(own, "tm", [(i, i ^ step) for i in range(groups)]))
    return dress(table, per, slabs, groups, slots, rows, count)[None]


def passed_along(shard, axis, by):
    count = lax.axis_size(axis)
    return lax.ppermute(shard, axis, [(i, (i + by) % count) for i in range(count)])


def shifted_sites(lattice_field, direction, offset):
    shaped = lattice_field.reshape(lattice_field.shape[:-1] + (LY, LZ))
    rolled = jnp.roll(shaped, -offset, axis=direction - 4)
    return rolled.reshape(lattice_field.shape)


def apply_link(link_field, vectors):
    total_re = None
    total_im = None
    for colour in range(3):
        link_re = link_field[0, :, colour][None]
        link_im = link_field[1, :, colour][None]
        vector_re = vectors[:, 0, colour][:, None]
        vector_im = vectors[:, 1, colour][:, None]
        part_re = link_re * vector_re - link_im * vector_im
        part_im = link_re * vector_im + link_im * vector_re
        if colour == 0:
            total_re, total_im = (part_re, part_im)
        else:
            total_re = total_re + part_re
            total_im = total_im + part_im
    return jnp.stack([total_re, total_im], axis=1)


def stacked_form(vectors):
    vector_count = vectors.shape[0]
    swapped = jnp.concatenate([-vectors[:, 1:2], vectors[:, 0:1]], axis=1)
    return jnp.concatenate(
        [vectors.reshape(vector_count, -1), swapped.reshape(vector_count, -1)], axis=0
    )


def paired_gram(stacked, lattice_field):
    vector_count = lattice_field.shape[0]
    flat_field = lattice_field.astype(jnp.bfloat16).reshape(vector_count, -1)
    product = lax.dot_general(
        stacked, flat_field, (((1,), (1,)), ((), ())), preferred_element_type=jnp.float32
    )
    return product.reshape(2, vector_count, vector_count)


def twisted_field(vectors, xcoord):
    phase_angle = 2.0 * math.pi / (vectors.shape[3] * lax.axis_size("space")) * xcoord
    cosine = jnp.cos(phase_angle)[:, None]
    sine_part = jnp.sin(phase_angle)[:, None]
    real_part = cosine * vectors[:, 0] + sine_part * vectors[:, 1]
    imag_part = cosine * vectors[:, 1] - sine_part * vectors[:, 0]
    return jnp.stack([real_part, imag_part], axis=1)


def antihermitian(paired):
    return 0.5 * jnp.stack([paired[0] - paired[0].T, paired[1] + paired[1].T], axis=0)


def plain_shards(eigvecs, gauge_links, perambulator, job_owner, job_elemental, job_source, job_spin):
    slice_count = eigvecs.shape[0]
    vector_count = eigvecs.shape[1]
    planes = eigvecs.shape[4]
    space_size = lax.axis_size("space")
    group_count = lax.axis_size("tm")
    row_count = vector_count // space_size
    capacity = 3 * ((JOB_DEV + group_count - 1) // group_count)
    xcoord = (lax.axis_index("space") * planes + jnp.arange(planes, dtype=jnp.int32)).astype(
        jnp.float32
    )
    upper_plane = passed_along(eigvecs[:, :, :, :, 0:1], "space", -1)
    low_vectors = eigvecs[0]
    vectors = low_vectors.astype(jnp.float32)
    stacked = stacked_form(low_vectors)
    results = [paired_gram(stacked, twisted_field(vectors, xcoord))]
    for direction in (1, 2, 3):
        link_field = gauge_links[0, direction - 1]
        if direction == 1:
            upper_rim = upper_plane[0].astype(jnp.float32)
            above_field = jnp.concatenate([vectors[:, :, :, 1:], upper_rim], axis=3)
        else:
            above_field = shifted_sites(vectors, direction, 1)
        forward = apply_link(link_field, above_field)
        results.append(antihermitian(paired_gram(stacked, forward)))
    partial_list = [jnp.stack(results, axis=0)]
    partial_value = jnp.stack(partial_list, axis=0)
    summed = lax.psum(partial_value, "space")
    own_rows = lax.dynamic_slice_in_dim(summed, lax.axis_index("space") * row_count, row_count, 3)
    slab_table = own_rows.astype(jnp.bfloat16).reshape(
        slice_count * OPS, 2 * row_count * vector_count
    )
    owners = job_owner[:, 0].reshape(group_count, -1)
    elements = job_elemental.reshape(group_count, -1)
    position = jnp.arange(owners.shape[1], dtype=jnp.int32)
    earlier = position[None, :] < position[:, None]
    same_owner = owners[:, :, None] == owners[:, None, :]
    slot_rank = jnp.sum(jnp.where(same_owner & earlier[None], 1, 0), axis=2).astype(jnp.int32)
    own_group = lax.axis_index("tm")
    slot_count = group_count * capacity
    live_jobs = owners == own_group
    slot_match = live_jobs[:, None, :] & (
        slot_rank[:, None, :] == jnp.arange(capacity, dtype=jnp.int32)[None, :, None]
    )
    sender_owners = lax.dynamic_index_in_dim(owners, own_group, 0, keepdims=False)
    sender_ranks = lax.dynamic_index_in_dim(slot_rank, own_group, 0, keepdims=False)
    sender_elements = lax.dynamic_index_in_dim(elements, own_group, 0, keepdims=False)
    slot_ids = sender_owners * capacity + sender_ranks
    slot_hot = (jnp.arange(slot_count, dtype=jnp.int32)[:, None] == slot_ids[None, :]).astype(
        jnp.float32
    )
    elem_hot = (
        sender_elements[:, None] == jnp.arange(slice_count * OPS, dtype=jnp.int32)[None, :]
    ).astype(jnp.float32)
    picker = jnp.dot(slot_hot, elem_hot, precision=lax.Precision.HIGHEST).astype(jnp.bfloat16)
    outgoing = jnp.dot(picker, slab_table, preferred_element_type=jnp.float32).astype(jnp.bfloat16)
    outgoing = outgoing.reshape(group_count, capacity, 2, row_count, vector_count)
    received = lax.all_to_all(outgoing, "tm", split_axis=0, concat_axis=0, tiled=True)
    block_index = job_source.reshape(group_count, -1) * SPIN + job_spin.reshape(group_count, -1)
    tau_index = jnp.sum(jnp.where(slot_match, block_index[:, None, :], 0), axis=2)
    blocks = perambulator.reshape(-1, 2 * vector_count, vector_count)
    chosen = jnp.take(blocks, tau_index.reshape(-1), axis=0)
    slab_rows = received.reshape(slot_count, 2, row_count, vector_count)
    real_rows = jnp.concatenate([slab_rows[:, 0], -slab_rows[:, 1]], axis=-1)
    imag_rows = jnp.concatenate([slab_rows[:, 1], slab_rows[:, 0]], axis=-1)
    left_side = jnp.stack([real_rows, imag_rows], axis=1).reshape(
        slot_count, 2 * row_count, 2 * vector_count
    )
    dressed = lax.dot_general(
        left_side, chosen, (((2,), (1,)), ((0,), (0,))), preferred_element_type=jnp.float32
    )
    return dressed.astype(jnp.bfloat16).reshape(
        1, group_count, capacity, 2, row_count, vector_count
    )


def shards(*args):
    eigvecs = args[0]
    count, planes, sites = eigvecs.shape[1], eigvecs.shape[4], eigvecs.shape[5]
    space_size, groups = lax.axis_size("space"), lax.axis_size("tm")
    whole_tiles = sites % (2 * LANES) == 0 and count == LANES and planes * (sites // LANES) == GROUP
    fits = groups * 3 * ((JOB_DEV + groups - 1) // groups) < LANES
    powers = space_size & (space_size - 1) == 0 and groups & (groups - 1) == 0
    small = space_size * GROUP == count and groups <= 8 and args[3].shape[0] <= LANES
    if whole_tiles and fits and powers and small and eigvecs.shape[0] == 1:
        return fast_shards(*args)
    return plain_shards(*args)


def solution(mesh):
    return jax.shard_map(
        shards,
        mesh=mesh,
        in_specs=(
            P("tm", None, None, None, "space", None),
            P("tm", None, None, None, None, "space", None),
            P("tm", None, None, None, None),
            P(),
            P(),
            P(),
            P(),
        ),
        out_specs=P("tm", None, None, None, "space", None),
        check_vma=False,
    )
```

```python
import math
from functools import partial

import numpy as np
import jax
import jax.numpy as jnp
from jax import lax
from jax.experimental import pallas as pl
from jax.experimental.pallas import tpu as pltpu
from jax.sharding import PartitionSpec as P

LY = 16
LZ = 32
OPS = 4
SPIN = 4
JOB_DEV = 24
LANES = 128
GROUP = 16
F32 = jnp.float32
BF16 = jnp.bfloat16
VMEM = pltpu.VMEM
SMEM = pltpu.SMEM


def vspec():
    return pl.BlockSpec(memory_space=VMEM)


def sspec():
    return pl.BlockSpec(memory_space=SMEM)


def cost(flops, moved):
    return pl.CostEstimate(flops=flops, bytes_accessed=moved, transcendentals=0)


def limit(mebibytes):
    return pltpu.CompilerParams(vmem_limit_bytes=mebibytes * 2**20)


def pick_matrix(rows, cols, source_of):
    row = lax.broadcasted_iota(jnp.int32, (rows, cols), 0)
    col = lax.broadcasted_iota(jnp.int32, (rows, cols), 1)
    return jnp.where(col == source_of(row), 1.0, 0.0).astype(BF16)


def nt_dot(left, right):
    return lax.dot_general(left, right, (((1,), (1,)), ((), ())), preferred_element_type=F32)


def chunk_copies(x_hbm, x_ref, sems, chunks):
    chunk = x_hbm.shape[0] // chunks
    copies = []
    for g in range(chunks):
        rows = pl.ds(g * chunk, chunk)
        copies.append(pltpu.make_async_copy(x_hbm.at[rows], x_ref.at[rows], sems.at[g]))
    return copies


def chunk_rows(x_ref, at, spots, first):
    block = x_ref[at * 6 * spots : (at + GROUP) * 6 * spots, :].reshape(GROUP, 6, spots, LANES)
    return jnp.concatenate([block[:, first + k].reshape(GROUP * spots, LANES) for k in range(2)], axis=1)


def rim_kernel(tiles, planes, count, cores, x_hbm, out_ref, x_ref, pick_ref, sems):
    spots = tiles * planes
    chunks = count // GROUP

    @pl.when((lax.axis_index("space") & (cores - 1)) == 0)
    def _():
        copies = chunk_copies(x_hbm, x_ref, sems, chunks)
        for copy in copies:
            copy.start()

        def source(row):
            return (row & (GROUP - 1)) * spots + (row // GROUP) * planes

        pick_ref[...] = pick_matrix(tiles * GROUP, GROUP * spots, source)
        chosen = pick_ref[...]
        for g in range(chunks):
            copies[g].wait()
            at = g * GROUP
            for part in range(0, 6, 2):
                taken = jnp.dot(chosen, chunk_rows(x_ref, at, spots, part), preferred_element_type=F32)
                taken = taken.astype(BF16)
                for k in range(2):
                    for tile in range(tiles):
                        out_ref[(part + k) * tiles + tile, at : at + GROUP] = taken[
                            tile * GROUP : (tile + 1) * GROUP, k * LANES : (k + 1) * LANES
                        ]


def rim_plane(x, count, tiles, planes, cores):
    spots = tiles * planes
    return pl.pallas_call(
        partial(rim_kernel, tiles, planes, count, cores),
        in_specs=[pl.BlockSpec(memory_space=pltpu.HBM)],
        out_specs=vspec(),
        out_shape=jax.ShapeDtypeStruct((6 * tiles, count, LANES), BF16),
        scratch_shapes=[
            VMEM(x.shape, BF16),
            VMEM((tiles * GROUP, GROUP * spots), BF16),
            pltpu.SemaphoreType.DMA((count // GROUP,)),
        ],
        compiler_params=limit(8),
        cost_estimate=cost(10**8, 4 * 10**6),
        name="rim",
    )(x)


def spread_kernel(
    tiles, planes, count, x_hbm, u_hbm, rim_hbm, v_ref, lhs_ref, out_ref, u_ref, x_ref, pick_ref, sems
):
    spots = tiles * planes
    pair = 2
    halves = tiles // pair
    chunks = count // GROUP
    copies = chunk_copies(x_hbm, x_ref, sems, chunks)
    copies.append(pltpu.make_async_copy(u_hbm, u_ref, sems.at[chunks]))
    for copy in copies:
        copy.start()

    def source(row):
        spot = row // GROUP
        return (row & (GROUP - 1)) * spots + (spot % tiles) * planes + spot // tiles

    pick_ref[...] = pick_matrix(GROUP * spots, GROUP * spots, source)
    chosen = pick_ref[...]
    for g in range(chunks):
        copies[g].wait()
        at = g * GROUP
        for first in range(0, 6, 2):
            taken = jnp.dot(chosen, chunk_rows(x_ref, at, spots, first), preferred_element_type=F32)
            for k in range(2):
                part = first + k
                half, colour = part // 3, part % 3
                for spot in range(spots):
                    piece = taken[spot * GROUP : (spot + 1) * GROUP, k * LANES : (k + 1) * LANES]
                    plane, tile = spot // tiles, spot % tiles
                    column = ((tile % pair) * 3 + colour) * LANES
                    v_ref[spot * 6 + part, at : at + GROUP, :] = piece
                    rounded = piece.astype(BF16)
                    lhs_ref[
                        plane * halves + tile // pair,
                        half * count + at : half * count + at + GROUP,
                        column : column + LANES,
                    ] = rounded
                    if plane == 0:
                        out_ref[part * tiles + tile, at : at + GROUP] = rounded
    copies[chunks].wait()


def spread(x, u, rim, count, tiles, planes):
    spots = tiles * planes
    pair = 2
    return pl.pallas_call(
        partial(spread_kernel, tiles, planes, count),
        in_specs=[pl.BlockSpec(memory_space=pltpu.HBM)] * 2 + [pl.BlockSpec(memory_space=pl.ANY)],
        out_specs=[vspec()] * 4,
        out_shape=[
            jax.ShapeDtypeStruct((spots * 6, count, LANES), F32),
            jax.ShapeDtypeStruct((planes * (tiles // pair), 2 * count, pair * 3 * LANES), BF16),
            jax.ShapeDtypeStruct((6 * tiles, count, LANES), BF16),
            jax.ShapeDtypeStruct(u.shape, F32),
        ],
        scratch_shapes=[
            VMEM(x.shape, BF16),
            VMEM((GROUP * spots, GROUP * spots), BF16),
            pltpu.SemaphoreType.DMA((count // GROUP + 1,)),
        ],
        compiler_params=limit(16),
        cost_estimate=cost(10**9, 14 * 10**6),
        name="spread",
    )(x, u, rim)


def link_product(links, vec_re, vec_im):
    plus = [vec_re[c] + vec_im[c] for c in range(3)]
    outs_re, outs_im = [], []
    for row in range(3):
        link_re, link_less, link_more = links[0][row], links[1][row], links[2][row]
        one = link_re[0] * plus[0] + link_re[1] * plus[1] + link_re[2] * plus[2]
        two = link_less[0] * vec_re[0] + link_less[1] * vec_re[1] + link_less[2] * vec_re[2]
        three = link_more[0] * vec_im[0] + link_more[1] * vec_im[1] + link_more[2] * vec_im[2]
        outs_re.append(one - three)
        outs_im.append(one + two)
    return outs_re, outs_im


def load_links(u_ref, direction, spot, spots):
    def one(part, row, col):
        at = (((direction * 2 + part) * 3 + row) * 3 + col) * spots + spot
        return jnp.broadcast_to(u_ref[pl.ds(at, 1), :], (8, LANES))

    grid = [[[one(part, row, col) for col in range(3)] for row in range(3)] for part in range(2)]
    less = [[grid[1][row][col] - grid[0][row][col] for col in range(3)] for row in range(3)]
    more = [[grid[1][row][col] + grid[0][row][col] for col in range(3)] for row in range(3)]
    return grid[0], less, more


def fill_table(groups, slots, empty, owner_ref, elem_ref, source_ref, spin_ref, table_ref):
    total = owner_ref.shape[1]
    jobs = total // groups
    row = lax.broadcasted_iota(jnp.int32, (total, total), 0)
    col = lax.broadcasted_iota(jnp.int32, (total, total), 1)

    def group_of(index):
        return sum((index >= group * jobs).astype(jnp.int32) for group in range(1, groups))

    live = jnp.where(owner_ref[...] == lax.axis_index("tm"), 1.0, 0.0)
    product = source_ref[...] * (SPIN * groups * OPS) + spin_ref[...] * (groups * OPS) + elem_ref[...]

    def column(mask, values):
        wide = jnp.broadcast_to(values.astype(F32), (total, total))
        return jnp.sum(jnp.where(mask, wide, 0.0), axis=1, keepdims=True)

    rank = column((col < row) & (group_of(col) == group_of(row)), live)
    alive = column(col == row, live)
    value = column(col == row, product)
    at_row = lax.broadcasted_iota(jnp.int32, (total, LANES), 0)
    at_col = lax.broadcasted_iota(jnp.int32, (total, LANES), 1)
    group = group_of(at_row).astype(F32)
    place = jnp.where(alive > 0.5, group * slots + rank, -1.0)
    found = at_col.astype(F32) == place
    picked = jnp.sum(jnp.where(found, value + group * OPS - empty, 0.0), axis=0, keepdims=True)
    table_ref[...] = (picked + empty).astype(jnp.int32)


def paired(grid, count):
    real = grid[:count, :count] + grid[count:, count:]
    imag = grid[count:, :count] - grid[:count, count:]
    return real, imag


def anti(real, imag):
    return 0.5 * (real.T - real), 0.5 * (imag.T + imag)


def gram_kernel(
    count, tiles, planes, lx, groups, slots, empty,
    v_ref, lhs_ref, u_ref, phase_ref, owner_ref, elem_ref, source_ref, spin_ref,
    sums_ref, table_ref,
    op_ref, acc_ref, g_ref,
):
    spots = tiles * planes
    pair = 2
    halves = tiles // pair
    steps = planes * halves
    acc_ref[...] = jnp.zeros_like(acc_ref)
    g_ref[...] = jnp.zeros_like(g_ref)
    lane = lax.broadcasted_iota(jnp.int32, (8, LANES), 1)
    wraps = (lane & (LZ - 1)) == LZ - 1
    spills = lane < LZ

    def elementwise(step, slot, directions):
        plane = step // halves
        half_tile = step % halves
        for sub in range(pair):
            tile = half_tile * pair + sub
            spot = plane * tiles + tile
            next_tile = plane * tiles + (tile + 1) % tiles
            for direction in directions:
                links = load_links(u_ref, direction, tile * planes + plane, spots)
                for at in range(0, count, 8):

                    def part(where, k):
                        return v_ref[where * 6 + k, at : at + 8, :]

                    if direction == 0:
                        vec = [part(spot + tiles, k) for k in range(6)]
                    elif direction == 1:
                        vec = [
                            pltpu.roll(jnp.where(spills, part(next_tile, k), part(spot, k)), LANES - LZ, 1)
                            for k in range(6)
                        ]
                    else:
                        vec = [
                            jnp.where(
                                wraps,
                                pltpu.roll(part(spot, k), LZ - 1, 1),
                                pltpu.roll(part(spot, k), LANES - 1, 1),
                            )
                            for k in range(6)
                        ]
                    outs = link_product(links, vec[:3], vec[3:])
                    for half in range(2):
                        row = (direction * 2 + half) * count + at
                        for colour in range(3):
                            column = (sub * 3 + colour) * LANES
                            op_ref[slot, row : row + 8, column : column + LANES] = outs[half][colour].astype(
                                BF16
                            )

    def multiply(step, slot, directions):
        fixed = lhs_ref[step]
        low = min(directions) * 2 * count
        high = (max(directions) + 1) * 2 * count
        got = nt_dot(jnp.concatenate([fixed, op_ref[slot, low:high, :]], axis=0), fixed)
        g_ref[step // halves] += got[: 2 * count]
        acc_ref[low:high, :] += got[2 * count :]

    every, side = (0, 1, 2), (1, 2)
    inner = steps - halves
    elementwise(inner, 0, side)
    for step in range(inner + 1, steps):
        multiply(step - 1, (step - 1) & 1, side)
        elementwise(step, step & 1, side)
    multiply(steps - 1, (steps - 1) & 1, side)
    elementwise(0, 0, every)

    def body(step, carry):
        slot = step & 1
        multiply(step - 1, 1 - slot, every)
        elementwise(step, slot, every)
        return carry

    lax.fori_loop(1, inner, body, 0)
    multiply(inner - 1, (inner - 1) & 1, every)
    fill_table(groups, slots, empty, owner_ref, elem_ref, source_ref, spin_ref, table_ref)

    first = lax.axis_index("space") * planes
    total_re = jnp.zeros((count, count), F32)
    total_im = jnp.zeros((count, count), F32)
    for plane in range(planes):
        real, imag = paired(g_ref[plane], count)
        cosine = phase_ref[first + plane]
        sine = phase_ref[lx + first + plane]
        total_re += cosine * real - sine * imag
        total_im += cosine * imag + sine * real
    sums_ref[0, 0] = total_re
    sums_ref[0, 1] = -total_im
    for direction in range(3):
        grid = acc_ref[direction * 2 * count : (direction + 1) * 2 * count, :]
        real, imag = anti(*paired(grid, count))
        sums_ref[direction + 1, 0] = real
        sums_ref[direction + 1, 1] = imag


def gram(v, lhs, u, phases, tables, count, tiles, planes, lx, groups, slots, empty):
    pair = 2
    wide = pair * 3 * LANES
    return pl.pallas_call(
        partial(gram_kernel, count, tiles, planes, lx, groups, slots, empty),
        in_specs=[vspec()] * 3 + [sspec()] + [vspec()] * 4,
        out_specs=[vspec()] * 2,
        out_shape=[
            jax.ShapeDtypeStruct((OPS, 2, count, count), F32),
            jax.ShapeDtypeStruct((1, LANES), jnp.int32),
        ],
        scratch_shapes=[
            VMEM((2, 6 * count, wide), BF16),
            VMEM((6 * count, 2 * count), F32),
            VMEM((planes, 2 * count, 2 * count), F32),
        ],
        compiler_params=limit(16),
        cost_estimate=cost(8 * 10**9, 5 * 10**6),
        name="gram",
    )(v, lhs, u, phases, *tables)


def edge_kernel(
    count, tiles, planes, rows, cores, far_ref, near_ref, lhs_ref, u_ref, sums_ref, keep_ref, send_ref, op_ref, tot_ref
):
    spots = tiles * planes
    pair = 2
    total = None
    for half_tile in range(tiles // pair):
        for sub in range(pair):
            tile = half_tile * pair + sub
            links = load_links(u_ref, 0, tile * planes + planes - 1, spots)
            for at in range(0, count, GROUP):
                parts = [
                    (far_ref[k * tiles + tile, at : at + GROUP] + near_ref[k * tiles + tile, at : at + GROUP])
                    .astype(F32)
                    for k in range(6)
                ]
                outs = [
                    link_product(
                        links,
                        [part[eight : eight + 8] for part in parts[:3]],
                        [part[eight : eight + 8] for part in parts[3:]],
                    )
                    for eight in (0, 8)
                ]
                for half in range(2):
                    for colour in range(3):
                        column = (sub * 3 + colour) * LANES
                        both = jnp.concatenate([outs[0][half][colour], outs[1][half][colour]], axis=0)
                        op_ref[
                            half_tile, half * count + at : half * count + at + GROUP, column : column + LANES
                        ] = both.astype(BF16)
        got = nt_dot(op_ref[half_tile], lhs_ref[(planes - 1) * (tiles // pair) + half_tile])
        total = got if total is None else total + got
    real, imag = anti(*paired(total, count))
    tot_ref[0] = real
    tot_ref[1] = imag
    mine = lax.axis_index("space") & (cores - 1)
    for chip in range(count // (rows * cores)):
        for which, ref in ((mine, keep_ref), (1 - mine, send_ref)):
            at = pl.multiple_of((chip * cores + which) * rows, rows)
            for op in range(OPS):
                for half in range(2):
                    piece = sums_ref[op, half, pl.ds(at, rows), :]
                    if op == 1:
                        piece = piece + tot_ref[half, pl.ds(at, rows), :]
                    ref[chip, op, half] = piece


def edge(far, near, lhs, u, sums, count, tiles, planes, rows, cores):
    pair = 2
    shape = jax.ShapeDtypeStruct((count // (rows * cores), OPS, 2, rows, count), F32)
    return pl.pallas_call(
        partial(edge_kernel, count, tiles, planes, rows, cores),
        in_specs=[vspec()] * 5,
        out_specs=[vspec(), vspec()],
        out_shape=[shape, shape],
        scratch_shapes=[
            VMEM((tiles // pair, 2 * count, pair * 3 * LANES), BF16),
            VMEM((2, count, count), F32),
        ],
        compiler_params=limit(8),
        cost_estimate=cost(10**9, 3 * 10**6),
        name="edge",
    )(far, near, lhs, u, sums)


def split_sum(block):
    high = block[0:1].astype(BF16)
    low = (block[0:1] - high.astype(F32)).astype(BF16)
    return jnp.concatenate([high, low, block[1:].astype(BF16)], axis=0)


def fold_kernel(chips, cores, keep_ref, got_ref, own_ref, *out_refs):
    me = lax.axis_index("space") // cores
    own_ref[...] = keep_ref[me] + got_ref[me]
    for step in range(1, chips):
        to = me ^ step
        out_refs[step - 1][...] = split_sum(keep_ref[to] + got_ref[to])


def fold(keep, got, cores):
    chips = keep.shape[0]
    shape = keep.shape[1:]
    sent = jax.ShapeDtypeStruct((shape[0] + 1,) + shape[1:], BF16)
    return pl.pallas_call(
        partial(fold_kernel, chips, cores),
        in_specs=[vspec()] * 2,
        out_specs=[vspec()] * chips,
        out_shape=[jax.ShapeDtypeStruct(shape, F32)] + [sent] * (chips - 1),
        compiler_params=limit(4),
        cost_estimate=cost(10**6, 10**6),
        name="fold",
    )(keep, got)


def total_kernel(own_ref, *refs):
    total_ref = refs[-1]
    first = own_ref[0:1]
    rest = own_ref[1:]
    for ref in refs[:-1]:
        first = first + (ref[0:1].astype(F32) + ref[1:2].astype(F32))
        rest = rest + ref[2:].astype(F32)
    total_ref[0:1] = first.astype(BF16)
    total_ref[1:] = rest.astype(BF16)


def total_rows(parts):
    return pl.pallas_call(
        total_kernel,
        in_specs=[vspec()] * len(parts),
        out_specs=vspec(),
        out_shape=jax.ShapeDtypeStruct(parts[0].shape, BF16),
        compiler_params=limit(4),
        cost_estimate=cost(10**6, 10**6),
        name="total",
    )(*parts)


def dress_kernel(groups, slots, taus, rows, count, table_ref, per_ref, *refs):
    slab_refs = refs[:groups]
    out_ref, lhs_ref, prod_ref = refs[groups:]
    me = lax.axis_index("tm")
    for step in range(groups):
        group = me ^ step
        for op in range(OPS):
            at = pl.multiple_of((group * OPS + op) * rows, rows)
            lhs_ref[pl.ds(at, rows), 0:count] = slab_refs[step][op, 0]
            lhs_ref[pl.ds(at, rows), count : 2 * count] = slab_refs[step][op, 1]
    left = lhs_ref[...]
    for tau in range(taus):
        real, imag = per_ref[tau, 0], per_ref[tau, 1]
        right = jnp.concatenate(
            [jnp.concatenate([real, imag], axis=1), jnp.concatenate([-imag, real], axis=1)], axis=0
        )
        got = jnp.dot(left, right, preferred_element_type=F32).astype(BF16)
        for piece in range(groups * OPS):
            prod_ref[tau * groups * OPS + piece] = got[piece * rows : (piece + 1) * rows]
    prod_ref[taus * groups * OPS] = jnp.zeros((rows, 2 * count), BF16)
    for group in range(groups):
        for slot in range(slots):
            piece = prod_ref[table_ref[0, group * slots + slot]]
            out_ref[group, slot, 0] = piece[:, :count]
            out_ref[group, slot, 1] = piece[:, count:]


def dress(table, per, slabs, groups, slots, rows, count):
    taus = per.shape[0]
    return pl.pallas_call(
        partial(dress_kernel, groups, slots, taus, rows, count),
        in_specs=[sspec(), vspec()] + [vspec()] * groups,
        out_specs=vspec(),
        out_shape=jax.ShapeDtypeStruct((groups, slots, 2, rows, count), BF16),
        scratch_shapes=[
            VMEM((groups * OPS * rows, 2 * count), BF16),
            VMEM((taus * groups * OPS + 1, rows, 2 * count), BF16),
        ],
        compiler_params=limit(8),
        cost_estimate=cost(10**9, 2 * 10**6),
        name="dress",
    )(table, per, *slabs)


def fast_shards(eigvecs, gauge_links, perambulator, job_owner, job_elemental, job_source, job_spin):
    count = eigvecs.shape[1]
    planes, sites = eigvecs.shape[4], eigvecs.shape[5]
    tiles = sites // LANES
    space_size = lax.axis_size("space")
    groups = lax.axis_size("tm")
    lx = planes * space_size
    rows = count // space_size
    slots = 3 * ((JOB_DEV + groups - 1) // groups)
    cores = 2

    def tiled(field):
        head = field.shape[:-2]
        order = tuple(range(len(head))) + (len(head) + 1, len(head), len(head) + 2)
        split = field.reshape(head + (planes, tiles, LANES))
        return split.transpose(order).reshape(-1, LANES)

    x = tiled(eigvecs)
    u = tiled(gauge_links)
    angle = 2.0 * math.pi / lx * np.arange(lx)
    phases = jnp.asarray(np.concatenate([np.cos(angle), np.sin(angle)]).astype(np.float32))

    per = perambulator.reshape(-1, 2, count, count)
    empty = per.shape[0] * groups * OPS
    x = pltpu.with_memory_space_constraint(x, pltpu.HBM)
    u = pltpu.with_memory_space_constraint(u, pltpu.HBM)
    down = [(i, (i - 1) % space_size) for i in range(space_size)]
    rim = rim_plane(x, count, tiles, planes, cores)
    far = lax.ppermute(rim, "space", [move for move in down if move[0] % cores == 0])
    v, lhs, rim, u = spread(x, u, rim, count, tiles, planes)
    near = lax.ppermute(rim, "space", [move for move in down if move[0] % cores != 0])
    tables = [job.reshape(1, -1) for job in (job_owner, job_elemental, job_source, job_spin)]
    sums, table = gram(
        v, lhs, u, phases, tables, count, tiles, planes, lx, groups, slots, empty
    )
    keep, send = edge(far, near, lhs, u, sums, count, tiles, planes, rows, cores)
    got = lax.ppermute(send, "space", [(i, i ^ 1) for i in range(space_size)])
    parts = fold(keep, got, cores)
    summed = [parts[0]]
    for step in range(1, space_size // cores):
        summed.append(
            lax.ppermute(parts[step], "space", [(i, i ^ (step * cores)) for i in range(space_size)])
        )
    own = total_rows(summed)
    slabs = [own]
    for step in range(1, groups):
        slabs.append(lax.ppermute(own, "tm", [(i, i ^ step) for i in range(groups)]))
    return dress(table, per, slabs, groups, slots, rows, count)[None]


def passed_along(shard, axis, by):
    count = lax.axis_size(axis)
    return lax.ppermute(shard, axis, [(i, (i + by) % count) for i in range(count)])


def shifted_sites(lattice_field, direction, offset):
    shaped = lattice_field.reshape(lattice_field.shape[:-1] + (LY, LZ))
    rolled = jnp.roll(shaped, -offset, axis=direction - 4)
    return rolled.reshape(lattice_field.shape)


def apply_link(link_field, vectors):
    total_re = None
    total_im = None
    for colour in range(3):
        link_re = link_field[0, :, colour][None]
        link_im = link_field[1, :, colour][None]
        vector_re = vectors[:, 0, colour][:, None]
        vector_im = vectors[:, 1, colour][:, None]
        part_re = link_re * vector_re - link_im * vector_im
        part_im = link_re * vector_im + link_im * vector_re
        if colour == 0:
            total_re, total_im = (part_re, part_im)
        else:
            total_re = total_re + part_re
            total_im = total_im + part_im
    return jnp.stack([total_re, total_im], axis=1)


def stacked_form(vectors):
    vector_count = vectors.shape[0]
    swapped = jnp.concatenate([-vectors[:, 1:2], vectors[:, 0:1]], axis=1)
    return jnp.concatenate(
        [vectors.reshape(vector_count, -1), swapped.reshape(vector_count, -1)], axis=0
    )


def paired_gram(stacked, lattice_field):
    vector_count = lattice_field.shape[0]
    flat_field = lattice_field.astype(jnp.bfloat16).reshape(vector_count, -1)
    product = lax.dot_general(
        stacked, flat_field, (((1,), (1,)), ((), ())), preferred_element_type=jnp.float32
    )
    return product.reshape(2, vector_count, vector_count)


def twisted_field(vectors, xcoord):
    phase_angle = 2.0 * math.pi / (vectors.shape[3] * lax.axis_size("space")) * xcoord
    cosine = jnp.cos(phase_angle)[:, None]
    sine_part = jnp.sin(phase_angle)[:, None]
    real_part = cosine * vectors[:, 0] + sine_part * vectors[:, 1]
    imag_part = cosine * vectors[:, 1] - sine_part * vectors[:, 0]
    return jnp.stack([real_part, imag_part], axis=1)


def antihermitian(paired):
    return 0.5 * jnp.stack([paired[0] - paired[0].T, paired[1] + paired[1].T], axis=0)


def plain_shards(eigvecs, gauge_links, perambulator, job_owner, job_elemental, job_source, job_spin):
    slice_count = eigvecs.shape[0]
    vector_count = eigvecs.shape[1]
    planes = eigvecs.shape[4]
    space_size = lax.axis_size("space")
    group_count = lax.axis_size("tm")
    row_count = vector_count // space_size
    capacity = 3 * ((JOB_DEV + group_count - 1) // group_count)
    xcoord = (lax.axis_index("space") * planes + jnp.arange(planes, dtype=jnp.int32)).astype(
        jnp.float32
    )
    upper_plane = passed_along(eigvecs[:, :, :, :, 0:1], "space", -1)
    low_vectors = eigvecs[0]
    vectors = low_vectors.astype(jnp.float32)
    stacked = stacked_form(low_vectors)
    results = [paired_gram(stacked, twisted_field(vectors, xcoord))]
    for direction in (1, 2, 3):
        link_field = gauge_links[0, direction - 1]
        if direction == 1:
            upper_rim = upper_plane[0].astype(jnp.float32)
            above_field = jnp.concatenate([vectors[:, :, :, 1:], upper_rim], axis=3)
        else:
            above_field = shifted_sites(vectors, direction, 1)
        forward = apply_link(link_field, above_field)
        results.append(antihermitian(paired_gram(stacked, forward)))
    partial_list = [jnp.stack(results, axis=0)]
    partial_value = jnp.stack(partial_list, axis=0)
    summed = lax.psum(partial_value, "space")
    own_rows = lax.dynamic_slice_in_dim(summed, lax.axis_index("space") * row_count, row_count, 3)
    slab_table = own_rows.astype(jnp.bfloat16).reshape(
        slice_count * OPS, 2 * row_count * vector_count
    )
    owners = job_owner[:, 0].reshape(group_count, -1)
    elements = job_elemental.reshape(group_count, -1)
    position = jnp.arange(owners.shape[1], dtype=jnp.int32)
    earlier = position[None, :] < position[:, None]
    same_owner = owners[:, :, None] == owners[:, None, :]
    slot_rank = jnp.sum(jnp.where(same_owner & earlier[None], 1, 0), axis=2).astype(jnp.int32)
    own_group = lax.axis_index("tm")
    slot_count = group_count * capacity
    live_jobs = owners == own_group
    slot_match = live_jobs[:, None, :] & (
        slot_rank[:, None, :] == jnp.arange(capacity, dtype=jnp.int32)[None, :, None]
    )
    sender_owners = lax.dynamic_index_in_dim(owners, own_group, 0, keepdims=False)
    sender_ranks = lax.dynamic_index_in_dim(slot_rank, own_group, 0, keepdims=False)
    sender_elements = lax.dynamic_index_in_dim(elements, own_group, 0, keepdims=False)
    slot_ids = sender_owners * capacity + sender_ranks
    slot_hot = (jnp.arange(slot_count, dtype=jnp.int32)[:, None] == slot_ids[None, :]).astype(
        jnp.float32
    )
    elem_hot = (
        sender_elements[:, None] == jnp.arange(slice_count * OPS, dtype=jnp.int32)[None, :]
    ).astype(jnp.float32)
    picker = jnp.dot(slot_hot, elem_hot, precision=lax.Precision.HIGHEST).astype(jnp.bfloat16)
    outgoing = jnp.dot(picker, slab_table, preferred_element_type=jnp.float32).astype(jnp.bfloat16)
    outgoing = outgoing.reshape(group_count, capacity, 2, row_count, vector_count)
    received = lax.all_to_all(outgoing, "tm", split_axis=0, concat_axis=0, tiled=True)
    block_index = job_source.reshape(group_count, -1) * SPIN + job_spin.reshape(group_count, -1)
    tau_index = jnp.sum(jnp.where(slot_match, block_index[:, None, :], 0), axis=2)
    blocks = perambulator.reshape(-1, 2 * vector_count, vector_count)
    chosen = jnp.take(blocks, tau_index.reshape(-1), axis=0)
    slab_rows = received.reshape(slot_count, 2, row_count, vector_count)
    real_rows = jnp.concatenate([slab_rows[:, 0], -slab_rows[:, 1]], axis=-1)
    imag_rows = jnp.concatenate([slab_rows[:, 1], slab_rows[:, 0]], axis=-1)
    left_side = jnp.stack([real_rows, imag_rows], axis=1).reshape(
        slot_count, 2 * row_count, 2 * vector_count
    )
    dressed = lax.dot_general(
        left_side, chosen, (((2,), (1,)), ((0,), (0,))), preferred_element_type=jnp.float32
    )
    return dressed.astype(jnp.bfloat16).reshape(
        1, group_count, capacity, 2, row_count, vector_count
    )


def shards(*args):
    eigvecs = args[0]
    count, planes, sites = eigvecs.shape[1], eigvecs.shape[4], eigvecs.shape[5]
    space_size, groups = lax.axis_size("space"), lax.axis_size("tm")
    whole_tiles = sites % (2 * LANES) == 0 and count == LANES and planes * (sites // LANES) == GROUP
    fits = groups * 3 * ((JOB_DEV + groups - 1) // groups) < LANES
    powers = space_size & (space_size - 1) == 0 and groups & (groups - 1) == 0
    small = space_size * GROUP == count and groups <= 8 and args[3].shape[0] <= LANES
    if whole_tiles and fits and powers and small and eigvecs.shape[0] == 1:
        return fast_shards(*args)
    return plain_shards(*args)


def solution(mesh):
    return jax.shard_map(
        shards,
        mesh=mesh,
        in_specs=(
            P("tm", None, None, None, "space", None),
            P("tm", None, None, None, None, "space", None),
            P("tm", None, None, None, None),
            P(),
            P(),
            P(),
            P(),
        ),
        out_specs=P("tm", None, None, None, "space", None),
        check_vma=False,
    )
```

```python
import math
from functools import partial

import numpy as np
import jax
import jax.numpy as jnp
from jax import lax
from jax.experimental import pallas as pl
from jax.experimental.pallas import tpu as pltpu
from jax.sharding import PartitionSpec as P

LY = 16
LZ = 32
OPS = 4
SPIN = 4
JOB_DEV = 24
LANES = 128
GROUP = 16
F32 = jnp.float32
BF16 = jnp.bfloat16
VMEM = pltpu.VMEM
SMEM = pltpu.SMEM


def vspec():
    return pl.BlockSpec(memory_space=VMEM)


def sspec():
    return pl.BlockSpec(memory_space=SMEM)


def cost(flops, moved):
    return pl.CostEstimate(flops=flops, bytes_accessed=moved, transcendentals=0)


def limit(mebibytes):
    return pltpu.CompilerParams(vmem_limit_bytes=mebibytes * 2**20)


def pick_matrix(rows, cols, source_of):
    row = lax.broadcasted_iota(jnp.int32, (rows, cols), 0)
    col = lax.broadcasted_iota(jnp.int32, (rows, cols), 1)
    return jnp.where(col == source_of(row), 1.0, 0.0).astype(BF16)


def nt_dot(left, right):
    return lax.dot_general(left, right, (((1,), (1,)), ((), ())), preferred_element_type=F32)


def rim_kernel(tiles, planes, x_hbm, u_hbm, out_ref, x_ref, u_ref, pick_ref, link_ref, sems):
    spots = tiles * planes
    pair = 2
    count = out_ref.shape[1] // 2
    chunk = GROUP * 6 * spots
    chunks = count // GROUP
    first = 18 * spots
    head, tail = pl.ds(0, first), pl.ds(first, u_hbm.shape[0] - first)
    copies = []
    for g in range(chunks):
        rows = pl.ds(g * chunk, chunk)
        copies.append(pltpu.make_async_copy(x_hbm.at[rows], x_ref.at[rows], sems.at[g]))
    link_copy = pltpu.make_async_copy(u_hbm.at[head], u_ref.at[head], sems.at[chunks])
    rest_copy = pltpu.make_async_copy(u_hbm.at[tail], u_ref.at[tail], sems.at[chunks + 1])
    for copy in [link_copy] + copies + [rest_copy]:
        copy.start()

    def source(row):
        return (row & (GROUP - 1)) * spots + (row // GROUP) * planes + planes - 1

    pick_ref[...] = pick_matrix(tiles * GROUP, GROUP * spots, source)
    link_copy.wait()
    for tile in range(tiles):
        flat = adjoint(load_rows(u_ref, 0, tile * planes + planes - 1, spots))
        for k, link in enumerate(flat):
            link_ref[tile, k] = link
    chosen = pick_ref[...]
    for g in range(chunks):
        copies[g].wait()
        block = x_ref[g * chunk : (g + 1) * chunk, :].reshape(GROUP, 6, spots, LANES)
        taken = []
        for part in range(0, 6, 2):
            rows = jnp.concatenate(
                [block[:, part + k].reshape(GROUP * spots, LANES) for k in range(2)], axis=1
            )
            got = jnp.dot(chosen, rows, preferred_element_type=F32)
            taken += [got[:, :LANES], got[:, LANES:]]
        for tile in range(tiles):
            links = [[[link_ref[tile, (p * 3 + r) * 3 + c] for c in range(3)] for r in range(3)] for p in range(3)]
            outs = []
            for eight in (0, 8):
                at = tile * GROUP + eight
                vec = [part[at : at + 8] for part in taken]
                outs.append(link_product(links, vec[:3], vec[3:]))
            for half in range(2):
                row = half * count + g * GROUP
                for colour in range(3):
                    column = ((tile % pair) * 3 + colour) * LANES
                    both = jnp.concatenate([outs[0][half][colour], outs[1][half][colour]], axis=0)
                    out_ref[tile // pair, row : row + GROUP, column : column + LANES] = both.astype(BF16)
    rest_copy.wait()


def rim_plane(x, u, count, tiles, planes):
    spots = tiles * planes
    pair = 2
    return pl.pallas_call(
        partial(rim_kernel, tiles, planes),
        in_specs=[pl.BlockSpec(memory_space=pltpu.HBM)] * 2,
        out_specs=[vspec()] * 3,
        out_shape=[
            jax.ShapeDtypeStruct((tiles // pair, 2 * count, pair * 3 * LANES), BF16),
            jax.ShapeDtypeStruct(x.shape, BF16),
            jax.ShapeDtypeStruct(u.shape, F32),
        ],
        scratch_shapes=[
            VMEM((tiles * GROUP, GROUP * spots), BF16),
            VMEM((tiles, 27, 8, LANES), F32),
            pltpu.SemaphoreType.DMA((count // GROUP + 2,)),
        ],
        compiler_params=limit(8),
        cost_estimate=cost(10**8, 4 * 10**6),
        name="rim",
    )(x, u)


def link_product(links, vec_re, vec_im):
    plus = [vec_re[c] + vec_im[c] for c in range(3)]
    outs_re, outs_im = [], []
    for row in range(3):
        link_re, link_less, link_more = links[0][row], links[1][row], links[2][row]
        one = link_re[0] * plus[0] + link_re[1] * plus[1] + link_re[2] * plus[2]
        two = link_less[0] * vec_re[0] + link_less[1] * vec_re[1] + link_less[2] * vec_re[2]
        three = link_more[0] * vec_im[0] + link_more[1] * vec_im[1] + link_more[2] * vec_im[2]
        outs_re.append(one - three)
        outs_im.append(one + two)
    return outs_re, outs_im


def load_rows(u_ref, direction, spot, spots):
    def one(part, row, col):
        at = (((direction * 2 + part) * 3 + row) * 3 + col) * spots + spot
        return jnp.broadcast_to(u_ref[pl.ds(at, 1), :], (8, LANES))

    return [[[one(part, row, col) for col in range(3)] for row in range(3)] for part in range(2)]


def load_links(u_ref, direction, spot, spots):
    real, imag = load_rows(u_ref, direction, spot, spots)
    less = [[imag[row][col] - real[row][col] for col in range(3)] for row in range(3)]
    more = [[imag[row][col] + real[row][col] for col in range(3)] for row in range(3)]
    return real, less, more


def adjoint(grid):
    real, imag = grid
    order = [(row, col) for row in range(3) for col in range(3)]
    return (
        [real[col][row] for row, col in order]
        + [-imag[col][row] - real[col][row] for row, col in order]
        + [real[col][row] - imag[col][row] for row, col in order]
    )


def fill_table(groups, slots, empty, owner_ref, elem_ref, source_ref, spin_ref, table_ref):
    total = owner_ref.shape[1]
    jobs = total // groups
    row = lax.broadcasted_iota(jnp.int32, (total, total), 0)
    col = lax.broadcasted_iota(jnp.int32, (total, total), 1)

    def group_of(index):
        return sum((index >= group * jobs).astype(jnp.int32) for group in range(1, groups))

    live = jnp.where(owner_ref[...] == lax.axis_index("tm"), 1.0, 0.0)
    product = source_ref[...] * (SPIN * groups * OPS) + spin_ref[...] * (groups * OPS) + elem_ref[...]

    def column(mask, values):
        wide = jnp.broadcast_to(values.astype(F32), (total, total))
        return jnp.sum(jnp.where(mask, wide, 0.0), axis=1, keepdims=True)

    rank = column((col < row) & (group_of(col) == group_of(row)), live)
    alive = column(col == row, live)
    value = column(col == row, product)
    at_row = lax.broadcasted_iota(jnp.int32, (total, LANES), 0)
    at_col = lax.broadcasted_iota(jnp.int32, (total, LANES), 1)
    group = group_of(at_row).astype(F32)
    place = jnp.where(alive > 0.5, group * slots + rank, -1.0)
    found = at_col.astype(F32) == place
    picked = jnp.sum(jnp.where(found, value + group * OPS - empty, 0.0), axis=0, keepdims=True)
    table_ref[...] = (picked + empty).astype(jnp.int32)


def paired(grid, count):
    real = grid[:count, :count] + grid[count:, count:]
    imag = grid[count:, :count] - grid[:count, count:]
    return real, imag


def anti(real, imag):
    return 0.5 * (real.T - real), 0.5 * (imag.T + imag)


def gram_kernel(
    count, tiles, planes, lx, groups, slots, empty,
    x_ref, u_ref, phase_ref, owner_ref, elem_ref, source_ref, spin_ref,
    sums_ref, rim_lhs_ref, table_ref,
    v_ref, lhs_ref, op_ref, acc_ref, g_ref, pick_ref,
):
    spots = tiles * planes
    pair = 2
    halves = tiles // pair
    steps = planes * halves

    def source(row):
        spot = row // GROUP
        return (row & (GROUP - 1)) * spots + (spot % tiles) * planes + spot // tiles

    pick_ref[...] = pick_matrix(GROUP * spots, GROUP * spots, source)
    acc_ref[...] = jnp.zeros_like(acc_ref)
    g_ref[...] = jnp.zeros_like(g_ref)

    chosen = pick_ref[...]
    for at in range(0, count, GROUP):
        block = x_ref[at * 6 * spots : (at + GROUP) * 6 * spots, :].reshape(GROUP, 6, spots, LANES)
        for first in range(0, 6, 2):
            rows = jnp.concatenate(
                [block[:, first + k].reshape(GROUP * spots, LANES) for k in range(2)], axis=1
            )
            taken = jnp.dot(chosen, rows, preferred_element_type=F32)
            for k in range(2):
                part = first + k
                half, colour = part // 3, part % 3
                for spot in range(spots):
                    piece = taken[spot * GROUP : (spot + 1) * GROUP, k * LANES : (k + 1) * LANES]
                    v_ref[spot * 6 + part, at : at + GROUP, :] = piece
                    plane, tile = spot // tiles, spot % tiles
                    lhs_ref[
                        plane * halves + tile // pair,
                        half * count + at : half * count + at + GROUP,
                        ((tile % pair) * 3 + colour) * LANES : ((tile % pair) * 3 + colour + 1) * LANES,
                    ] = piece.astype(BF16)

    lane = lax.broadcasted_iota(jnp.int32, (8, LANES), 1)
    wraps = (lane & (LZ - 1)) == LZ - 1
    spills = lane < LZ

    def elementwise(step, slot, directions):
        plane = step // halves
        half_tile = step % halves
        for sub in range(pair):
            tile = half_tile * pair + sub
            spot = plane * tiles + tile
            next_tile = plane * tiles + (tile + 1) % tiles
            for direction in directions:
                links = load_links(u_ref, direction, tile * planes + plane, spots)
                for at in range(0, count, 8):

                    def part(where, k):
                        return v_ref[where * 6 + k, at : at + 8, :]

                    if direction == 0:
                        vec = [part(spot + tiles, k) for k in range(6)]
                    elif direction == 1:
                        vec = [
                            pltpu.roll(jnp.where(spills, part(next_tile, k), part(spot, k)), LANES - LZ, 1)
                            for k in range(6)
                        ]
                    else:
                        vec = [
                            jnp.where(
                                wraps,
                                pltpu.roll(part(spot, k), LZ - 1, 1),
                                pltpu.roll(part(spot, k), LANES - 1, 1),
                            )
                            for k in range(6)
                        ]
                    outs = link_product(links, vec[:3], vec[3:])
                    for half in range(2):
                        row = (direction * 2 + half) * count + at
                        for colour in range(3):
                            column = (sub * 3 + colour) * LANES
                            op_ref[slot, row : row + 8, column : column + LANES] = outs[half][colour].astype(
                                BF16
                            )

    def multiply(step, slot, directions):
        fixed = lhs_ref[step]
        low = min(directions) * 2 * count
        high = (max(directions) + 1) * 2 * count
        got = nt_dot(jnp.concatenate([fixed, op_ref[slot, low:high, :]], axis=0), fixed)
        g_ref[step // halves] += got[: 2 * count]
        acc_ref[low:high, :] += got[2 * count :]

    every, side = (0, 1, 2), (1, 2)
    inner = steps - halves
    elementwise(inner, 0, side)
    for step in range(inner + 1, steps):
        multiply(step - 1, (step - 1) & 1, side)
        elementwise(step, step & 1, side)
    multiply(steps - 1, (steps - 1) & 1, side)
    elementwise(0, 0, every)

    def body(step, carry):
        slot = step & 1
        multiply(step - 1, 1 - slot, every)
        elementwise(step, slot, every)
        return carry

    lax.fori_loop(1, inner, body, 0)
    multiply(inner - 1, (inner - 1) & 1, every)
    fill_table(groups, slots, empty, owner_ref, elem_ref, source_ref, spin_ref, table_ref)

    first = lax.axis_index("space") * planes
    total_re = jnp.zeros((count, count), F32)
    total_im = jnp.zeros((count, count), F32)
    for plane in range(planes):
        real, imag = paired(g_ref[plane], count)
        cosine = phase_ref[first + plane]
        sine = phase_ref[lx + first + plane]
        total_re += cosine * real - sine * imag
        total_im += cosine * imag + sine * real
    sums_ref[0, 0] = total_re
    sums_ref[0, 1] = -total_im
    for direction in range(3):
        grid = acc_ref[direction * 2 * count : (direction + 1) * 2 * count, :]
        real, imag = anti(*paired(grid, count))
        sums_ref[direction + 1, 0] = real
        sums_ref[direction + 1, 1] = imag
    for half in range(halves):
        rim_lhs_ref[half] = lhs_ref[half]


def gram(x, u, phases, tables, count, tiles, planes, lx, groups, slots, empty):
    spots = tiles * planes
    pair = 2
    steps = planes * (tiles // pair)
    wide = pair * 3 * LANES
    return pl.pallas_call(
        partial(gram_kernel, count, tiles, planes, lx, groups, slots, empty),
        in_specs=[vspec()] * 2 + [sspec()] + [vspec()] * 4,
        out_specs=[vspec()] * 3,
        out_shape=[
            jax.ShapeDtypeStruct((OPS, 2, count, count), F32),
            jax.ShapeDtypeStruct((tiles // pair, 2 * count, wide), BF16),
            jax.ShapeDtypeStruct((1, LANES), jnp.int32),
        ],
        scratch_shapes=[
            VMEM((spots * 6, count, LANES), F32),
            VMEM((steps, 2 * count, wide), BF16),
            VMEM((2, 6 * count, wide), BF16),
            VMEM((6 * count, 2 * count), F32),
            VMEM((planes, 2 * count, 2 * count), F32),
            VMEM((GROUP * spots, GROUP * spots), BF16),
        ],
        compiler_params=limit(26),
        cost_estimate=cost(8 * 10**9, 5 * 10**6),
        name="gram",
    )(x, u, phases, *tables)


def edge_kernel(count, rows, cores, halo_ref, lhs_ref, sums_ref, keep_ref, send_ref, tot_ref):
    total = None
    for half in range(halo_ref.shape[0]):
        got = nt_dot(halo_ref[half], lhs_ref[half])
        total = got if total is None else total + got
    real = total[:count, :count] + total[count:, count:]
    imag = total[:count, count:] - total[count:, :count]
    tot_ref[0] = 0.5 * (real - real.T)
    tot_ref[1] = 0.5 * (imag + imag.T)
    mine = lax.axis_index("space") & (cores - 1)
    for chip in range(count // (rows * cores)):
        for which, ref in ((mine, keep_ref), (1 - mine, send_ref)):
            at = pl.multiple_of((chip * cores + which) * rows, rows)
            for op in range(OPS):
                for half in range(2):
                    piece = sums_ref[op, half, pl.ds(at, rows), :]
                    if op == 1:
                        piece = piece + tot_ref[half, pl.ds(at, rows), :]
                    ref[chip, op, half] = piece


def edge(halo, rim_lhs, sums, count, rows, cores):
    shape = jax.ShapeDtypeStruct((count // (rows * cores), OPS, 2, rows, count), F32)
    return pl.pallas_call(
        partial(edge_kernel, count, rows, cores),
        in_specs=[vspec()] * 3,
        out_specs=[vspec(), vspec()],
        out_shape=[shape, shape],
        scratch_shapes=[VMEM((2, count, count), F32)],
        compiler_params=limit(8),
        cost_estimate=cost(10**9, 3 * 10**6),
        name="edge",
    )(halo, rim_lhs, sums)


def split_sum(block):
    high = block[0:1].astype(BF16)
    low = (block[0:1] - high.astype(F32)).astype(BF16)
    return jnp.concatenate([high, low, block[1:].astype(BF16)], axis=0)


def fold_kernel(chips, cores, keep_ref, got_ref, own_ref, *out_refs):
    me = lax.axis_index("space") // cores
    own_ref[...] = keep_ref[me] + got_ref[me]
    for step in range(1, chips):
        to = me ^ step
        out_refs[step - 1][...] = split_sum(keep_ref[to] + got_ref[to])


def fold(keep, got, cores):
    chips = keep.shape[0]
    shape = keep.shape[1:]
    sent = jax.ShapeDtypeStruct((shape[0] + 1,) + shape[1:], BF16)
    return pl.pallas_call(
        partial(fold_kernel, chips, cores),
        in_specs=[vspec()] * 2,
        out_specs=[vspec()] * chips,
        out_shape=[jax.ShapeDtypeStruct(shape, F32)] + [sent] * (chips - 1),
        compiler_params=limit(4),
        cost_estimate=cost(10**6, 10**6),
        name="fold",
    )(keep, got)


def total_kernel(own_ref, *refs):
    total_ref = refs[-1]
    first = own_ref[0:1]
    rest = own_ref[1:]
    for ref in refs[:-1]:
        first = first + (ref[0:1].astype(F32) + ref[1:2].astype(F32))
        rest = rest + ref[2:].astype(F32)
    total_ref[0:1] = first.astype(BF16)
    total_ref[1:] = rest.astype(BF16)


def total_rows(parts):
    return pl.pallas_call(
        total_kernel,
        in_specs=[vspec()] * len(parts),
        out_specs=vspec(),
        out_shape=jax.ShapeDtypeStruct(parts[0].shape, BF16),
        compiler_params=limit(4),
        cost_estimate=cost(10**6, 10**6),
        name="total",
    )(*parts)


def dress_kernel(groups, slots, taus, rows, count, table_ref, per_ref, *refs):
    slab_refs = refs[:groups]
    out_ref, lhs_ref, prod_ref = refs[groups:]
    me = lax.axis_index("tm")
    for step in range(groups):
        group = me ^ step
        for op in range(OPS):
            at = pl.multiple_of((group * OPS + op) * rows, rows)
            lhs_ref[pl.ds(at, rows), 0:count] = slab_refs[step][op, 0]
            lhs_ref[pl.ds(at, rows), count : 2 * count] = slab_refs[step][op, 1]
    left = lhs_ref[...]
    for tau in range(taus):
        real, imag = per_ref[tau, 0], per_ref[tau, 1]
        right = jnp.concatenate(
            [jnp.concatenate([real, imag], axis=1), jnp.concatenate([-imag, real], axis=1)], axis=0
        )
        got = jnp.dot(left, right, preferred_element_type=F32).astype(BF16)
        for piece in range(groups * OPS):
            prod_ref[tau * groups * OPS + piece] = got[piece * rows : (piece + 1) * rows]
    prod_ref[taus * groups * OPS] = jnp.zeros((rows, 2 * count), BF16)
    for group in range(groups):
        for slot in range(slots):
            piece = prod_ref[table_ref[0, group * slots + slot]]
            out_ref[group, slot, 0] = piece[:, :count]
            out_ref[group, slot, 1] = piece[:, count:]


def dress(table, per, slabs, groups, slots, rows, count):
    taus = per.shape[0]
    return pl.pallas_call(
        partial(dress_kernel, groups, slots, taus, rows, count),
        in_specs=[sspec(), vspec()] + [vspec()] * groups,
        out_specs=vspec(),
        out_shape=jax.ShapeDtypeStruct((groups, slots, 2, rows, count), BF16),
        scratch_shapes=[
            VMEM((groups * OPS * rows, 2 * count), BF16),
            VMEM((taus * groups * OPS + 1, rows, 2 * count), BF16),
        ],
        compiler_params=limit(8),
        cost_estimate=cost(10**9, 2 * 10**6),
        name="dress",
    )(table, per, *slabs)


def fast_shards(eigvecs, gauge_links, perambulator, job_owner, job_elemental, job_source, job_spin):
    count = eigvecs.shape[1]
    planes, sites = eigvecs.shape[4], eigvecs.shape[5]
    tiles = sites // LANES
    space_size = lax.axis_size("space")
    groups = lax.axis_size("tm")
    lx = planes * space_size
    rows = count // space_size
    slots = 3 * ((JOB_DEV + groups - 1) // groups)
    cores = 2

    def tiled(field):
        head = field.shape[:-2]
        order = tuple(range(len(head))) + (len(head) + 1, len(head), len(head) + 2)
        split = field.reshape(head + (planes, tiles, LANES))
        return split.transpose(order).reshape(-1, LANES)

    x = tiled(eigvecs)
    u = tiled(gauge_links)
    angle = 2.0 * math.pi / lx * np.arange(lx)
    phases = jnp.asarray(np.concatenate([np.cos(angle), np.sin(angle)]).astype(np.float32))

    per = perambulator.reshape(-1, 2, count, count)
    empty = per.shape[0] * groups * OPS
    x = pltpu.with_memory_space_constraint(x, pltpu.HBM)
    u = pltpu.with_memory_space_constraint(u, pltpu.HBM)
    rim, x, u = rim_plane(x, u, count, tiles, planes)
    halo = lax.ppermute(rim, "space", [(i, (i + 1) % space_size) for i in range(space_size)])
    tables = [job.reshape(1, -1) for job in (job_owner, job_elemental, job_source, job_spin)]
    sums, rim_lhs, table = gram(
        x, u, phases, tables, count, tiles, planes, lx, groups, slots, empty
    )
    keep, send = edge(halo, rim_lhs, sums, count, rows, cores)
    got = lax.ppermute(send, "space", [(i, i ^ 1) for i in range(space_size)])
    parts = fold(keep, got, cores)
    summed = [parts[0]]
    for step in range(1, space_size // cores):
        summed.append(
            lax.ppermute(parts[step], "space", [(i, i ^ (step * cores)) for i in range(space_size)])
        )
    own = total_rows(summed)
    slabs = [own]
    for step in range(1, groups):
        slabs.append(lax.ppermute(own, "tm", [(i, i ^ step) for i in range(groups)]))
    return dress(table, per, slabs, groups, slots, rows, count)[None]


def passed_along(shard, axis, by):
    count = lax.axis_size(axis)
    return lax.ppermute(shard, axis, [(i, (i + by) % count) for i in range(count)])


def shifted_sites(lattice_field, direction, offset):
    shaped = lattice_field.reshape(lattice_field.shape[:-1] + (LY, LZ))
    rolled = jnp.roll(shaped, -offset, axis=direction - 4)
    return rolled.reshape(lattice_field.shape)


def apply_link(link_field, vectors):
    total_re = None
    total_im = None
    for colour in range(3):
        link_re = link_field[0, :, colour][None]
        link_im = link_field[1, :, colour][None]
        vector_re = vectors[:, 0, colour][:, None]
        vector_im = vectors[:, 1, colour][:, None]
        part_re = link_re * vector_re - link_im * vector_im
        part_im = link_re * vector_im + link_im * vector_re
        if colour == 0:
            total_re, total_im = (part_re, part_im)
        else:
            total_re = total_re + part_re
            total_im = total_im + part_im
    return jnp.stack([total_re, total_im], axis=1)


def stacked_form(vectors):
    vector_count = vectors.shape[0]
    swapped = jnp.concatenate([-vectors[:, 1:2], vectors[:, 0:1]], axis=1)
    return jnp.concatenate(
        [vectors.reshape(vector_count, -1), swapped.reshape(vector_count, -1)], axis=0
    )


def paired_gram(stacked, lattice_field):
    vector_count = lattice_field.shape[0]
    flat_field = lattice_field.astype(jnp.bfloat16).reshape(vector_count, -1)
    product = lax.dot_general(
        stacked, flat_field, (((1,), (1,)), ((), ())), preferred_element_type=jnp.float32
    )
    return product.reshape(2, vector_count, vector_count)


def twisted_field(vectors, xcoord):
    phase_angle = 2.0 * math.pi / (vectors.shape[3] * lax.axis_size("space")) * xcoord
    cosine = jnp.cos(phase_angle)[:, None]
    sine_part = jnp.sin(phase_angle)[:, None]
    real_part = cosine * vectors[:, 0] + sine_part * vectors[:, 1]
    imag_part = cosine * vectors[:, 1] - sine_part * vectors[:, 0]
    return jnp.stack([real_part, imag_part], axis=1)


def antihermitian(paired):
    return 0.5 * jnp.stack([paired[0] - paired[0].T, paired[1] + paired[1].T], axis=0)


def plain_shards(eigvecs, gauge_links, perambulator, job_owner, job_elemental, job_source, job_spin):
    slice_count = eigvecs.shape[0]
    vector_count = eigvecs.shape[1]
    planes = eigvecs.shape[4]
    space_size = lax.axis_size("space")
    group_count = lax.axis_size("tm")
    row_count = vector_count // space_size
    capacity = 3 * ((JOB_DEV + group_count - 1) // group_count)
    xcoord = (lax.axis_index("space") * planes + jnp.arange(planes, dtype=jnp.int32)).astype(
        jnp.float32
    )
    upper_plane = passed_along(eigvecs[:, :, :, :, 0:1], "space", -1)
    low_vectors = eigvecs[0]
    vectors = low_vectors.astype(jnp.float32)
    stacked = stacked_form(low_vectors)
    results = [paired_gram(stacked, twisted_field(vectors, xcoord))]
    for direction in (1, 2, 3):
        link_field = gauge_links[0, direction - 1]
        if direction == 1:
            upper_rim = upper_plane[0].astype(jnp.float32)
            above_field = jnp.concatenate([vectors[:, :, :, 1:], upper_rim], axis=3)
        else:
            above_field = shifted_sites(vectors, direction, 1)
        forward = apply_link(link_field, above_field)
        results.append(antihermitian(paired_gram(stacked, forward)))
    partial_list = [jnp.stack(results, axis=0)]
    partial_value = jnp.stack(partial_list, axis=0)
    summed = lax.psum(partial_value, "space")
    own_rows = lax.dynamic_slice_in_dim(summed, lax.axis_index("space") * row_count, row_count, 3)
    slab_table = own_rows.astype(jnp.bfloat16).reshape(
        slice_count * OPS, 2 * row_count * vector_count
    )
    owners = job_owner[:, 0].reshape(group_count, -1)
    elements = job_elemental.reshape(group_count, -1)
    position = jnp.arange(owners.shape[1], dtype=jnp.int32)
    earlier = position[None, :] < position[:, None]
    same_owner = owners[:, :, None] == owners[:, None, :]
    slot_rank = jnp.sum(jnp.where(same_owner & earlier[None], 1, 0), axis=2).astype(jnp.int32)
    own_group = lax.axis_index("tm")
    slot_count = group_count * capacity
    live_jobs = owners == own_group
    slot_match = live_jobs[:, None, :] & (
        slot_rank[:, None, :] == jnp.arange(capacity, dtype=jnp.int32)[None, :, None]
    )
    sender_owners = lax.dynamic_index_in_dim(owners, own_group, 0, keepdims=False)
    sender_ranks = lax.dynamic_index_in_dim(slot_rank, own_group, 0, keepdims=False)
    sender_elements = lax.dynamic_index_in_dim(elements, own_group, 0, keepdims=False)
    slot_ids = sender_owners * capacity + sender_ranks
    slot_hot = (jnp.arange(slot_count, dtype=jnp.int32)[:, None] == slot_ids[None, :]).astype(
        jnp.float32
    )
    elem_hot = (
        sender_elements[:, None] == jnp.arange(slice_count * OPS, dtype=jnp.int32)[None, :]
    ).astype(jnp.float32)
    picker = jnp.dot(slot_hot, elem_hot, precision=lax.Precision.HIGHEST).astype(jnp.bfloat16)
    outgoing = jnp.dot(picker, slab_table, preferred_element_type=jnp.float32).astype(jnp.bfloat16)
    outgoing = outgoing.reshape(group_count, capacity, 2, row_count, vector_count)
    received = lax.all_to_all(outgoing, "tm", split_axis=0, concat_axis=0, tiled=True)
    block_index = job_source.reshape(group_count, -1) * SPIN + job_spin.reshape(group_count, -1)
    tau_index = jnp.sum(jnp.where(slot_match, block_index[:, None, :], 0), axis=2)
    blocks = perambulator.reshape(-1, 2 * vector_count, vector_count)
    chosen = jnp.take(blocks, tau_index.reshape(-1), axis=0)
    slab_rows = received.reshape(slot_count, 2, row_count, vector_count)
    real_rows = jnp.concatenate([slab_rows[:, 0], -slab_rows[:, 1]], axis=-1)
    imag_rows = jnp.concatenate([slab_rows[:, 1], slab_rows[:, 0]], axis=-1)
    left_side = jnp.stack([real_rows, imag_rows], axis=1).reshape(
        slot_count, 2 * row_count, 2 * vector_count
    )
    dressed = lax.dot_general(
        left_side, chosen, (((2,), (1,)), ((0,), (0,))), preferred_element_type=jnp.float32
    )
    return dressed.astype(jnp.bfloat16).reshape(
        1, group_count, capacity, 2, row_count, vector_count
    )


def shards(*args):
    eigvecs = args[0]
    count, planes, sites = eigvecs.shape[1], eigvecs.shape[4], eigvecs.shape[5]
    space_size, groups = lax.axis_size("space"), lax.axis_size("tm")
    whole_tiles = sites % (2 * LANES) == 0 and count == LANES and planes * (sites // LANES) == GROUP
    fits = groups * 3 * ((JOB_DEV + groups - 1) // groups) < LANES
    powers = space_size & (space_size - 1) == 0 and groups & (groups - 1) == 0
    small = space_size * GROUP == count and groups <= 8 and args[3].shape[0] <= LANES
    if whole_tiles and fits and powers and small and eigvecs.shape[0] == 1:
        return fast_shards(*args)
    return plain_shards(*args)


def solution(mesh):
    return jax.shard_map(
        shards,
        mesh=mesh,
        in_specs=(
            P("tm", None, None, None, "space", None),
            P("tm", None, None, None, None, "space", None),
            P("tm", None, None, None, None),
            P(),
            P(),
            P(),
            P(),
        ),
        out_specs=P("tm", None, None, None, "space", None),
        check_vma=False,
    )
```

```python
import math
from functools import partial

import numpy as np
import jax
import jax.numpy as jnp
from jax import lax
from jax.experimental import pallas as pl
from jax.experimental.pallas import tpu as pltpu
from jax.sharding import PartitionSpec as P

LY = 16
LZ = 32
OPS = 4
SPIN = 4
JOB_DEV = 24
LANES = 128
GROUP = 16
NARROW = (1, 2)
F32 = jnp.float32
BF16 = jnp.bfloat16
VMEM = pltpu.VMEM
SMEM = pltpu.SMEM


def vspec():
    return pl.BlockSpec(memory_space=VMEM)


def sspec():
    return pl.BlockSpec(memory_space=SMEM)


def cost(flops, moved):
    return pl.CostEstimate(flops=flops, bytes_accessed=moved, transcendentals=0)


def limit(mebibytes):
    return pltpu.CompilerParams(vmem_limit_bytes=mebibytes * 2**20)


def pick_matrix(rows, cols, source_of):
    row = lax.broadcasted_iota(jnp.int32, (rows, cols), 0)
    col = lax.broadcasted_iota(jnp.int32, (rows, cols), 1)
    return jnp.where(col == source_of(row), 1.0, 0.0).astype(BF16)


def joined(pieces):
    return jnp.concatenate(pieces, axis=1)


def nt_dot(left, right):
    return lax.dot_general(left, right, (((1,), (1,)), ((), ())), preferred_element_type=F32)


def rim_kernel(tiles, planes, x_hbm, u_hbm, out_ref, x_ref, u_ref, pick_ref, link_ref, sems):
    spots = tiles * planes
    pair = 2
    count = out_ref.shape[2] // 2
    chunk = GROUP * 6 * spots
    chunks = count // GROUP
    first = 18 * spots
    head, tail = pl.ds(0, first), pl.ds(first, u_hbm.shape[0] - first)
    copies = []
    for g in range(chunks):
        rows = pl.ds(g * chunk, chunk)
        copies.append(pltpu.make_async_copy(x_hbm.at[rows], x_ref.at[rows], sems.at[g]))
    link_copy = pltpu.make_async_copy(u_hbm.at[head], u_ref.at[head], sems.at[chunks])
    rest_copy = pltpu.make_async_copy(u_hbm.at[tail], u_ref.at[tail], sems.at[chunks + 1])
    for copy in [link_copy] + copies + [rest_copy]:
        copy.start()

    def source(row):
        return (row & (GROUP - 1)) * spots + (row // GROUP) * planes + planes - 1

    pick_ref[...] = pick_matrix(tiles * GROUP, GROUP * spots, source)
    link_copy.wait()
    for tile in range(tiles):
        flat = adjoint(load_rows(u_ref, 0, tile * planes + planes - 1, spots))
        for k, link in enumerate(flat):
            link_ref[tile, k] = link
    chosen = pick_ref[...]
    for g in range(chunks):
        copies[g].wait()
        block = x_ref[g * chunk : (g + 1) * chunk, :].reshape(GROUP, 6, spots, LANES)
        taken = []
        for part in range(0, 6, 2):
            rows = jnp.concatenate(
                [block[:, part + k].reshape(GROUP * spots, LANES) for k in range(2)], axis=1
            )
            got = jnp.dot(chosen, rows, preferred_element_type=F32)
            taken += [got[:, :LANES], got[:, LANES:]]
        for tile in range(tiles):
            links = [[[link_ref[tile, (p * 3 + r) * 3 + c] for c in range(3)] for r in range(3)] for p in range(3)]
            outs = []
            for eight in (0, 8):
                at = tile * GROUP + eight
                vec = [part[at : at + 8] for part in taken]
                outs.append(link_product(links, vec[:3], vec[3:]))
            for half in range(2):
                row = half * count + g * GROUP
                for colour in range(3):
                    both = jnp.concatenate([outs[0][half][colour], outs[1][half][colour]], axis=0)
                    out_ref[tile // pair, (tile % pair) * 3 + colour, row : row + GROUP] = both.astype(BF16)
    rest_copy.wait()


def rim_plane(x, u, count, tiles, planes):
    spots = tiles * planes
    pair = 2
    return pl.pallas_call(
        partial(rim_kernel, tiles, planes),
        in_specs=[pl.BlockSpec(memory_space=pltpu.HBM)] * 2,
        out_specs=[vspec()] * 3,
        out_shape=[
            jax.ShapeDtypeStruct((tiles // pair, 3 * pair, 2 * count, LANES), BF16),
            jax.ShapeDtypeStruct(x.shape, BF16),
            jax.ShapeDtypeStruct(u.shape, F32),
        ],
        scratch_shapes=[
            VMEM((tiles * GROUP, GROUP * spots), BF16),
            VMEM((tiles, 27, 8, LANES), F32),
            pltpu.SemaphoreType.DMA((count // GROUP + 2,)),
        ],
        compiler_params=limit(8),
        cost_estimate=cost(10**8, 4 * 10**6),
        name="rim",
    )(x, u)


def link_product(links, vec_re, vec_im):
    plus = [vec_re[c] + vec_im[c] for c in range(3)]
    outs_re, outs_im = [], []
    for row in range(3):
        link_re, link_less, link_more = links[0][row], links[1][row], links[2][row]
        one = link_re[0] * plus[0] + link_re[1] * plus[1] + link_re[2] * plus[2]
        two = link_less[0] * vec_re[0] + link_less[1] * vec_re[1] + link_less[2] * vec_re[2]
        three = link_more[0] * vec_im[0] + link_more[1] * vec_im[1] + link_more[2] * vec_im[2]
        outs_re.append(one - three)
        outs_im.append(one + two)
    return outs_re, outs_im


def narrow_product(links, vec_re, vec_im):
    real, imag = links
    outs_re, outs_im = [], []
    for row in range(3):
        ones = [real[row][c] * vec_re[c] - imag[row][c] * vec_im[c] for c in range(3)]
        twos = [real[row][c] * vec_im[c] + imag[row][c] * vec_re[c] for c in range(3)]
        outs_re.append(ones[0] + ones[1] + ones[2])
        outs_im.append(twos[0] + twos[1] + twos[2])
    return outs_re, outs_im


def narrow_links(u_ref, direction, spot, spots):
    def one(part, row, col):
        at = (((direction * 2 + part) * 3 + row) * 3 + col) * spots + spot
        return jnp.broadcast_to(u_ref[pl.ds(at, 1), :], (GROUP, LANES)).astype(BF16)

    return [[[one(part, row, col) for col in range(3)] for row in range(3)] for part in range(2)]


def load_rows(u_ref, direction, spot, spots):
    def one(part, row, col):
        at = (((direction * 2 + part) * 3 + row) * 3 + col) * spots + spot
        return jnp.broadcast_to(u_ref[pl.ds(at, 1), :], (8, LANES))

    return [[[one(part, row, col) for col in range(3)] for row in range(3)] for part in range(2)]


def load_links(u_ref, direction, spot, spots):
    real, imag = load_rows(u_ref, direction, spot, spots)
    less = [[imag[row][col] - real[row][col] for col in range(3)] for row in range(3)]
    more = [[imag[row][col] + real[row][col] for col in range(3)] for row in range(3)]
    return real, less, more


def adjoint(grid):
    real, imag = grid
    order = [(row, col) for row in range(3) for col in range(3)]
    return (
        [real[col][row] for row, col in order]
        + [-imag[col][row] - real[col][row] for row, col in order]
        + [real[col][row] - imag[col][row] for row, col in order]
    )


def fill_table(groups, slots, empty, owner_ref, elem_ref, source_ref, spin_ref, table_ref):
    total = owner_ref.shape[1]
    jobs = total // groups
    row = lax.broadcasted_iota(jnp.int32, (total, total), 0)
    col = lax.broadcasted_iota(jnp.int32, (total, total), 1)

    def group_of(index):
        return sum((index >= group * jobs).astype(jnp.int32) for group in range(1, groups))

    live = jnp.where(owner_ref[...] == lax.axis_index("tm"), 1.0, 0.0)
    product = source_ref[...] * (SPIN * groups * OPS) + spin_ref[...] * (groups * OPS) + elem_ref[...]

    def column(mask, values):
        wide = jnp.broadcast_to(values.astype(F32), (total, total))
        return jnp.sum(jnp.where(mask, wide, 0.0), axis=1, keepdims=True)

    rank = column((col < row) & (group_of(col) == group_of(row)), live)
    alive = column(col == row, live)
    value = column(col == row, product)
    at_row = lax.broadcasted_iota(jnp.int32, (total, LANES), 0)
    at_col = lax.broadcasted_iota(jnp.int32, (total, LANES), 1)
    group = group_of(at_row).astype(F32)
    place = jnp.where(alive > 0.5, group * slots + rank, -1.0)
    found = at_col.astype(F32) == place
    picked = jnp.sum(jnp.where(found, value + group * OPS - empty, 0.0), axis=0, keepdims=True)
    table_ref[...] = (picked + empty).astype(jnp.int32)


def paired(grid, count):
    real = grid[:count, :count] + grid[count:, count:]
    imag = grid[count:, :count] - grid[:count, count:]
    return real, imag


def anti(real, imag):
    return 0.5 * (real.T - real), 0.5 * (imag.T + imag)


def gram_kernel(
    count, tiles, planes, lx, groups, slots, empty,
    x_ref, u_ref, phase_ref, owner_ref, elem_ref, source_ref, spin_ref,
    sums_ref, rim_lhs_ref, table_ref,
    lhs_ref, op_ref, acc_ref, g_ref, pick_ref,
):
    spots = tiles * planes
    pair = 2
    halves = tiles // pair
    steps = planes * halves

    def source(row):
        spot = row // GROUP
        return (row & (GROUP - 1)) * spots + (spot % tiles) * planes + spot // tiles

    pick_ref[...] = pick_matrix(GROUP * spots, GROUP * spots, source)
    acc_ref[...] = jnp.zeros_like(acc_ref)
    g_ref[...] = jnp.zeros_like(g_ref)

    chosen = pick_ref[...]
    for at in range(0, count, GROUP):
        block = x_ref[at * 6 * spots : (at + GROUP) * 6 * spots, :].reshape(GROUP, 6, spots, LANES)
        for first in range(0, 6, 2):
            rows = jnp.concatenate(
                [block[:, first + k].reshape(GROUP * spots, LANES) for k in range(2)], axis=1
            )
            taken = jnp.dot(chosen, rows, preferred_element_type=F32)
            for k in range(2):
                part = first + k
                half, colour = part // 3, part % 3
                for spot in range(spots):
                    piece = taken[spot * GROUP : (spot + 1) * GROUP, k * LANES : (k + 1) * LANES]
                    plane, tile = spot // tiles, spot % tiles
                    lhs_ref[
                        plane * halves + tile // pair,
                        (tile % pair) * 3 + colour,
                        half * count + at : half * count + at + GROUP,
                    ] = piece.astype(BF16)

    lane = lax.broadcasted_iota(jnp.int32, (GROUP, LANES), 1)
    wraps = (lane & (LZ - 1)) == LZ - 1
    spills = lane < LZ

    def elementwise(step, slot, directions):
        plane = step // halves
        half_tile = step % halves
        for sub in range(pair):
            tile = half_tile * pair + sub
            ahead = step if sub + 1 < pair else plane * halves + (half_tile + 1) % halves
            for direction in directions:
                narrow = direction in NARROW
                links = (narrow_links if narrow else load_links)(
                    u_ref, direction, tile * planes + plane, spots
                )
                for at in range(0, count, GROUP):

                    def part(where, turn, k):
                        row = k // 3 * count + at
                        return lhs_ref[where, turn * 3 + k % 3, row : row + GROUP]

                    if direction == 0:
                        vec = [part(step + halves, sub, k) for k in range(6)]
                    elif direction == 1:
                        vec = [
                            pltpu.roll(
                                jnp.where(spills, part(ahead, (sub + 1) % pair, k), part(step, sub, k)), LANES - LZ, 1
                            )
                            for k in range(6)
                        ]
                    else:
                        vec = [
                            jnp.where(
                                wraps,
                                pltpu.roll(part(step, sub, k), LZ - 1, 1),
                                pltpu.roll(part(step, sub, k), LANES - 1, 1),
                            )
                            for k in range(6)
                        ]
                    if narrow:
                        outs = narrow_product(links, vec[:3], vec[3:])
                    else:
                        wide = [piece.astype(F32) for piece in vec]
                        pieces = [[piece[eight : eight + 8] for piece in wide] for eight in (0, 8)]
                        low, high = [link_product(links, piece[:3], piece[3:]) for piece in pieces]
                        outs = [
                            [
                                jnp.concatenate([low[half][colour], high[half][colour]], axis=0).astype(BF16)
                                for colour in range(3)
                            ]
                            for half in range(2)
                        ]
                    for half in range(2):
                        row = (direction * 2 + half) * count + at
                        for colour in range(3):
                            op_ref[slot, sub * 3 + colour, row : row + GROUP] = outs[half][colour]

    def multiply(step, slot, directions):
        fixed = joined([lhs_ref[step, k] for k in range(3 * pair)])
        low = min(directions) * 2 * count
        high = (max(directions) + 1) * 2 * count
        moving = joined([op_ref[slot, k, low:high] for k in range(3 * pair)])
        got = nt_dot(jnp.concatenate([fixed, moving], axis=0), fixed)
        g_ref[step // halves] += got[: 2 * count]
        acc_ref[low:high, :] += got[2 * count :]

    every, side = (0, 1, 2), (1, 2)
    inner = steps - halves
    elementwise(inner, 0, side)
    for step in range(inner + 1, steps):
        multiply(step - 1, (step - 1) & 1, side)
        elementwise(step, step & 1, side)
    multiply(steps - 1, (steps - 1) & 1, side)
    elementwise(0, 0, every)

    for step in range(1, inner):
        multiply(step - 1, (step - 1) & 1, every)
        elementwise(step, step & 1, every)
    multiply(inner - 1, (inner - 1) & 1, every)
    fill_table(groups, slots, empty, owner_ref, elem_ref, source_ref, spin_ref, table_ref)

    first = lax.axis_index("space") * planes
    total_re = jnp.zeros((count, count), F32)
    total_im = jnp.zeros((count, count), F32)
    for plane in range(planes):
        real, imag = paired(g_ref[plane], count)
        cosine = phase_ref[first + plane]
        sine = phase_ref[lx + first + plane]
        total_re += cosine * real - sine * imag
        total_im += cosine * imag + sine * real
    sums_ref[0, 0] = total_re
    sums_ref[0, 1] = -total_im
    for direction in range(3):
        grid = acc_ref[direction * 2 * count : (direction + 1) * 2 * count, :]
        real, imag = anti(*paired(grid, count))
        sums_ref[direction + 1, 0] = real
        sums_ref[direction + 1, 1] = imag
    for half in range(halves):
        rim_lhs_ref[half] = lhs_ref[half]


def gram(x, u, phases, tables, count, tiles, planes, lx, groups, slots, empty):
    spots = tiles * planes
    pair = 2
    steps = planes * (tiles // pair)
    return pl.pallas_call(
        partial(gram_kernel, count, tiles, planes, lx, groups, slots, empty),
        in_specs=[vspec()] * 2 + [sspec()] + [vspec()] * 4,
        out_specs=[vspec()] * 3,
        out_shape=[
            jax.ShapeDtypeStruct((OPS, 2, count, count), F32),
            jax.ShapeDtypeStruct((tiles // pair, 3 * pair, 2 * count, LANES), BF16),
            jax.ShapeDtypeStruct((1, LANES), jnp.int32),
        ],
        scratch_shapes=[
            VMEM((steps, 3 * pair, 2 * count, LANES), BF16),
            VMEM((2, 3 * pair, 6 * count, LANES), BF16),
            VMEM((6 * count, 2 * count), F32),
            VMEM((planes, 2 * count, 2 * count), F32),
            VMEM((GROUP * spots, GROUP * spots), BF16),
        ],
        compiler_params=limit(26),
        cost_estimate=cost(8 * 10**9, 5 * 10**6),
        name="gram",
    )(x, u, phases, *tables)


def edge_kernel(count, rows, cores, halo_ref, lhs_ref, sums_ref, keep_ref, send_ref, tot_ref):
    total = None
    for half in range(halo_ref.shape[0]):
        sides = [joined([ref[half, k] for k in range(ref.shape[1])]) for ref in (halo_ref, lhs_ref)]
        got = nt_dot(*sides)
        total = got if total is None else total + got
    real = total[:count, :count] + total[count:, count:]
    imag = total[:count, count:] - total[count:, :count]
    tot_ref[0] = 0.5 * (real - real.T)
    tot_ref[1] = 0.5 * (imag + imag.T)
    mine = lax.axis_index("space") & (cores - 1)
    for chip in range(count // (rows * cores)):
        for which, ref in ((mine, keep_ref), (1 - mine, send_ref)):
            at = pl.multiple_of((chip * cores + which) * rows, rows)
            for op in range(OPS):
                for half in range(2):
                    piece = sums_ref[op, half, pl.ds(at, rows), :]
                    if op == 1:
                        piece = piece + tot_ref[half, pl.ds(at, rows), :]
                    ref[chip, op, half] = piece


def edge(halo, rim_lhs, sums, count, rows, cores):
    shape = jax.ShapeDtypeStruct((count // (rows * cores), OPS, 2, rows, count), F32)
    return pl.pallas_call(
        partial(edge_kernel, count, rows, cores),
        in_specs=[vspec()] * 3,
        out_specs=[vspec(), vspec()],
        out_shape=[shape, shape],
        scratch_shapes=[VMEM((2, count, count), F32)],
        compiler_params=limit(8),
        cost_estimate=cost(10**9, 3 * 10**6),
        name="edge",
    )(halo, rim_lhs, sums)


def split_sum(block):
    high = block[0:1].astype(BF16)
    low = (block[0:1] - high.astype(F32)).astype(BF16)
    return jnp.concatenate([high, low, block[1:].astype(BF16)], axis=0)


def fold_kernel(chips, cores, keep_ref, got_ref, own_ref, *out_refs):
    me = lax.axis_index("space") // cores
    own_ref[...] = keep_ref[me] + got_ref[me]
    for step in range(1, chips):
        to = me ^ step
        out_refs[step - 1][...] = split_sum(keep_ref[to] + got_ref[to])


def fold(keep, got, cores):
    chips = keep.shape[0]
    shape = keep.shape[1:]
    sent = jax.ShapeDtypeStruct((shape[0] + 1,) + shape[1:], BF16)
    return pl.pallas_call(
        partial(fold_kernel, chips, cores),
        in_specs=[vspec()] * 2,
        out_specs=[vspec()] * chips,
        out_shape=[jax.ShapeDtypeStruct(shape, F32)] + [sent] * (chips - 1),
        compiler_params=limit(4),
        cost_estimate=cost(10**6, 10**6),
        name="fold",
    )(keep, got)


def total_kernel(own_ref, *refs):
    total_ref = refs[-1]
    first = own_ref[0:1]
    rest = own_ref[1:]
    for ref in refs[:-1]:
        first = first + (ref[0:1].astype(F32) + ref[1:2].astype(F32))
        rest = rest + ref[2:].astype(F32)
    total_ref[0:1] = first.astype(BF16)
    total_ref[1:] = rest.astype(BF16)


def total_rows(parts):
    return pl.pallas_call(
        total_kernel,
        in_specs=[vspec()] * len(parts),
        out_specs=vspec(),
        out_shape=jax.ShapeDtypeStruct(parts[0].shape, BF16),
        compiler_params=limit(4),
        cost_estimate=cost(10**6, 10**6),
        name="total",
    )(*parts)


def dress_kernel(groups, slots, taus, rows, count, table_ref, per_ref, *refs):
    slab_refs = refs[:groups]
    out_ref, lhs_ref, prod_ref = refs[groups:]
    me = lax.axis_index("tm")
    for step in range(groups):
        group = me ^ step
        for op in range(OPS):
            at = pl.multiple_of((group * OPS + op) * rows, rows)
            lhs_ref[pl.ds(at, rows), 0:count] = slab_refs[step][op, 0]
            lhs_ref[pl.ds(at, rows), count : 2 * count] = slab_refs[step][op, 1]
    left = lhs_ref[...]
    for tau in range(taus):
        real, imag = per_ref[tau, 0], per_ref[tau, 1]
        right = jnp.concatenate(
            [jnp.concatenate([real, imag], axis=1), jnp.concatenate([-imag, real], axis=1)], axis=0
        )
        got = jnp.dot(left, right, preferred_element_type=F32).astype(BF16)
        for piece in range(groups * OPS):
            prod_ref[tau * groups * OPS + piece] = got[piece * rows : (piece + 1) * rows]
    prod_ref[taus * groups * OPS] = jnp.zeros((rows, 2 * count), BF16)
    for group in range(groups):
        for slot in range(slots):
            piece = prod_ref[table_ref[0, group * slots + slot]]
            out_ref[group, slot, 0] = piece[:, :count]
            out_ref[group, slot, 1] = piece[:, count:]


def dress(table, per, slabs, groups, slots, rows, count):
    taus = per.shape[0]
    return pl.pallas_call(
        partial(dress_kernel, groups, slots, taus, rows, count),
        in_specs=[sspec(), vspec()] + [vspec()] * groups,
        out_specs=vspec(),
        out_shape=jax.ShapeDtypeStruct((groups, slots, 2, rows, count), BF16),
        scratch_shapes=[
            VMEM((groups * OPS * rows, 2 * count), BF16),
            VMEM((taus * groups * OPS + 1, rows, 2 * count), BF16),
        ],
        compiler_params=limit(8),
        cost_estimate=cost(10**9, 2 * 10**6),
        name="dress",
    )(table, per, *slabs)


def fast_shards(eigvecs, gauge_links, perambulator, job_owner, job_elemental, job_source, job_spin):
    count = eigvecs.shape[1]
    planes, sites = eigvecs.shape[4], eigvecs.shape[5]
    tiles = sites // LANES
    space_size = lax.axis_size("space")
    groups = lax.axis_size("tm")
    lx = planes * space_size
    rows = count // space_size
    slots = 3 * ((JOB_DEV + groups - 1) // groups)
    cores = 2

    def tiled(field):
        head = field.shape[:-2]
        order = tuple(range(len(head))) + (len(head) + 1, len(head), len(head) + 2)
        split = field.reshape(head + (planes, tiles, LANES))
        return split.transpose(order).reshape(-1, LANES)

    x = tiled(eigvecs)
    u = tiled(gauge_links)
    angle = 2.0 * math.pi / lx * np.arange(lx)
    phases = jnp.asarray(np.concatenate([np.cos(angle), np.sin(angle)]).astype(np.float32))

    per = perambulator.reshape(-1, 2, count, count)
    empty = per.shape[0] * groups * OPS
    x = pltpu.with_memory_space_constraint(x, pltpu.HBM)
    u = pltpu.with_memory_space_constraint(u, pltpu.HBM)
    rim, x, u = rim_plane(x, u, count, tiles, planes)
    halo = lax.ppermute(rim, "space", [(i, (i + 1) % space_size) for i in range(space_size)])
    tables = [job.reshape(1, -1) for job in (job_owner, job_elemental, job_source, job_spin)]
    sums, rim_lhs, table = gram(
        x, u, phases, tables, count, tiles, planes, lx, groups, slots, empty
    )
    keep, send = edge(halo, rim_lhs, sums, count, rows, cores)
    got = lax.ppermute(send, "space", [(i, i ^ 1) for i in range(space_size)])
    parts = fold(keep, got, cores)
    summed = [parts[0]]
    for step in range(1, space_size // cores):
        summed.append(
            lax.ppermute(parts[step], "space", [(i, i ^ (step * cores)) for i in range(space_size)])
        )
    own = total_rows(summed)
    slabs = [own]
    for step in range(1, groups):
        slabs.append(lax.ppermute(own, "tm", [(i, i ^ step) for i in range(groups)]))
    return dress(table, per, slabs, groups, slots, rows, count)[None]


def passed_along(shard, axis, by):
    count = lax.axis_size(axis)
    return lax.ppermute(shard, axis, [(i, (i + by) % count) for i in range(count)])


def shifted_sites(lattice_field, direction, offset):
    shaped = lattice_field.reshape(lattice_field.shape[:-1] + (LY, LZ))
    rolled = jnp.roll(shaped, -offset, axis=direction - 4)
    return rolled.reshape(lattice_field.shape)


def apply_link(link_field, vectors):
    total_re = None
    total_im = None
    for colour in range(3):
        link_re = link_field[0, :, colour][None]
        link_im = link_field[1, :, colour][None]
        vector_re = vectors[:, 0, colour][:, None]
        vector_im = vectors[:, 1, colour][:, None]
        part_re = link_re * vector_re - link_im * vector_im
        part_im = link_re * vector_im + link_im * vector_re
        if colour == 0:
            total_re, total_im = (part_re, part_im)
        else:
            total_re = total_re + part_re
            total_im = total_im + part_im
    return jnp.stack([total_re, total_im], axis=1)


def stacked_form(vectors):
    vector_count = vectors.shape[0]
    swapped = jnp.concatenate([-vectors[:, 1:2], vectors[:, 0:1]], axis=1)
    return jnp.concatenate(
        [vectors.reshape(vector_count, -1), swapped.reshape(vector_count, -1)], axis=0
    )


def paired_gram(stacked, lattice_field):
    vector_count = lattice_field.shape[0]
    flat_field = lattice_field.astype(jnp.bfloat16).reshape(vector_count, -1)
    product = lax.dot_general(
        stacked, flat_field, (((1,), (1,)), ((), ())), preferred_element_type=jnp.float32
    )
    return product.reshape(2, vector_count, vector_count)


def twisted_field(vectors, xcoord):
    phase_angle = 2.0 * math.pi / (vectors.shape[3] * lax.axis_size("space")) * xcoord
    cosine = jnp.cos(phase_angle)[:, None]
    sine_part = jnp.sin(phase_angle)[:, None]
    real_part = cosine * vectors[:, 0] + sine_part * vectors[:, 1]
    imag_part = cosine * vectors[:, 1] - sine_part * vectors[:, 0]
    return jnp.stack([real_part, imag_part], axis=1)


def antihermitian(paired):
    return 0.5 * jnp.stack([paired[0] - paired[0].T, paired[1] + paired[1].T], axis=0)


def plain_shards(eigvecs, gauge_links, perambulator, job_owner, job_elemental, job_source, job_spin):
    slice_count = eigvecs.shape[0]
    vector_count = eigvecs.shape[1]
    planes = eigvecs.shape[4]
    space_size = lax.axis_size("space")
    group_count = lax.axis_size("tm")
    row_count = vector_count // space_size
    capacity = 3 * ((JOB_DEV + group_count - 1) // group_count)
    xcoord = (lax.axis_index("space") * planes + jnp.arange(planes, dtype=jnp.int32)).astype(
        jnp.float32
    )
    upper_plane = passed_along(eigvecs[:, :, :, :, 0:1], "space", -1)
    low_vectors = eigvecs[0]
    vectors = low_vectors.astype(jnp.float32)
    stacked = stacked_form(low_vectors)
    results = [paired_gram(stacked, twisted_field(vectors, xcoord))]
    for direction in (1, 2, 3):
        link_field = gauge_links[0, direction - 1]
        if direction == 1:
            upper_rim = upper_plane[0].astype(jnp.float32)
            above_field = jnp.concatenate([vectors[:, :, :, 1:], upper_rim], axis=3)
        else:
            above_field = shifted_sites(vectors, direction, 1)
        forward = apply_link(link_field, above_field)
        results.append(antihermitian(paired_gram(stacked, forward)))
    partial_list = [jnp.stack(results, axis=0)]
    partial_value = jnp.stack(partial_list, axis=0)
    summed = lax.psum(partial_value, "space")
    own_rows = lax.dynamic_slice_in_dim(summed, lax.axis_index("space") * row_count, row_count, 3)
    slab_table = own_rows.astype(jnp.bfloat16).reshape(
        slice_count * OPS, 2 * row_count * vector_count
    )
    owners = job_owner[:, 0].reshape(group_count, -1)
    elements = job_elemental.reshape(group_count, -1)
    position = jnp.arange(owners.shape[1], dtype=jnp.int32)
    earlier = position[None, :] < position[:, None]
    same_owner = owners[:, :, None] == owners[:, None, :]
    slot_rank = jnp.sum(jnp.where(same_owner & earlier[None], 1, 0), axis=2).astype(jnp.int32)
    own_group = lax.axis_index("tm")
    slot_count = group_count * capacity
    live_jobs = owners == own_group
    slot_match = live_jobs[:, None, :] & (
        slot_rank[:, None, :] == jnp.arange(capacity, dtype=jnp.int32)[None, :, None]
    )
    sender_owners = lax.dynamic_index_in_dim(owners, own_group, 0, keepdims=False)
    sender_ranks = lax.dynamic_index_in_dim(slot_rank, own_group, 0, keepdims=False)
    sender_elements = lax.dynamic_index_in_dim(elements, own_group, 0, keepdims=False)
    slot_ids = sender_owners * capacity + sender_ranks
    slot_hot = (jnp.arange(slot_count, dtype=jnp.int32)[:, None] == slot_ids[None, :]).astype(
        jnp.float32
    )
    elem_hot = (
        sender_elements[:, None] == jnp.arange(slice_count * OPS, dtype=jnp.int32)[None, :]
    ).astype(jnp.float32)
    picker = jnp.dot(slot_hot, elem_hot, precision=lax.Precision.HIGHEST).astype(jnp.bfloat16)
    outgoing = jnp.dot(picker, slab_table, preferred_element_type=jnp.float32).astype(jnp.bfloat16)
    outgoing = outgoing.reshape(group_count, capacity, 2, row_count, vector_count)
    received = lax.all_to_all(outgoing, "tm", split_axis=0, concat_axis=0, tiled=True)
    block_index = job_source.reshape(group_count, -1) * SPIN + job_spin.reshape(group_count, -1)
    tau_index = jnp.sum(jnp.where(slot_match, block_index[:, None, :], 0), axis=2)
    blocks = perambulator.reshape(-1, 2 * vector_count, vector_count)
    chosen = jnp.take(blocks, tau_index.reshape(-1), axis=0)
    slab_rows = received.reshape(slot_count, 2, row_count, vector_count)
    real_rows = jnp.concatenate([slab_rows[:, 0], -slab_rows[:, 1]], axis=-1)
    imag_rows = jnp.concatenate([slab_rows[:, 1], slab_rows[:, 0]], axis=-1)
    left_side = jnp.stack([real_rows, imag_rows], axis=1).reshape(
        slot_count, 2 * row_count, 2 * vector_count
    )
    dressed = lax.dot_general(
        left_side, chosen, (((2,), (1,)), ((0,), (0,))), preferred_element_type=jnp.float32
    )
    return dressed.astype(jnp.bfloat16).reshape(
        1, group_count, capacity, 2, row_count, vector_count
    )


def shards(*args):
    eigvecs = args[0]
    count, planes, sites = eigvecs.shape[1], eigvecs.shape[4], eigvecs.shape[5]
    space_size, groups = lax.axis_size("space"), lax.axis_size("tm")
    whole_tiles = sites % (2 * LANES) == 0 and count == LANES and planes * (sites // LANES) == GROUP
    fits = groups * 3 * ((JOB_DEV + groups - 1) // groups) < LANES
    powers = space_size & (space_size - 1) == 0 and groups & (groups - 1) == 0
    small = space_size * GROUP == count and groups <= 8 and args[3].shape[0] <= LANES
    if whole_tiles and fits and powers and small and eigvecs.shape[0] == 1:
        return fast_shards(*args)
    return plain_shards(*args)


def solution(mesh):
    return jax.shard_map(
        shards,
        mesh=mesh,
        in_specs=(
            P("tm", None, None, None, "space", None),
            P("tm", None, None, None, None, "space", None),
            P("tm", None, None, None, None),
            P(),
            P(),
            P(),
            P(),
        ),
        out_specs=P("tm", None, None, None, "space", None),
        check_vma=False,
    )
```

```python
import math
from functools import partial

import numpy as np
import jax
import jax.numpy as jnp
from jax import lax
from jax.experimental import pallas as pl
from jax.experimental.pallas import tpu as pltpu
from jax.sharding import PartitionSpec as P

LY = 16
LZ = 32
OPS = 4
SPIN = 4
JOB_DEV = 24
LANES = 128
GROUP = 16
NARROW = (1, 2)
F32 = jnp.float32
BF16 = jnp.bfloat16
VMEM = pltpu.VMEM
SMEM = pltpu.SMEM


def vspec():
    return pl.BlockSpec(memory_space=VMEM)


def sspec():
    return pl.BlockSpec(memory_space=SMEM)


def cost(flops, moved):
    return pl.CostEstimate(flops=flops, bytes_accessed=moved, transcendentals=0)


def limit(mebibytes):
    return pltpu.CompilerParams(vmem_limit_bytes=mebibytes * 2**20)


def pick_matrix(rows, cols, source_of):
    row = lax.broadcasted_iota(jnp.int32, (rows, cols), 0)
    col = lax.broadcasted_iota(jnp.int32, (rows, cols), 1)
    return jnp.where(col == source_of(row), 1.0, 0.0).astype(BF16)


def joined(pieces):
    return jnp.concatenate(pieces, axis=1)


def nt_dot(left, right):
    return lax.dot_general(left, right, (((1,), (1,)), ((), ())), preferred_element_type=F32)


def rim_kernel(tiles, planes, start, leads, x_hbm, u_hbm, *refs):
    if leads:
        out_ref, x_ref, link_ref, u_ref, pick_ref, sems = refs
    else:
        link_ref, out_ref, x_ref, u_ref, pick_ref, sems = refs
    spots = tiles * planes
    pair = 2
    part_count = out_ref.shape[2] // 2
    chunk = GROUP * 6 * spots
    chunks = part_count // GROUP
    rows_of = [pl.ds(g * chunk, chunk) for g in range(chunks)]
    copies = [
        pltpu.make_async_copy(x_hbm.at[pl.ds((start + g) * chunk, chunk)], x_ref.at[rows], sems.at[g])
        for g, rows in enumerate(rows_of)
    ]
    link_copy = pltpu.make_async_copy(u_hbm.at[pl.ds(0, u_ref.shape[0])], u_ref, sems.at[chunks])
    for copy in [link_copy] + copies if leads else copies + [link_copy]:
        copy.start()

    def source(row):
        return (row & (GROUP - 1)) * spots + (row // GROUP) * planes + planes - 1

    pick_ref[...] = pick_matrix(tiles * GROUP, GROUP * spots, source)
    if leads:
        link_copy.wait()
        for tile in range(tiles):
            flat = adjoint(load_rows(u_ref, 0, tile * planes + planes - 1, spots))
            for k, link in enumerate(flat):
                link_ref[tile, k] = link
    chosen = pick_ref[...]
    for g in range(chunks):
        copies[g].wait()
        block = x_ref[g * chunk : (g + 1) * chunk, :].reshape(GROUP, 6, spots, LANES)
        taken = []
        for part in range(0, 6, 2):
            rows = joined([block[:, part + k].reshape(GROUP * spots, LANES) for k in range(2)])
            got = jnp.dot(chosen, rows, preferred_element_type=F32)
            taken += [got[:, :LANES], got[:, LANES:]]
        for tile in range(tiles):
            links = [[[link_ref[tile, (p * 3 + r) * 3 + c] for c in range(3)] for r in range(3)] for p in range(3)]
            outs = []
            for eight in (0, 8):
                at = tile * GROUP + eight
                vec = [part[at : at + 8] for part in taken]
                outs.append(link_product(links, vec[:3], vec[3:]))
            for half in range(2):
                row = half * part_count + g * GROUP
                for colour in range(3):
                    both = jnp.concatenate([outs[0][half][colour], outs[1][half][colour]], axis=0)
                    out_ref[tile // pair, (tile % pair) * 3 + colour, row : row + GROUP] = both.astype(BF16)
    if not leads:
        link_copy.wait()


def rim_plane(x, u, links, count, tiles, planes):
    spots = tiles * planes
    pair = 2
    leads = links is None
    part_count = count // 2
    chunks = part_count // GROUP
    hbm = pl.BlockSpec(memory_space=pltpu.HBM)
    out_shape = [
        jax.ShapeDtypeStruct((tiles // pair, 3 * pair, 2 * part_count, LANES), BF16),
        jax.ShapeDtypeStruct((x.shape[0] // 2, LANES), BF16),
    ]
    scratch = [
        VMEM((tiles * GROUP, GROUP * spots), BF16),
        pltpu.SemaphoreType.DMA((chunks + 1,)),
    ]
    if leads:
        out_shape.append(jax.ShapeDtypeStruct((tiles, 27, 8, LANES), F32))
        scratch = [VMEM((18 * spots, LANES), F32)] + scratch
    else:
        out_shape.append(jax.ShapeDtypeStruct(u.shape, F32))
    return pl.pallas_call(
        partial(rim_kernel, tiles, planes, 0 if leads else chunks, leads),
        in_specs=[hbm, hbm] + ([] if leads else [vspec()]),
        out_specs=[vspec()] * 3,
        out_shape=out_shape,
        scratch_shapes=scratch,
        compiler_params=limit(6),
        cost_estimate=cost(10**8, 2 * 10**6),
        name="rim" if leads else "rest",
    )(x, u, *([] if leads else [links]))


def link_product(links, vec_re, vec_im):
    plus = [vec_re[c] + vec_im[c] for c in range(3)]
    outs_re, outs_im = [], []
    for row in range(3):
        link_re, link_less, link_more = links[0][row], links[1][row], links[2][row]
        one = link_re[0] * plus[0] + link_re[1] * plus[1] + link_re[2] * plus[2]
        two = link_less[0] * vec_re[0] + link_less[1] * vec_re[1] + link_less[2] * vec_re[2]
        three = link_more[0] * vec_im[0] + link_more[1] * vec_im[1] + link_more[2] * vec_im[2]
        outs_re.append(one - three)
        outs_im.append(one + two)
    return outs_re, outs_im


def narrow_product(links, vec_re, vec_im):
    real, imag = links
    outs_re, outs_im = [], []
    for row in range(3):
        ones = [real[row][c] * vec_re[c] - imag[row][c] * vec_im[c] for c in range(3)]
        twos = [real[row][c] * vec_im[c] + imag[row][c] * vec_re[c] for c in range(3)]
        outs_re.append(ones[0] + ones[1] + ones[2])
        outs_im.append(twos[0] + twos[1] + twos[2])
    return outs_re, outs_im


def narrow_links(u_ref, direction, spot, spots):
    def one(part, row, col):
        at = (((direction * 2 + part) * 3 + row) * 3 + col) * spots + spot
        return jnp.broadcast_to(u_ref[pl.ds(at, 1), :], (GROUP, LANES)).astype(BF16)

    return [[[one(part, row, col) for col in range(3)] for row in range(3)] for part in range(2)]


def load_rows(u_ref, direction, spot, spots):
    def one(part, row, col):
        at = (((direction * 2 + part) * 3 + row) * 3 + col) * spots + spot
        return jnp.broadcast_to(u_ref[pl.ds(at, 1), :], (8, LANES))

    return [[[one(part, row, col) for col in range(3)] for row in range(3)] for part in range(2)]


def load_links(u_ref, direction, spot, spots):
    real, imag = load_rows(u_ref, direction, spot, spots)
    less = [[imag[row][col] - real[row][col] for col in range(3)] for row in range(3)]
    more = [[imag[row][col] + real[row][col] for col in range(3)] for row in range(3)]
    return real, less, more


def adjoint(grid):
    real, imag = grid
    order = [(row, col) for row in range(3) for col in range(3)]
    return (
        [real[col][row] for row, col in order]
        + [-imag[col][row] - real[col][row] for row, col in order]
        + [real[col][row] - imag[col][row] for row, col in order]
    )


def fill_table(groups, slots, empty, owner_ref, elem_ref, source_ref, spin_ref, table_ref):
    total = owner_ref.shape[1]
    jobs = total // groups
    row = lax.broadcasted_iota(jnp.int32, (total, total), 0)
    col = lax.broadcasted_iota(jnp.int32, (total, total), 1)

    def group_of(index):
        return sum((index >= group * jobs).astype(jnp.int32) for group in range(1, groups))

    live = jnp.where(owner_ref[...] == lax.axis_index("tm"), 1.0, 0.0)
    product = source_ref[...] * (SPIN * groups * OPS) + spin_ref[...] * (groups * OPS) + elem_ref[...]

    def column(mask, values):
        wide = jnp.broadcast_to(values.astype(F32), (total, total))
        return jnp.sum(jnp.where(mask, wide, 0.0), axis=1, keepdims=True)

    rank = column((col < row) & (group_of(col) == group_of(row)), live)
    alive = column(col == row, live)
    value = column(col == row, product)
    at_row = lax.broadcasted_iota(jnp.int32, (total, LANES), 0)
    at_col = lax.broadcasted_iota(jnp.int32, (total, LANES), 1)
    group = group_of(at_row).astype(F32)
    place = jnp.where(alive > 0.5, group * slots + rank, -1.0)
    found = at_col.astype(F32) == place
    picked = jnp.sum(jnp.where(found, value + group * OPS - empty, 0.0), axis=0, keepdims=True)
    table_ref[...] = (picked + empty).astype(jnp.int32)


def paired(grid, count):
    real = grid[:count, :count] + grid[count:, count:]
    imag = grid[count:, :count] - grid[:count, count:]
    return real, imag


def anti(real, imag):
    return 0.5 * (real.T - real), 0.5 * (imag.T + imag)


def gram_kernel(
    count, tiles, planes, lx, groups, slots, empty,
    low_ref, high_ref, u_ref, phase_ref, owner_ref, elem_ref, source_ref, spin_ref,
    sums_ref, rim_lhs_ref, table_ref,
    lhs_ref, op_ref, acc_ref, g_ref, pick_ref,
):
    spots = tiles * planes
    pair = 2
    halves = tiles // pair
    steps = planes * halves

    def source(row):
        spot = row // GROUP
        return (row & (GROUP - 1)) * spots + (spot % tiles) * planes + spot // tiles

    pick_ref[...] = pick_matrix(GROUP * spots, GROUP * spots, source)
    acc_ref[...] = jnp.zeros_like(acc_ref)
    g_ref[...] = jnp.zeros_like(g_ref)

    chosen = pick_ref[...]
    for at in range(0, count, GROUP):
        x_ref, near = (low_ref, at) if at < count // 2 else (high_ref, at - count // 2)
        block = x_ref[near * 6 * spots : (near + GROUP) * 6 * spots, :].reshape(GROUP, 6, spots, LANES)
        for first in range(0, 6, 2):
            rows = jnp.concatenate(
                [block[:, first + k].reshape(GROUP * spots, LANES) for k in range(2)], axis=1
            )
            taken = jnp.dot(chosen, rows, preferred_element_type=F32)
            for k in range(2):
                part = first + k
                half, colour = part // 3, part % 3
                for spot in range(spots):
                    piece = taken[spot * GROUP : (spot + 1) * GROUP, k * LANES : (k + 1) * LANES]
                    plane, tile = spot // tiles, spot % tiles
                    lhs_ref[
                        plane * halves + tile // pair,
                        (tile % pair) * 3 + colour,
                        half * count + at : half * count + at + GROUP,
                    ] = piece.astype(BF16)

    lane = lax.broadcasted_iota(jnp.int32, (GROUP, LANES), 1)
    wraps = (lane & (LZ - 1)) == LZ - 1
    spills = lane < LZ

    def elementwise(step, slot, directions):
        plane = step // halves
        half_tile = step % halves
        for sub in range(pair):
            tile = half_tile * pair + sub
            ahead = step if sub + 1 < pair else plane * halves + (half_tile + 1) % halves
            for direction in directions:
                narrow = direction in NARROW
                links = (narrow_links if narrow else load_links)(
                    u_ref, direction, tile * planes + plane, spots
                )
                for at in range(0, count, GROUP):

                    def part(where, turn, k):
                        row = k // 3 * count + at
                        return lhs_ref[where, turn * 3 + k % 3, row : row + GROUP]

                    if direction == 0:
                        vec = [part(step + halves, sub, k) for k in range(6)]
                    elif direction == 1:
                        vec = [
                            pltpu.roll(
                                jnp.where(spills, part(ahead, (sub + 1) % pair, k), part(step, sub, k)), LANES - LZ, 1
                            )
                            for k in range(6)
                        ]
                    else:
                        vec = [
                            jnp.where(
                                wraps,
                                pltpu.roll(part(step, sub, k), LZ - 1, 1),
                                pltpu.roll(part(step, sub, k), LANES - 1, 1),
                            )
                            for k in range(6)
                        ]
                    if narrow:
                        outs = narrow_product(links, vec[:3], vec[3:])
                    else:
                        wide = [piece.astype(F32) for piece in vec]
                        pieces = [[piece[eight : eight + 8] for piece in wide] for eight in (0, 8)]
                        low, high = [link_product(links, piece[:3], piece[3:]) for piece in pieces]
                        outs = [
                            [
                                jnp.concatenate([low[half][colour], high[half][colour]], axis=0).astype(BF16)
                                for colour in range(3)
                            ]
                            for half in range(2)
                        ]
                    for half in range(2):
                        row = (direction * 2 + half) * count + at
                        for colour in range(3):
                            op_ref[slot, sub * 3 + colour, row : row + GROUP] = outs[half][colour]

    def multiply(step, slot, directions):
        fixed = joined([lhs_ref[step, k] for k in range(3 * pair)])
        low = min(directions) * 2 * count
        high = (max(directions) + 1) * 2 * count
        moving = joined([op_ref[slot, k, low:high] for k in range(3 * pair)])
        got = nt_dot(jnp.concatenate([fixed, moving], axis=0), fixed)
        g_ref[step // halves] += got[: 2 * count]
        acc_ref[low:high, :] += got[2 * count :]

    every, side = (0, 1, 2), (1, 2)
    inner = steps - halves
    elementwise(inner, 0, side)
    for step in range(inner + 1, steps):
        multiply(step - 1, (step - 1) & 1, side)
        elementwise(step, step & 1, side)
    multiply(steps - 1, (steps - 1) & 1, side)
    elementwise(0, 0, every)

    for step in range(1, inner):
        multiply(step - 1, (step - 1) & 1, every)
        elementwise(step, step & 1, every)
    multiply(inner - 1, (inner - 1) & 1, every)
    fill_table(groups, slots, empty, owner_ref, elem_ref, source_ref, spin_ref, table_ref)

    first = lax.axis_index("space") * planes
    total_re = jnp.zeros((count, count), F32)
    total_im = jnp.zeros((count, count), F32)
    for plane in range(planes):
        real, imag = paired(g_ref[plane], count)
        cosine = phase_ref[first + plane]
        sine = phase_ref[lx + first + plane]
        total_re += cosine * real - sine * imag
        total_im += cosine * imag + sine * real
    sums_ref[0, 0] = total_re
    sums_ref[0, 1] = -total_im
    for direction in range(3):
        grid = acc_ref[direction * 2 * count : (direction + 1) * 2 * count, :]
        real, imag = anti(*paired(grid, count))
        sums_ref[direction + 1, 0] = real
        sums_ref[direction + 1, 1] = imag
    for half in range(halves):
        rim_lhs_ref[half] = lhs_ref[half]


def gram(low, high, u, phases, tables, count, tiles, planes, lx, groups, slots, empty):
    spots = tiles * planes
    pair = 2
    steps = planes * (tiles // pair)
    return pl.pallas_call(
        partial(gram_kernel, count, tiles, planes, lx, groups, slots, empty),
        in_specs=[vspec()] * 3 + [sspec()] + [vspec()] * 4,
        out_specs=[vspec()] * 3,
        out_shape=[
            jax.ShapeDtypeStruct((OPS, 2, count, count), F32),
            jax.ShapeDtypeStruct((tiles // pair, 3 * pair, 2 * count, LANES), BF16),
            jax.ShapeDtypeStruct((1, LANES), jnp.int32),
        ],
        scratch_shapes=[
            VMEM((steps, 3 * pair, 2 * count, LANES), BF16),
            VMEM((2, 3 * pair, 6 * count, LANES), BF16),
            VMEM((6 * count, 2 * count), F32),
            VMEM((planes, 2 * count, 2 * count), F32),
            VMEM((GROUP * spots, GROUP * spots), BF16),
        ],
        compiler_params=limit(26),
        cost_estimate=cost(8 * 10**9, 5 * 10**6),
        name="gram",
    )(low, high, u, phases, *tables)


def edge_kernel(count, rows, cores, low_ref, high_ref, lhs_ref, sums_ref, keep_ref, send_ref, tot_ref):
    reals, imags = [], []
    for halo_ref in (low_ref, high_ref):
        total = None
        for half in range(halo_ref.shape[0]):
            sides = [joined([ref[half, k] for k in range(ref.shape[1])]) for ref in (halo_ref, lhs_ref)]
            got = nt_dot(*sides)
            total = got if total is None else total + got
        mid = total.shape[0] // 2
        reals.append(total[:mid, :count] + total[mid:, count:])
        imags.append(total[:mid, count:] - total[mid:, :count])
    real, imag = jnp.concatenate(reals, axis=0), jnp.concatenate(imags, axis=0)
    tot_ref[0] = 0.5 * (real - real.T)
    tot_ref[1] = 0.5 * (imag + imag.T)
    mine = lax.axis_index("space") & (cores - 1)
    for chip in range(count // (rows * cores)):
        for which, ref in ((mine, keep_ref), (1 - mine, send_ref)):
            at = pl.multiple_of((chip * cores + which) * rows, rows)
            for op in range(OPS):
                for half in range(2):
                    piece = sums_ref[op, half, pl.ds(at, rows), :]
                    if op == 1:
                        piece = piece + tot_ref[half, pl.ds(at, rows), :]
                    ref[chip, op, half] = piece


def edge(halos, rim_lhs, sums, count, rows, cores):
    shape = jax.ShapeDtypeStruct((count // (rows * cores), OPS, 2, rows, count), F32)
    return pl.pallas_call(
        partial(edge_kernel, count, rows, cores),
        in_specs=[vspec()] * 4,
        out_specs=[vspec(), vspec()],
        out_shape=[shape, shape],
        scratch_shapes=[VMEM((2, count, count), F32)],
        compiler_params=limit(8),
        cost_estimate=cost(10**9, 3 * 10**6),
        name="edge",
    )(*halos, rim_lhs, sums)


def split_sum(block):
    high = block[0:1].astype(BF16)
    low = (block[0:1] - high.astype(F32)).astype(BF16)
    return jnp.concatenate([high, low, block[1:].astype(BF16)], axis=0)


def fold_kernel(chips, cores, keep_ref, got_ref, own_ref, *out_refs):
    me = lax.axis_index("space") // cores
    own_ref[...] = keep_ref[me] + got_ref[me]
    for step in range(1, chips):
        to = me ^ step
        out_refs[step - 1][...] = split_sum(keep_ref[to] + got_ref[to])


def fold(keep, got, cores):
    chips = keep.shape[0]
    shape = keep.shape[1:]
    sent = jax.ShapeDtypeStruct((shape[0] + 1,) + shape[1:], BF16)
    return pl.pallas_call(
        partial(fold_kernel, chips, cores),
        in_specs=[vspec()] * 2,
        out_specs=[vspec()] * chips,
        out_shape=[jax.ShapeDtypeStruct(shape, F32)] + [sent] * (chips - 1),
        compiler_params=limit(4),
        cost_estimate=cost(10**6, 10**6),
        name="fold",
    )(keep, got)


def total_kernel(own_ref, *refs):
    total_ref = refs[-1]
    first = own_ref[0:1]
    rest = own_ref[1:]
    for ref in refs[:-1]:
        first = first + (ref[0:1].astype(F32) + ref[1:2].astype(F32))
        rest = rest + ref[2:].astype(F32)
    total_ref[0:1] = first.astype(BF16)
    total_ref[1:] = rest.astype(BF16)


def total_rows(parts):
    return pl.pallas_call(
        total_kernel,
        in_specs=[vspec()] * len(parts),
        out_specs=vspec(),
        out_shape=jax.ShapeDtypeStruct(parts[0].shape, BF16),
        compiler_params=limit(4),
        cost_estimate=cost(10**6, 10**6),
        name="total",
    )(*parts)


def dress_kernel(groups, slots, taus, rows, count, table_ref, per_ref, *refs):
    slab_refs = refs[:groups]
    out_ref, lhs_ref, prod_ref = refs[groups:]
    me = lax.axis_index("tm")
    for step in range(groups):
        group = me ^ step
        for op in range(OPS):
            at = pl.multiple_of((group * OPS + op) * rows, rows)
            lhs_ref[pl.ds(at, rows), 0:count] = slab_refs[step][op, 0]
            lhs_ref[pl.ds(at, rows), count : 2 * count] = slab_refs[step][op, 1]
    left = lhs_ref[...]
    for tau in range(taus):
        real, imag = per_ref[tau, 0], per_ref[tau, 1]
        right = jnp.concatenate(
            [jnp.concatenate([real, imag], axis=1), jnp.concatenate([-imag, real], axis=1)], axis=0
        )
        got = jnp.dot(left, right, preferred_element_type=F32).astype(BF16)
        for piece in range(groups * OPS):
            prod_ref[tau * groups * OPS + piece] = got[piece * rows : (piece + 1) * rows]
    prod_ref[taus * groups * OPS] = jnp.zeros((rows, 2 * count), BF16)
    for group in range(groups):
        for slot in range(slots):
            piece = prod_ref[table_ref[0, group * slots + slot]]
            out_ref[group, slot, 0] = piece[:, :count]
            out_ref[group, slot, 1] = piece[:, count:]


def dress(table, per, slabs, groups, slots, rows, count):
    taus = per.shape[0]
    return pl.pallas_call(
        partial(dress_kernel, groups, slots, taus, rows, count),
        in_specs=[sspec(), vspec()] + [vspec()] * groups,
        out_specs=vspec(),
        out_shape=jax.ShapeDtypeStruct((groups, slots, 2, rows, count), BF16),
        scratch_shapes=[
            VMEM((groups * OPS * rows, 2 * count), BF16),
            VMEM((taus * groups * OPS + 1, rows, 2 * count), BF16),
        ],
        compiler_params=limit(8),
        cost_estimate=cost(10**9, 2 * 10**6),
        name="dress",
    )(table, per, *slabs)


def fast_shards(eigvecs, gauge_links, perambulator, job_owner, job_elemental, job_source, job_spin):
    count = eigvecs.shape[1]
    planes, sites = eigvecs.shape[4], eigvecs.shape[5]
    tiles = sites // LANES
    space_size = lax.axis_size("space")
    groups = lax.axis_size("tm")
    lx = planes * space_size
    rows = count // space_size
    slots = 3 * ((JOB_DEV + groups - 1) // groups)
    cores = 2

    def tiled(field):
        head = field.shape[:-2]
        order = tuple(range(len(head))) + (len(head) + 1, len(head), len(head) + 2)
        split = field.reshape(head + (planes, tiles, LANES))
        return split.transpose(order).reshape(-1, LANES)

    x = tiled(eigvecs)
    u = tiled(gauge_links)
    angle = 2.0 * math.pi / lx * np.arange(lx)
    phases = jnp.asarray(np.concatenate([np.cos(angle), np.sin(angle)]).astype(np.float32))

    per = perambulator.reshape(-1, 2, count, count)
    empty = per.shape[0] * groups * OPS
    x = pltpu.with_memory_space_constraint(x, pltpu.HBM)
    u = pltpu.with_memory_space_constraint(u, pltpu.HBM)
    up = [(i, (i + 1) % space_size) for i in range(space_size)]
    rim, low, links = rim_plane(x, u, None, count, tiles, planes)
    halos = [lax.ppermute(rim, "space", up)]
    rim, high, u = rim_plane(x, u, links, count, tiles, planes)
    halos.append(lax.ppermute(rim, "space", up))
    tables = [job.reshape(1, -1) for job in (job_owner, job_elemental, job_source, job_spin)]
    sums, rim_lhs, table = gram(
        low, high, u, phases, tables, count, tiles, planes, lx, groups, slots, empty
    )
    keep, send = edge(halos, rim_lhs, sums, count, rows, cores)
    got = lax.ppermute(send, "space", [(i, i ^ 1) for i in range(space_size)])
    parts = fold(keep, got, cores)
    summed = [parts[0]]
    chips = space_size // cores
    for step in sorted(range(1, chips), key=lambda step: -bin(step).count("1")):
        summed.append(
            lax.ppermute(parts[step], "space", [(i, i ^ (step * cores)) for i in range(space_size)])
        )
    own = total_rows(summed)
    slabs = [own]
    for step in range(1, groups):
        slabs.append(lax.ppermute(own, "tm", [(i, i ^ step) for i in range(groups)]))
    return dress(table, per, slabs, groups, slots, rows, count)[None]


def passed_along(shard, axis, by):
    count = lax.axis_size(axis)
    return lax.ppermute(shard, axis, [(i, (i + by) % count) for i in range(count)])


def shifted_sites(lattice_field, direction, offset):
    shaped = lattice_field.reshape(lattice_field.shape[:-1] + (LY, LZ))
    rolled = jnp.roll(shaped, -offset, axis=direction - 4)
    return rolled.reshape(lattice_field.shape)


def apply_link(link_field, vectors):
    total_re = None
    total_im = None
    for colour in range(3):
        link_re = link_field[0, :, colour][None]
        link_im = link_field[1, :, colour][None]
        vector_re = vectors[:, 0, colour][:, None]
        vector_im = vectors[:, 1, colour][:, None]
        part_re = link_re * vector_re - link_im * vector_im
        part_im = link_re * vector_im + link_im * vector_re
        if colour == 0:
            total_re, total_im = (part_re, part_im)
        else:
            total_re = total_re + part_re
            total_im = total_im + part_im
    return jnp.stack([total_re, total_im], axis=1)


def stacked_form(vectors):
    vector_count = vectors.shape[0]
    swapped = jnp.concatenate([-vectors[:, 1:2], vectors[:, 0:1]], axis=1)
    return jnp.concatenate(
        [vectors.reshape(vector_count, -1), swapped.reshape(vector_count, -1)], axis=0
    )


def paired_gram(stacked, lattice_field):
    vector_count = lattice_field.shape[0]
    flat_field = lattice_field.astype(jnp.bfloat16).reshape(vector_count, -1)
    product = lax.dot_general(
        stacked, flat_field, (((1,), (1,)), ((), ())), preferred_element_type=jnp.float32
    )
    return product.reshape(2, vector_count, vector_count)


def twisted_field(vectors, xcoord):
    phase_angle = 2.0 * math.pi / (vectors.shape[3] * lax.axis_size("space")) * xcoord
    cosine = jnp.cos(phase_angle)[:, None]
    sine_part = jnp.sin(phase_angle)[:, None]
    real_part = cosine * vectors[:, 0] + sine_part * vectors[:, 1]
    imag_part = cosine * vectors[:, 1] - sine_part * vectors[:, 0]
    return jnp.stack([real_part, imag_part], axis=1)


def antihermitian(paired):
    return 0.5 * jnp.stack([paired[0] - paired[0].T, paired[1] + paired[1].T], axis=0)


def plain_shards(eigvecs, gauge_links, perambulator, job_owner, job_elemental, job_source, job_spin):
    slice_count = eigvecs.shape[0]
    vector_count = eigvecs.shape[1]
    planes = eigvecs.shape[4]
    space_size = lax.axis_size("space")
    group_count = lax.axis_size("tm")
    row_count = vector_count // space_size
    capacity = 3 * ((JOB_DEV + group_count - 1) // group_count)
    xcoord = (lax.axis_index("space") * planes + jnp.arange(planes, dtype=jnp.int32)).astype(
        jnp.float32
    )
    upper_plane = passed_along(eigvecs[:, :, :, :, 0:1], "space", -1)
    low_vectors = eigvecs[0]
    vectors = low_vectors.astype(jnp.float32)
    stacked = stacked_form(low_vectors)
    results = [paired_gram(stacked, twisted_field(vectors, xcoord))]
    for direction in (1, 2, 3):
        link_field = gauge_links[0, direction - 1]
        if direction == 1:
            upper_rim = upper_plane[0].astype(jnp.float32)
            above_field = jnp.concatenate([vectors[:, :, :, 1:], upper_rim], axis=3)
        else:
            above_field = shifted_sites(vectors, direction, 1)
        forward = apply_link(link_field, above_field)
        results.append(antihermitian(paired_gram(stacked, forward)))
    partial_list = [jnp.stack(results, axis=0)]
    partial_value = jnp.stack(partial_list, axis=0)
    summed = lax.psum(partial_value, "space")
    own_rows = lax.dynamic_slice_in_dim(summed, lax.axis_index("space") * row_count, row_count, 3)
    slab_table = own_rows.astype(jnp.bfloat16).reshape(
        slice_count * OPS, 2 * row_count * vector_count
    )
    owners = job_owner[:, 0].reshape(group_count, -1)
    elements = job_elemental.reshape(group_count, -1)
    position = jnp.arange(owners.shape[1], dtype=jnp.int32)
    earlier = position[None, :] < position[:, None]
    same_owner = owners[:, :, None] == owners[:, None, :]
    slot_rank = jnp.sum(jnp.where(same_owner & earlier[None], 1, 0), axis=2).astype(jnp.int32)
    own_group = lax.axis_index("tm")
    slot_count = group_count * capacity
    live_jobs = owners == own_group
    slot_match = live_jobs[:, None, :] & (
        slot_rank[:, None, :] == jnp.arange(capacity, dtype=jnp.int32)[None, :, None]
    )
    sender_owners = lax.dynamic_index_in_dim(owners, own_group, 0, keepdims=False)
    sender_ranks = lax.dynamic_index_in_dim(slot_rank, own_group, 0, keepdims=False)
    sender_elements = lax.dynamic_index_in_dim(elements, own_group, 0, keepdims=False)
    slot_ids = sender_owners * capacity + sender_ranks
    slot_hot = (jnp.arange(slot_count, dtype=jnp.int32)[:, None] == slot_ids[None, :]).astype(
        jnp.float32
    )
    elem_hot = (
        sender_elements[:, None] == jnp.arange(slice_count * OPS, dtype=jnp.int32)[None, :]
    ).astype(jnp.float32)
    picker = jnp.dot(slot_hot, elem_hot, precision=lax.Precision.HIGHEST).astype(jnp.bfloat16)
    outgoing = jnp.dot(picker, slab_table, preferred_element_type=jnp.float32).astype(jnp.bfloat16)
    outgoing = outgoing.reshape(group_count, capacity, 2, row_count, vector_count)
    received = lax.all_to_all(outgoing, "tm", split_axis=0, concat_axis=0, tiled=True)
    block_index = job_source.reshape(group_count, -1) * SPIN + job_spin.reshape(group_count, -1)
    tau_index = jnp.sum(jnp.where(slot_match, block_index[:, None, :], 0), axis=2)
    blocks = perambulator.reshape(-1, 2 * vector_count, vector_count)
    chosen = jnp.take(blocks, tau_index.reshape(-1), axis=0)
    slab_rows = received.reshape(slot_count, 2, row_count, vector_count)
    real_rows = jnp.concatenate([slab_rows[:, 0], -slab_rows[:, 1]], axis=-1)
    imag_rows = jnp.concatenate([slab_rows[:, 1], slab_rows[:, 0]], axis=-1)
    left_side = jnp.stack([real_rows, imag_rows], axis=1).reshape(
        slot_count, 2 * row_count, 2 * vector_count
    )
    dressed = lax.dot_general(
        left_side, chosen, (((2,), (1,)), ((0,), (0,))), preferred_element_type=jnp.float32
    )
    return dressed.astype(jnp.bfloat16).reshape(
        1, group_count, capacity, 2, row_count, vector_count
    )


def shards(*args):
    eigvecs = args[0]
    count, planes, sites = eigvecs.shape[1], eigvecs.shape[4], eigvecs.shape[5]
    space_size, groups = lax.axis_size("space"), lax.axis_size("tm")
    whole_tiles = sites % (2 * LANES) == 0 and count == LANES and planes * (sites // LANES) == GROUP
    fits = groups * 3 * ((JOB_DEV + groups - 1) // groups) < LANES
    powers = space_size & (space_size - 1) == 0 and groups & (groups - 1) == 0
    small = space_size * GROUP == count and groups <= 8 and args[3].shape[0] <= LANES
    if whole_tiles and fits and powers and small and eigvecs.shape[0] == 1:
        return fast_shards(*args)
    return plain_shards(*args)


def solution(mesh):
    return jax.shard_map(
        shards,
        mesh=mesh,
        in_specs=(
            P("tm", None, None, None, "space", None),
            P("tm", None, None, None, None, "space", None),
            P("tm", None, None, None, None),
            P(),
            P(),
            P(),
            P(),
        ),
        out_specs=P("tm", None, None, None, "space", None),
        check_vma=False,
    )
```

```python
import math
from functools import partial

import numpy as np
import jax
import jax.numpy as jnp
from jax import lax
from jax.experimental import pallas as pl
from jax.experimental.pallas import tpu as pltpu
from jax.sharding import PartitionSpec as P

LY = 16
LZ = 32
OPS = 4
SPIN = 4
JOB_DEV = 24
LANES = 128
GROUP = 16
NARROW = (1, 2)
F32 = jnp.float32
BF16 = jnp.bfloat16
VMEM = pltpu.VMEM
SMEM = pltpu.SMEM


def vspec():
    return pl.BlockSpec(memory_space=VMEM)


def sspec():
    return pl.BlockSpec(memory_space=SMEM)


def cost(flops, moved):
    return pl.CostEstimate(flops=flops, bytes_accessed=moved, transcendentals=0)


def limit(mebibytes):
    return pltpu.CompilerParams(vmem_limit_bytes=mebibytes * 2**20)


def pick_matrix(rows, cols, source_of):
    row = lax.broadcasted_iota(jnp.int32, (rows, cols), 0)
    col = lax.broadcasted_iota(jnp.int32, (rows, cols), 1)
    return jnp.where(col == source_of(row), 1.0, 0.0).astype(BF16)


def joined(pieces):
    return jnp.concatenate(pieces, axis=1)


def nt_dot(left, right):
    return lax.dot_general(left, right, (((1,), (1,)), ((), ())), preferred_element_type=F32)


def rim_kernel(tiles, planes, start, leads, x_hbm, u_hbm, *refs):
    if leads:
        out_ref, x_ref, link_ref, u_ref, pick_ref, sems = refs
    else:
        link_ref, out_ref, x_ref, u_ref, pick_ref, sems = refs
    spots = tiles * planes
    pair = 2
    part_count = out_ref.shape[2] // 2
    chunk = GROUP * 6 * spots
    chunks = part_count // GROUP
    rows_of = [pl.ds(g * chunk, chunk) for g in range(chunks)]
    copies = [
        pltpu.make_async_copy(x_hbm.at[pl.ds((start + g) * chunk, chunk)], x_ref.at[rows], sems.at[g])
        for g, rows in enumerate(rows_of)
    ]
    link_copy = pltpu.make_async_copy(u_hbm.at[pl.ds(0, u_ref.shape[0])], u_ref, sems.at[chunks])
    for copy in [link_copy] + copies if leads else copies + [link_copy]:
        copy.start()

    def source(row):
        return (row & (GROUP - 1)) * spots + (row // GROUP) * planes + planes - 1

    pick_ref[...] = pick_matrix(tiles * GROUP, GROUP * spots, source)
    if leads:
        link_copy.wait()
        for tile in range(tiles):
            flat = adjoint(load_rows(u_ref, 0, tile * planes + planes - 1, spots))
            for k, link in enumerate(flat):
                link_ref[tile, k] = link
    chosen = pick_ref[...]
    for g in range(chunks):
        copies[g].wait()
        block = x_ref[g * chunk : (g + 1) * chunk, :].reshape(GROUP, 6, spots, LANES)
        taken = []
        for part in range(0, 6, 2):
            rows = joined([block[:, part + k].reshape(GROUP * spots, LANES) for k in range(2)])
            got = jnp.dot(chosen, rows, preferred_element_type=F32)
            taken += [got[:, :LANES], got[:, LANES:]]
        for tile in range(tiles):
            links = [[[link_ref[tile, (p * 3 + r) * 3 + c] for c in range(3)] for r in range(3)] for p in range(3)]
            outs = []
            for eight in (0, 8):
                at = tile * GROUP + eight
                vec = [part[at : at + 8] for part in taken]
                outs.append(link_product(links, vec[:3], vec[3:]))
            for half in range(2):
                row = half * part_count + g * GROUP
                for colour in range(3):
                    both = jnp.concatenate([outs[0][half][colour], outs[1][half][colour]], axis=0)
                    out_ref[tile // pair, (tile % pair) * 3 + colour, row : row + GROUP] = both.astype(BF16)
    if not leads:
        link_copy.wait()


def rim_plane(x, u, links, count, tiles, planes):
    spots = tiles * planes
    pair = 2
    leads = links is None
    part_count = count // 2
    chunks = part_count // GROUP
    hbm = pl.BlockSpec(memory_space=pltpu.HBM)
    out_shape = [
        jax.ShapeDtypeStruct((tiles // pair, 3 * pair, 2 * part_count, LANES), BF16),
        jax.ShapeDtypeStruct((x.shape[0] // 2, LANES), BF16),
    ]
    scratch = [
        VMEM((tiles * GROUP, GROUP * spots), BF16),
        pltpu.SemaphoreType.DMA((chunks + 1,)),
    ]
    if leads:
        out_shape.append(jax.ShapeDtypeStruct((tiles, 27, 8, LANES), F32))
        scratch = [VMEM((18 * spots, LANES), F32)] + scratch
    else:
        out_shape.append(jax.ShapeDtypeStruct(u.shape, F32))
    return pl.pallas_call(
        partial(rim_kernel, tiles, planes, 0 if leads else chunks, leads),
        in_specs=[hbm, hbm] + ([] if leads else [vspec()]),
        out_specs=[vspec()] * 3,
        out_shape=out_shape,
        scratch_shapes=scratch,
        compiler_params=limit(6),
        cost_estimate=cost(10**8, 2 * 10**6),
        name="rim" if leads else "rest",
    )(x, u, *([] if leads else [links]))


def link_product(links, vec_re, vec_im):
    plus = [vec_re[c] + vec_im[c] for c in range(3)]
    outs_re, outs_im = [], []
    for row in range(3):
        link_re, link_less, link_more = links[0][row], links[1][row], links[2][row]
        one = link_re[0] * plus[0] + link_re[1] * plus[1] + link_re[2] * plus[2]
        two = link_less[0] * vec_re[0] + link_less[1] * vec_re[1] + link_less[2] * vec_re[2]
        three = link_more[0] * vec_im[0] + link_more[1] * vec_im[1] + link_more[2] * vec_im[2]
        outs_re.append(one - three)
        outs_im.append(one + two)
    return outs_re, outs_im


def narrow_product(links, vec_re, vec_im):
    real, imag = links
    outs_re, outs_im = [], []
    for row in range(3):
        ones = [real[row][c] * vec_re[c] - imag[row][c] * vec_im[c] for c in range(3)]
        twos = [real[row][c] * vec_im[c] + imag[row][c] * vec_re[c] for c in range(3)]
        outs_re.append(ones[0] + ones[1] + ones[2])
        outs_im.append(twos[0] + twos[1] + twos[2])
    return outs_re, outs_im


def narrow_links(u_ref, direction, spot, spots):
    def one(part, row, col):
        at = (((direction * 2 + part) * 3 + row) * 3 + col) * spots + spot
        return jnp.broadcast_to(u_ref[pl.ds(at, 1), :], (GROUP, LANES)).astype(BF16)

    return [[[one(part, row, col) for col in range(3)] for row in range(3)] for part in range(2)]


def load_rows(u_ref, direction, spot, spots):
    def one(part, row, col):
        at = (((direction * 2 + part) * 3 + row) * 3 + col) * spots + spot
        return jnp.broadcast_to(u_ref[pl.ds(at, 1), :], (8, LANES))

    return [[[one(part, row, col) for col in range(3)] for row in range(3)] for part in range(2)]


def load_links(u_ref, direction, spot, spots):
    real, imag = load_rows(u_ref, direction, spot, spots)
    less = [[imag[row][col] - real[row][col] for col in range(3)] for row in range(3)]
    more = [[imag[row][col] + real[row][col] for col in range(3)] for row in range(3)]
    return real, less, more


def adjoint(grid):
    real, imag = grid
    order = [(row, col) for row in range(3) for col in range(3)]
    return (
        [real[col][row] for row, col in order]
        + [-imag[col][row] - real[col][row] for row, col in order]
        + [real[col][row] - imag[col][row] for row, col in order]
    )


def fill_table(groups, slots, empty, owner_ref, elem_ref, source_ref, spin_ref, table_ref):
    total = owner_ref.shape[1]
    jobs = total // groups
    row = lax.broadcasted_iota(jnp.int32, (total, total), 0)
    col = lax.broadcasted_iota(jnp.int32, (total, total), 1)

    def group_of(index):
        return sum((index >= group * jobs).astype(jnp.int32) for group in range(1, groups))

    live = jnp.where(owner_ref[...] == lax.axis_index("tm"), 1.0, 0.0)
    product = source_ref[...] * (SPIN * groups * OPS) + spin_ref[...] * (groups * OPS) + elem_ref[...]

    def column(mask, values):
        wide = jnp.broadcast_to(values.astype(F32), (total, total))
        return jnp.sum(jnp.where(mask, wide, 0.0), axis=1, keepdims=True)

    rank = column((col < row) & (group_of(col) == group_of(row)), live)
    alive = column(col == row, live)
    value = column(col == row, product)
    at_row = lax.broadcasted_iota(jnp.int32, (total, LANES), 0)
    at_col = lax.broadcasted_iota(jnp.int32, (total, LANES), 1)
    group = group_of(at_row).astype(F32)
    place = jnp.where(alive > 0.5, group * slots + rank, -1.0)
    found = at_col.astype(F32) == place
    picked = jnp.sum(jnp.where(found, value + group * OPS - empty, 0.0), axis=0, keepdims=True)
    table_ref[...] = (picked + empty).astype(jnp.int32)


def paired(grid, count):
    real = grid[:count, :count] + grid[count:, count:]
    imag = grid[count:, :count] - grid[:count, count:]
    return real, imag


def anti(real, imag):
    return 0.5 * (real.T - real), 0.5 * (imag.T + imag)


def gram_kernel(
    count, tiles, planes, lx, groups, slots, empty,
    low_ref, high_ref, u_ref, phase_ref, owner_ref, elem_ref, source_ref, spin_ref,
    sums_ref, rim_lhs_ref, table_ref,
    lhs_ref, op_ref, acc_ref, g_ref, pick_ref,
):
    spots = tiles * planes
    pair = 2
    halves = tiles // pair
    steps = planes * halves

    def source(row):
        spot = row // GROUP
        return (row & (GROUP - 1)) * spots + (spot % tiles) * planes + spot // tiles

    pick_ref[...] = pick_matrix(GROUP * spots, GROUP * spots, source)
    acc_ref[...] = jnp.zeros_like(acc_ref)
    g_ref[...] = jnp.zeros_like(g_ref)

    chosen = pick_ref[...]
    for at in range(0, count, GROUP):
        x_ref, near = (low_ref, at) if at < count // 2 else (high_ref, at - count // 2)
        block = x_ref[near * 6 * spots : (near + GROUP) * 6 * spots, :].reshape(GROUP, 6, spots, LANES)
        for first in range(0, 6, 2):
            rows = jnp.concatenate(
                [block[:, first + k].reshape(GROUP * spots, LANES) for k in range(2)], axis=1
            )
            taken = jnp.dot(chosen, rows, preferred_element_type=F32)
            for k in range(2):
                part = first + k
                half, colour = part // 3, part % 3
                for spot in range(spots):
                    piece = taken[spot * GROUP : (spot + 1) * GROUP, k * LANES : (k + 1) * LANES]
                    plane, tile = spot // tiles, spot % tiles
                    lhs_ref[
                        plane * halves + tile // pair,
                        (tile % pair) * 3 + colour,
                        half * count + at : half * count + at + GROUP,
                    ] = piece.astype(BF16)

    lane = lax.broadcasted_iota(jnp.int32, (GROUP, LANES), 1)
    wraps = (lane & (LZ - 1)) == LZ - 1
    spills = lane < LZ

    def elementwise(step, slot, directions):
        plane = step // halves
        half_tile = step % halves
        for sub in range(pair):
            tile = half_tile * pair + sub
            ahead = step if sub + 1 < pair else plane * halves + (half_tile + 1) % halves
            for direction in directions:
                narrow = direction in NARROW
                links = (narrow_links if narrow else load_links)(
                    u_ref, direction, tile * planes + plane, spots
                )
                for at in range(0, count, GROUP):

                    def part(where, turn, k):
                        row = k // 3 * count + at
                        return lhs_ref[where, turn * 3 + k % 3, row : row + GROUP]

                    if direction == 0:
                        vec = [part(step + halves, sub, k) for k in range(6)]
                    elif direction == 1:
                        vec = [
                            pltpu.roll(
                                jnp.where(spills, part(ahead, (sub + 1) % pair, k), part(step, sub, k)), LANES - LZ, 1
                            )
                            for k in range(6)
                        ]
                    else:
                        vec = [
                            jnp.where(
                                wraps,
                                pltpu.roll(part(step, sub, k), LZ - 1, 1),
                                pltpu.roll(part(step, sub, k), LANES - 1, 1),
                            )
                            for k in range(6)
                        ]
                    if narrow:
                        outs = narrow_product(links, vec[:3], vec[3:])
                    else:
                        wide = [piece.astype(F32) for piece in vec]
                        pieces = [[piece[eight : eight + 8] for piece in wide] for eight in (0, 8)]
                        low, high = [link_product(links, piece[:3], piece[3:]) for piece in pieces]
                        outs = [
                            [
                                jnp.concatenate([low[half][colour], high[half][colour]], axis=0).astype(BF16)
                                for colour in range(3)
                            ]
                            for half in range(2)
                        ]
                    for half in range(2):
                        row = (direction * 2 + half) * count + at
                        for colour in range(3):
                            op_ref[slot, sub * 3 + colour, row : row + GROUP] = outs[half][colour]

    def multiply(step, slot, directions):
        fixed = joined([lhs_ref[step, k] for k in range(3 * pair)])
        low = min(directions) * 2 * count
        high = (max(directions) + 1) * 2 * count
        moving = joined([op_ref[slot, k, low:high] for k in range(3 * pair)])
        got = nt_dot(jnp.concatenate([fixed, moving], axis=0), fixed)
        g_ref[step // halves] += got[: 2 * count]
        acc_ref[low:high, :] += got[2 * count :]

    every, side = (0, 1, 2), (1, 2)
    inner = steps - halves
    elementwise(inner, 0, side)
    for step in range(inner + 1, steps):
        multiply(step - 1, (step - 1) & 1, side)
        elementwise(step, step & 1, side)
    multiply(steps - 1, (steps - 1) & 1, side)
    elementwise(0, 0, every)

    for step in range(1, inner):
        multiply(step - 1, (step - 1) & 1, every)
        elementwise(step, step & 1, every)
    multiply(inner - 1, (inner - 1) & 1, every)
    fill_table(groups, slots, empty, owner_ref, elem_ref, source_ref, spin_ref, table_ref)

    first = lax.axis_index("space") * planes
    total_re = jnp.zeros((count, count), F32)
    total_im = jnp.zeros((count, count), F32)
    for plane in range(planes):
        real, imag = paired(g_ref[plane], count)
        cosine = phase_ref[first + plane]
        sine = phase_ref[lx + first + plane]
        total_re += cosine * real - sine * imag
        total_im += cosine * imag + sine * real
    sums_ref[0, 0] = total_re
    sums_ref[0, 1] = -total_im
    for direction in range(3):
        grid = acc_ref[direction * 2 * count : (direction + 1) * 2 * count, :]
        real, imag = anti(*paired(grid, count))
        sums_ref[direction + 1, 0] = real
        sums_ref[direction + 1, 1] = imag
    for half in range(halves):
        rim_lhs_ref[half] = lhs_ref[half]


def gram(low, high, u, phases, tables, count, tiles, planes, lx, groups, slots, empty):
    spots = tiles * planes
    pair = 2
    steps = planes * (tiles // pair)
    return pl.pallas_call(
        partial(gram_kernel, count, tiles, planes, lx, groups, slots, empty),
        in_specs=[vspec()] * 3 + [sspec()] + [vspec()] * 4,
        out_specs=[vspec()] * 3,
        out_shape=[
            jax.ShapeDtypeStruct((OPS, 2, count, count), F32),
            jax.ShapeDtypeStruct((tiles // pair, 3 * pair, 2 * count, LANES), BF16),
            jax.ShapeDtypeStruct((1, LANES), jnp.int32),
        ],
        scratch_shapes=[
            VMEM((steps, 3 * pair, 2 * count, LANES), BF16),
            VMEM((2, 3 * pair, 6 * count, LANES), BF16),
            VMEM((6 * count, 2 * count), F32),
            VMEM((planes, 2 * count, 2 * count), F32),
            VMEM((GROUP * spots, GROUP * spots), BF16),
        ],
        compiler_params=limit(26),
        cost_estimate=cost(8 * 10**9, 5 * 10**6),
        name="gram",
    )(low, high, u, phases, *tables)


def edge_kernel(count, rows, cores, low_ref, high_ref, lhs_ref, sums_ref, keep_ref, send_ref, tot_ref):
    total = None
    for half in range(low_ref.shape[0]):
        sides = [joined([ref[half, k] for k in range(ref.shape[1])]) for ref in (low_ref, high_ref, lhs_ref)]
        got = nt_dot(jnp.concatenate(sides[:2], axis=0), sides[2])
        total = got if total is None else total + got
    reals, imags = [], []
    mid = count // 2
    for at in (0, count):
        reals.append(total[at : at + mid, :count] + total[at + mid : at + count, count:])
        imags.append(total[at : at + mid, count:] - total[at + mid : at + count, :count])
    real, imag = jnp.concatenate(reals, axis=0), jnp.concatenate(imags, axis=0)
    tot_ref[0] = 0.5 * (real - real.T)
    tot_ref[1] = 0.5 * (imag + imag.T)
    mine = lax.axis_index("space") & (cores - 1)
    for chip in range(count // (rows * cores)):
        for which, ref in ((mine, keep_ref), (1 - mine, send_ref)):
            at = pl.multiple_of((chip * cores + which) * rows, rows)
            for op in range(OPS):
                for half in range(2):
                    piece = sums_ref[op, half, pl.ds(at, rows), :]
                    if op == 1:
                        piece = piece + tot_ref[half, pl.ds(at, rows), :]
                    ref[chip, op, half] = piece


def edge(halos, rim_lhs, sums, count, rows, cores):
    shape = jax.ShapeDtypeStruct((count // (rows * cores), OPS, 2, rows, count), F32)
    return pl.pallas_call(
        partial(edge_kernel, count, rows, cores),
        in_specs=[vspec()] * 4,
        out_specs=[vspec(), vspec()],
        out_shape=[shape, shape],
        scratch_shapes=[VMEM((2, count, count), F32)],
        compiler_params=limit(8),
        cost_estimate=cost(10**9, 3 * 10**6),
        name="edge",
    )(*halos, rim_lhs, sums)


def split_sum(block):
    high = block[0:1].astype(BF16)
    low = (block[0:1] - high.astype(F32)).astype(BF16)
    return jnp.concatenate([high, low, block[1:].astype(BF16)], axis=0)


def fold_kernel(chips, cores, keep_ref, got_ref, own_ref, *out_refs):
    me = lax.axis_index("space") // cores
    own_ref[...] = keep_ref[me] + got_ref[me]
    for step in range(1, chips):
        to = me ^ step
        out_refs[step - 1][...] = split_sum(keep_ref[to] + got_ref[to])


def fold(keep, got, cores):
    chips = keep.shape[0]
    shape = keep.shape[1:]
    sent = jax.ShapeDtypeStruct((shape[0] + 1,) + shape[1:], BF16)
    return pl.pallas_call(
        partial(fold_kernel, chips, cores),
        in_specs=[vspec()] * 2,
        out_specs=[vspec()] * chips,
        out_shape=[jax.ShapeDtypeStruct(shape, F32)] + [sent] * (chips - 1),
        compiler_params=limit(4),
        cost_estimate=cost(10**6, 10**6),
        name="fold",
    )(keep, got)


def total_kernel(own_ref, *refs):
    total_ref = refs[-1]
    first = own_ref[0:1]
    rest = own_ref[1:]
    for ref in refs[:-1]:
        first = first + (ref[0:1].astype(F32) + ref[1:2].astype(F32))
        rest = rest + ref[2:].astype(F32)
    total_ref[0:1] = first.astype(BF16)
    total_ref[1:] = rest.astype(BF16)


def total_rows(parts):
    return pl.pallas_call(
        total_kernel,
        in_specs=[vspec()] * len(parts),
        out_specs=vspec(),
        out_shape=jax.ShapeDtypeStruct(parts[0].shape, BF16),
        compiler_params=limit(4),
        cost_estimate=cost(10**6, 10**6),
        name="total",
    )(*parts)


def dress_kernel(groups, slots, taus, rows, count, table_any, per_ref, *refs):
    slab_refs = refs[:groups]
    out_hbm, lhs_ref, prod_ref, stage_ref, table_ref, sems = refs[groups:]
    table_copy = pltpu.make_async_copy(table_any, table_ref, sems.at[groups])
    table_copy.start()
    me = lax.axis_index("tm")
    for step in range(groups):
        group = me ^ step
        for op in range(OPS):
            at = pl.multiple_of((group * OPS + op) * rows, rows)
            lhs_ref[pl.ds(at, rows), 0:count] = slab_refs[step][op, 0]
            lhs_ref[pl.ds(at, rows), count : 2 * count] = slab_refs[step][op, 1]
    left = lhs_ref[...]
    for tau in range(taus):
        real, imag = per_ref[tau, 0], per_ref[tau, 1]
        right = jnp.concatenate([joined([real, imag]), joined([-imag, real])], axis=0)
        got = jnp.dot(left, right, preferred_element_type=F32).astype(BF16)
        for piece in range(groups * OPS):
            for half in range(2):
                prod_ref[tau * groups * OPS + piece, half] = got[
                    piece * rows : (piece + 1) * rows, half * count : (half + 1) * count
                ]
    prod_ref[taus * groups * OPS] = jnp.zeros((2, rows, count), BF16)
    table_copy.wait()
    copies = []
    for group in range(groups):
        for slot in range(slots):
            stage_ref[group, slot] = prod_ref[table_ref[0, group * slots + slot]]
        copies.append(pltpu.make_async_copy(stage_ref.at[group], out_hbm.at[group], sems.at[group]))
        copies[group].start()
    for copy in copies:
        copy.wait()


def dress(table, per, slabs, groups, slots, rows, count):
    taus = per.shape[0]
    shape = (groups, slots, 2, rows, count)
    return pl.pallas_call(
        partial(dress_kernel, groups, slots, taus, rows, count),
        in_specs=[pl.BlockSpec(memory_space=pl.ANY), vspec()] + [vspec()] * groups,
        out_specs=pl.BlockSpec(memory_space=pltpu.HBM),
        out_shape=jax.ShapeDtypeStruct(shape, BF16),
        scratch_shapes=[
            VMEM((groups * OPS * rows, 2 * count), BF16),
            VMEM((taus * groups * OPS + 1, 2, rows, count), BF16),
            VMEM(shape, BF16),
            SMEM(table.shape, jnp.int32),
            pltpu.SemaphoreType.DMA((groups + 1,)),
        ],
        compiler_params=limit(8),
        cost_estimate=cost(10**9, 2 * 10**6),
        name="dress",
    )(table, per, *slabs)


def fast_shards(eigvecs, gauge_links, perambulator, job_owner, job_elemental, job_source, job_spin):
    count = eigvecs.shape[1]
    planes, sites = eigvecs.shape[4], eigvecs.shape[5]
    tiles = sites // LANES
    space_size = lax.axis_size("space")
    groups = lax.axis_size("tm")
    lx = planes * space_size
    rows = count // space_size
    slots = 3 * ((JOB_DEV + groups - 1) // groups)
    cores = 2

    def tiled(field):
        head = field.shape[:-2]
        order = tuple(range(len(head))) + (len(head) + 1, len(head), len(head) + 2)
        split = field.reshape(head + (planes, tiles, LANES))
        return split.transpose(order).reshape(-1, LANES)

    x = tiled(eigvecs)
    u = tiled(gauge_links)
    angle = 2.0 * math.pi / lx * np.arange(lx)
    phases = jnp.asarray(np.concatenate([np.cos(angle), np.sin(angle)]).astype(np.float32))

    per = perambulator.reshape(-1, 2, count, count)
    empty = per.shape[0] * groups * OPS
    x = pltpu.with_memory_space_constraint(x, pltpu.HBM)
    u = pltpu.with_memory_space_constraint(u, pltpu.HBM)
    up = [(i, (i + 1) % space_size) for i in range(space_size)]
    rim, low, links = rim_plane(x, u, None, count, tiles, planes)
    halos = [lax.ppermute(rim, "space", up)]
    rim, high, u = rim_plane(x, u, links, count, tiles, planes)
    halos.append(lax.ppermute(rim, "space", up))
    tables = [job.reshape(1, -1) for job in (job_owner, job_elemental, job_source, job_spin)]
    sums, rim_lhs, table = gram(
        low, high, u, phases, tables, count, tiles, planes, lx, groups, slots, empty
    )
    keep, send = edge(halos, rim_lhs, sums, count, rows, cores)
    got = lax.ppermute(send, "space", [(i, i ^ 1) for i in range(space_size)])
    parts = fold(keep, got, cores)
    summed = [parts[0]]
    chips = space_size // cores
    for step in sorted(range(1, chips), key=lambda step: -bin(step).count("1")):
        summed.append(
            lax.ppermute(parts[step], "space", [(i, i ^ (step * cores)) for i in range(space_size)])
        )
    own = total_rows(summed)
    slabs = [own]
    for step in range(1, groups):
        slabs.append(lax.ppermute(own, "tm", [(i, i ^ step) for i in range(groups)]))
    return dress(table, per, slabs, groups, slots, rows, count)[None]


def passed_along(shard, axis, by):
    count = lax.axis_size(axis)
    return lax.ppermute(shard, axis, [(i, (i + by) % count) for i in range(count)])


def shifted_sites(lattice_field, direction, offset):
    shaped = lattice_field.reshape(lattice_field.shape[:-1] + (LY, LZ))
    rolled = jnp.roll(shaped, -offset, axis=direction - 4)
    return rolled.reshape(lattice_field.shape)


def apply_link(link_field, vectors):
    total_re = None
    total_im = None
    for colour in range(3):
        link_re = link_field[0, :, colour][None]
        link_im = link_field[1, :, colour][None]
        vector_re = vectors[:, 0, colour][:, None]
        vector_im = vectors[:, 1, colour][:, None]
        part_re = link_re * vector_re - link_im * vector_im
        part_im = link_re * vector_im + link_im * vector_re
        if colour == 0:
            total_re, total_im = (part_re, part_im)
        else:
            total_re = total_re + part_re
            total_im = total_im + part_im
    return jnp.stack([total_re, total_im], axis=1)


def stacked_form(vectors):
    vector_count = vectors.shape[0]
    swapped = jnp.concatenate([-vectors[:, 1:2], vectors[:, 0:1]], axis=1)
    return jnp.concatenate(
        [vectors.reshape(vector_count, -1), swapped.reshape(vector_count, -1)], axis=0
    )


def paired_gram(stacked, lattice_field):
    vector_count = lattice_field.shape[0]
    flat_field = lattice_field.astype(jnp.bfloat16).reshape(vector_count, -1)
    product = lax.dot_general(
        stacked, flat_field, (((1,), (1,)), ((), ())), preferred_element_type=jnp.float32
    )
    return product.reshape(2, vector_count, vector_count)


def twisted_field(vectors, xcoord):
    phase_angle = 2.0 * math.pi / (vectors.shape[3] * lax.axis_size("space")) * xcoord
    cosine = jnp.cos(phase_angle)[:, None]
    sine_part = jnp.sin(phase_angle)[:, None]
    real_part = cosine * vectors[:, 0] + sine_part * vectors[:, 1]
    imag_part = cosine * vectors[:, 1] - sine_part * vectors[:, 0]
    return jnp.stack([real_part, imag_part], axis=1)


def antihermitian(paired):
    return 0.5 * jnp.stack([paired[0] - paired[0].T, paired[1] + paired[1].T], axis=0)


def plain_shards(eigvecs, gauge_links, perambulator, job_owner, job_elemental, job_source, job_spin):
    slice_count = eigvecs.shape[0]
    vector_count = eigvecs.shape[1]
    planes = eigvecs.shape[4]
    space_size = lax.axis_size("space")
    group_count = lax.axis_size("tm")
    row_count = vector_count // space_size
    capacity = 3 * ((JOB_DEV + group_count - 1) // group_count)
    xcoord = (lax.axis_index("space") * planes + jnp.arange(planes, dtype=jnp.int32)).astype(
        jnp.float32
    )
    upper_plane = passed_along(eigvecs[:, :, :, :, 0:1], "space", -1)
    low_vectors = eigvecs[0]
    vectors = low_vectors.astype(jnp.float32)
    stacked = stacked_form(low_vectors)
    results = [paired_gram(stacked, twisted_field(vectors, xcoord))]
    for direction in (1, 2, 3):
        link_field = gauge_links[0, direction - 1]
        if direction == 1:
            upper_rim = upper_plane[0].astype(jnp.float32)
            above_field = jnp.concatenate([vectors[:, :, :, 1:], upper_rim], axis=3)
        else:
            above_field = shifted_sites(vectors, direction, 1)
        forward = apply_link(link_field, above_field)
        results.append(antihermitian(paired_gram(stacked, forward)))
    partial_list = [jnp.stack(results, axis=0)]
    partial_value = jnp.stack(partial_list, axis=0)
    summed = lax.psum(partial_value, "space")
    own_rows = lax.dynamic_slice_in_dim(summed, lax.axis_index("space") * row_count, row_count, 3)
    slab_table = own_rows.astype(jnp.bfloat16).reshape(
        slice_count * OPS, 2 * row_count * vector_count
    )
    owners = job_owner[:, 0].reshape(group_count, -1)
    elements = job_elemental.reshape(group_count, -1)
    position = jnp.arange(owners.shape[1], dtype=jnp.int32)
    earlier = position[None, :] < position[:, None]
    same_owner = owners[:, :, None] == owners[:, None, :]
    slot_rank = jnp.sum(jnp.where(same_owner & earlier[None], 1, 0), axis=2).astype(jnp.int32)
    own_group = lax.axis_index("tm")
    slot_count = group_count * capacity
    live_jobs = owners == own_group
    slot_match = live_jobs[:, None, :] & (
        slot_rank[:, None, :] == jnp.arange(capacity, dtype=jnp.int32)[None, :, None]
    )
    sender_owners = lax.dynamic_index_in_dim(owners, own_group, 0, keepdims=False)
    sender_ranks = lax.dynamic_index_in_dim(slot_rank, own_group, 0, keepdims=False)
    sender_elements = lax.dynamic_index_in_dim(elements, own_group, 0, keepdims=False)
    slot_ids = sender_owners * capacity + sender_ranks
    slot_hot = (jnp.arange(slot_count, dtype=jnp.int32)[:, None] == slot_ids[None, :]).astype(
        jnp.float32
    )
    elem_hot = (
        sender_elements[:, None] == jnp.arange(slice_count * OPS, dtype=jnp.int32)[None, :]
    ).astype(jnp.float32)
    picker = jnp.dot(slot_hot, elem_hot, precision=lax.Precision.HIGHEST).astype(jnp.bfloat16)
    outgoing = jnp.dot(picker, slab_table, preferred_element_type=jnp.float32).astype(jnp.bfloat16)
    outgoing = outgoing.reshape(group_count, capacity, 2, row_count, vector_count)
    received = lax.all_to_all(outgoing, "tm", split_axis=0, concat_axis=0, tiled=True)
    block_index = job_source.reshape(group_count, -1) * SPIN + job_spin.reshape(group_count, -1)
    tau_index = jnp.sum(jnp.where(slot_match, block_index[:, None, :], 0), axis=2)
    blocks = perambulator.reshape(-1, 2 * vector_count, vector_count)
    chosen = jnp.take(blocks, tau_index.reshape(-1), axis=0)
    slab_rows = received.reshape(slot_count, 2, row_count, vector_count)
    real_rows = jnp.concatenate([slab_rows[:, 0], -slab_rows[:, 1]], axis=-1)
    imag_rows = jnp.concatenate([slab_rows[:, 1], slab_rows[:, 0]], axis=-1)
    left_side = jnp.stack([real_rows, imag_rows], axis=1).reshape(
        slot_count, 2 * row_count, 2 * vector_count
    )
    dressed = lax.dot_general(
        left_side, chosen, (((2,), (1,)), ((0,), (0,))), preferred_element_type=jnp.float32
    )
    return dressed.astype(jnp.bfloat16).reshape(
        1, group_count, capacity, 2, row_count, vector_count
    )


def shards(*args):
    eigvecs = args[0]
    count, planes, sites = eigvecs.shape[1], eigvecs.shape[4], eigvecs.shape[5]
    space_size, groups = lax.axis_size("space"), lax.axis_size("tm")
    whole_tiles = sites % (2 * LANES) == 0 and count == LANES and planes * (sites // LANES) == GROUP
    fits = groups * 3 * ((JOB_DEV + groups - 1) // groups) < LANES
    powers = space_size & (space_size - 1) == 0 and groups & (groups - 1) == 0
    small = space_size * GROUP == count and groups <= 8 and args[3].shape[0] <= LANES
    if whole_tiles and fits and powers and small and eigvecs.shape[0] == 1:
        return fast_shards(*args)
    return plain_shards(*args)


def solution(mesh):
    return jax.shard_map(
        shards,
        mesh=mesh,
        in_specs=(
            P("tm", None, None, None, "space", None),
            P("tm", None, None, None, None, "space", None),
            P("tm", None, None, None, None),
            P(),
            P(),
            P(),
            P(),
        ),
        out_specs=P("tm", None, None, None, "space", None),
        check_vma=False,
    )
```

```python
import math
from functools import partial

import numpy as np
import jax
import jax.numpy as jnp
from jax import lax
from jax.experimental import pallas as pl
from jax.experimental.pallas import tpu as pltpu
from jax.sharding import PartitionSpec as P

LY = 16
LZ = 32
OPS = 4
SPIN = 4
JOB_DEV = 24
LANES = 128
GROUP = 16
NARROW = (1, 2)
F32 = jnp.float32
BF16 = jnp.bfloat16
VMEM = pltpu.VMEM
SMEM = pltpu.SMEM


def vspec():
    return pl.BlockSpec(memory_space=VMEM)


def cost(flops, moved):
    return pl.CostEstimate(flops=flops, bytes_accessed=moved, transcendentals=0)


def limit(mebibytes):
    return pltpu.CompilerParams(vmem_limit_bytes=mebibytes * 2**20)


def pick_matrix(rows, cols, source_of):
    row = lax.broadcasted_iota(jnp.int32, (rows, cols), 0)
    col = lax.broadcasted_iota(jnp.int32, (rows, cols), 1)
    return jnp.where(col == source_of(row), 1.0, 0.0).astype(BF16)


def joined(pieces):
    return jnp.concatenate(pieces, axis=1)


def nt_dot(left, right):
    return lax.dot_general(left, right, (((1,), (1,)), ((), ())), preferred_element_type=F32)


def rim_kernel(tiles, planes, start, leads, x_hbm, u_hbm, *refs):
    if leads:
        out_ref, x_ref, link_ref, u_ref, pick_ref, sems = refs
    else:
        link_ref, out_ref, x_ref, u_ref, pick_ref, sems = refs
    spots = tiles * planes
    pair = 2
    part_count = out_ref.shape[2] // 2
    chunk = GROUP * 6 * spots
    chunks = part_count // GROUP
    rows_of = [pl.ds(g * chunk, chunk) for g in range(chunks)]
    copies = [
        pltpu.make_async_copy(x_hbm.at[pl.ds((start + g) * chunk, chunk)], x_ref.at[rows], sems.at[g])
        for g, rows in enumerate(rows_of)
    ]
    link_copy = pltpu.make_async_copy(u_hbm.at[pl.ds(0, u_ref.shape[0])], u_ref, sems.at[chunks])
    for copy in [link_copy] + copies if leads else copies + [link_copy]:
        copy.start()

    def source(row):
        return (row & (GROUP - 1)) * spots + (row // GROUP) * planes + planes - 1

    pick_ref[...] = pick_matrix(tiles * GROUP, GROUP * spots, source)
    if leads:
        link_copy.wait()
        for tile in range(tiles):
            flat = adjoint(load_rows(u_ref, 0, tile * planes + planes - 1, spots))
            for k, link in enumerate(flat):
                link_ref[tile, k] = link
    chosen = pick_ref[...]
    for g in range(chunks):
        copies[g].wait()
        block = x_ref[g * chunk : (g + 1) * chunk, :].reshape(GROUP, 6, spots, LANES)
        taken = []
        for part in range(0, 6, 2):
            rows = joined([block[:, part + k].reshape(GROUP * spots, LANES) for k in range(2)])
            got = jnp.dot(chosen, rows, preferred_element_type=F32)
            taken += [got[:, :LANES], got[:, LANES:]]
        for tile in range(tiles):
            links = [[[link_ref[tile, (p * 3 + r) * 3 + c] for c in range(3)] for r in range(3)] for p in range(3)]
            outs = []
            for eight in (0, 8):
                at = tile * GROUP + eight
                vec = [part[at : at + 8] for part in taken]
                outs.append(link_product(links, vec[:3], vec[3:]))
            for half in range(2):
                row = half * part_count + g * GROUP
                for colour in range(3):
                    both = jnp.concatenate([outs[0][half][colour], outs[1][half][colour]], axis=0)
                    out_ref[tile // pair, (tile % pair) * 3 + colour, row : row + GROUP] = both.astype(BF16)
    if not leads:
        link_copy.wait()


def lead_count(count):
    return count // (4 * GROUP) * GROUP


def rim_plane(x, u, links, count, tiles, planes):
    spots = tiles * planes
    pair = 2
    leads = links is None
    part_count = lead_count(count) if leads else count - lead_count(count)
    chunks = part_count // GROUP
    hbm = pl.BlockSpec(memory_space=pltpu.HBM)
    out_shape = [
        jax.ShapeDtypeStruct((tiles // pair, 3 * pair, 2 * part_count, LANES), BF16),
        jax.ShapeDtypeStruct((part_count * 6 * spots, LANES), BF16),
    ]
    scratch = [
        VMEM((tiles * GROUP, GROUP * spots), BF16),
        pltpu.SemaphoreType.DMA((chunks + 1,)),
    ]
    if leads:
        out_shape.append(jax.ShapeDtypeStruct((tiles, 27, 8, LANES), F32))
        scratch = [VMEM((18 * spots, LANES), F32)] + scratch
    else:
        out_shape.append(jax.ShapeDtypeStruct(u.shape, F32))
    return pl.pallas_call(
        partial(rim_kernel, tiles, planes, 0 if leads else lead_count(count) // GROUP, leads),
        in_specs=[hbm, hbm] + ([] if leads else [vspec()]),
        out_specs=[vspec()] * 3,
        out_shape=out_shape,
        scratch_shapes=scratch,
        compiler_params=limit(6),
        cost_estimate=cost(10**8, 2 * 10**6),
        name="rim" if leads else "rest",
    )(x, u, *([] if leads else [links]))


def link_product(links, vec_re, vec_im):
    plus = [vec_re[c] + vec_im[c] for c in range(3)]
    outs_re, outs_im = [], []
    for row in range(3):
        link_re, link_less, link_more = links[0][row], links[1][row], links[2][row]
        one = link_re[0] * plus[0] + link_re[1] * plus[1] + link_re[2] * plus[2]
        two = link_less[0] * vec_re[0] + link_less[1] * vec_re[1] + link_less[2] * vec_re[2]
        three = link_more[0] * vec_im[0] + link_more[1] * vec_im[1] + link_more[2] * vec_im[2]
        outs_re.append(one - three)
        outs_im.append(one + two)
    return outs_re, outs_im


def narrow_product(links, vec_re, vec_im):
    real, imag = links
    outs_re, outs_im = [], []
    for row in range(3):
        ones = [real[row][c] * vec_re[c] - imag[row][c] * vec_im[c] for c in range(3)]
        twos = [real[row][c] * vec_im[c] + imag[row][c] * vec_re[c] for c in range(3)]
        outs_re.append(ones[0] + ones[1] + ones[2])
        outs_im.append(twos[0] + twos[1] + twos[2])
    return outs_re, outs_im


def narrow_links(u_ref, direction, spot, spots):
    def one(part, row, col):
        at = (((direction * 2 + part) * 3 + row) * 3 + col) * spots + spot
        return jnp.broadcast_to(u_ref[pl.ds(at, 1), :], (GROUP, LANES)).astype(BF16)

    return [[[one(part, row, col) for col in range(3)] for row in range(3)] for part in range(2)]


def load_rows(u_ref, direction, spot, spots):
    def one(part, row, col):
        at = (((direction * 2 + part) * 3 + row) * 3 + col) * spots + spot
        return jnp.broadcast_to(u_ref[pl.ds(at, 1), :], (8, LANES))

    return [[[one(part, row, col) for col in range(3)] for row in range(3)] for part in range(2)]


def load_links(u_ref, direction, spot, spots):
    real, imag = load_rows(u_ref, direction, spot, spots)
    less = [[imag[row][col] - real[row][col] for col in range(3)] for row in range(3)]
    more = [[imag[row][col] + real[row][col] for col in range(3)] for row in range(3)]
    return real, less, more


def adjoint(grid):
    real, imag = grid
    order = [(row, col) for row in range(3) for col in range(3)]
    return (
        [real[col][row] for row, col in order]
        + [-imag[col][row] - real[col][row] for row, col in order]
        + [real[col][row] - imag[col][row] for row, col in order]
    )


def fill_table(groups, slots, empty, owner_ref, elem_ref, source_ref, spin_ref, table_ref):
    total = owner_ref.shape[1]
    jobs = total // groups
    row = lax.broadcasted_iota(jnp.int32, (total, total), 0)
    col = lax.broadcasted_iota(jnp.int32, (total, total), 1)

    def group_of(index):
        return sum((index >= group * jobs).astype(jnp.int32) for group in range(1, groups))

    live = jnp.where(owner_ref[...] == lax.axis_index("tm"), 1.0, 0.0)
    product = source_ref[...] * (SPIN * groups * OPS) + spin_ref[...] * (groups * OPS) + elem_ref[...]

    def column(mask, values):
        wide = jnp.broadcast_to(values.astype(F32), (total, total))
        return jnp.sum(jnp.where(mask, wide, 0.0), axis=1, keepdims=True)

    rank = column((col < row) & (group_of(col) == group_of(row)), live)
    alive = column(col == row, live)
    value = column(col == row, product)
    at_row = lax.broadcasted_iota(jnp.int32, (total, LANES), 0)
    at_col = lax.broadcasted_iota(jnp.int32, (total, LANES), 1)
    group = group_of(at_row).astype(F32)
    place = jnp.where(alive > 0.5, group * slots + rank, -1.0)
    found = at_col.astype(F32) == place
    picked = jnp.sum(jnp.where(found, value + group * OPS - empty, 0.0), axis=0, keepdims=True)
    table_ref[...] = (picked + empty).astype(jnp.int32)


def paired(grid, count):
    real = grid[:count, :count] + grid[count:, count:]
    imag = grid[count:, :count] - grid[:count, count:]
    return real, imag


def anti(real, imag):
    return 0.5 * (real.T - real), 0.5 * (imag.T + imag)


def gram_kernel(
    count, tiles, planes, lx, groups, slots, empty,
    low_ref, high_ref, u_ref, phase_ref, owner_ref, elem_ref, source_ref, spin_ref,
    sums_ref, rim_lhs_ref, table_ref,
    lhs_ref, op_ref, acc_ref, g_ref, pick_ref,
):
    spots = tiles * planes
    pair = 2
    halves = tiles // pair
    steps = planes * halves

    def source(row):
        spot = row // GROUP
        return (row & (GROUP - 1)) * spots + (spot % tiles) * planes + spot // tiles

    pick_ref[...] = pick_matrix(GROUP * spots, GROUP * spots, source)
    acc_ref[...] = jnp.zeros_like(acc_ref)
    g_ref[...] = jnp.zeros_like(g_ref)

    chosen = pick_ref[...]
    for at in range(0, count, GROUP):
        lead = lead_count(count)
        x_ref, near = (low_ref, at) if at < lead else (high_ref, at - lead)
        block = x_ref[near * 6 * spots : (near + GROUP) * 6 * spots, :].reshape(GROUP, 6, spots, LANES)
        for first in range(0, 6, 2):
            rows = jnp.concatenate(
                [block[:, first + k].reshape(GROUP * spots, LANES) for k in range(2)], axis=1
            )
            taken = jnp.dot(chosen, rows, preferred_element_type=F32)
            for k in range(2):
                part = first + k
                half, colour = part // 3, part % 3
                for spot in range(spots):
                    piece = taken[spot * GROUP : (spot + 1) * GROUP, k * LANES : (k + 1) * LANES]
                    plane, tile = spot // tiles, spot % tiles
                    lhs_ref[
                        plane * halves + tile // pair,
                        (tile % pair) * 3 + colour,
                        half * count + at : half * count + at + GROUP,
                    ] = piece.astype(BF16)

    lane = lax.broadcasted_iota(jnp.int32, (GROUP, LANES), 1)
    wraps = (lane & (LZ - 1)) == LZ - 1
    spills = lane < LZ

    def elementwise(step, slot, directions):
        plane = step // halves
        half_tile = step % halves
        for sub in range(pair):
            tile = half_tile * pair + sub
            ahead = step if sub + 1 < pair else plane * halves + (half_tile + 1) % halves
            for direction in directions:
                narrow = direction in NARROW
                links = (narrow_links if narrow else load_links)(
                    u_ref, direction, tile * planes + plane, spots
                )
                for at in range(0, count, GROUP):

                    def part(where, turn, k):
                        row = k // 3 * count + at
                        return lhs_ref[where, turn * 3 + k % 3, row : row + GROUP]

                    if direction == 0:
                        vec = [part(step + halves, sub, k) for k in range(6)]
                    elif direction == 1:
                        vec = [
                            pltpu.roll(
                                jnp.where(spills, part(ahead, (sub + 1) % pair, k), part(step, sub, k)), LANES - LZ, 1
                            )
                            for k in range(6)
                        ]
                    else:
                        vec = [
                            jnp.where(
                                wraps,
                                pltpu.roll(part(step, sub, k), LZ - 1, 1),
                                pltpu.roll(part(step, sub, k), LANES - 1, 1),
                            )
                            for k in range(6)
                        ]
                    if narrow:
                        outs = narrow_product(links, vec[:3], vec[3:])
                    else:
                        wide = [piece.astype(F32) for piece in vec]
                        pieces = [[piece[eight : eight + 8] for piece in wide] for eight in (0, 8)]
                        low, high = [link_product(links, piece[:3], piece[3:]) for piece in pieces]
                        outs = [
                            [
                                jnp.concatenate([low[half][colour], high[half][colour]], axis=0).astype(BF16)
                                for colour in range(3)
                            ]
                            for half in range(2)
                        ]
                    for half in range(2):
                        row = (direction * 2 + half) * count + at
                        for colour in range(3):
                            op_ref[slot, sub * 3 + colour, row : row + GROUP] = outs[half][colour]

    def multiply(step, slot, directions):
        fixed = joined([lhs_ref[step, k] for k in range(3 * pair)])
        low = min(directions) * 2 * count
        high = (max(directions) + 1) * 2 * count
        moving = joined([op_ref[slot, k, low:high] for k in range(3 * pair)])
        got = nt_dot(jnp.concatenate([fixed, moving], axis=0), fixed)
        g_ref[step // halves] += got[: 2 * count]
        acc_ref[low:high, :] += got[2 * count :]

    every, side = (0, 1, 2), (1, 2)
    inner = steps - halves
    elementwise(inner, 0, side)
    for step in range(inner + 1, steps):
        multiply(step - 1, (step - 1) & 1, side)
        elementwise(step, step & 1, side)
    multiply(steps - 1, (steps - 1) & 1, side)
    elementwise(0, 0, every)

    for step in range(1, inner):
        multiply(step - 1, (step - 1) & 1, every)
        elementwise(step, step & 1, every)
    multiply(inner - 1, (inner - 1) & 1, every)
    fill_table(groups, slots, empty, owner_ref, elem_ref, source_ref, spin_ref, table_ref)

    first = lax.axis_index("space") * planes
    place = lax.broadcasted_iota(jnp.int32, phase_ref.shape, 1)
    total_re = jnp.zeros((count, count), F32)
    total_im = jnp.zeros((count, count), F32)
    for plane in range(planes):
        real, imag = paired(g_ref[plane], count)
        cosine = jnp.sum(jnp.where(place == first + plane, phase_ref[...], 0.0), axis=1, keepdims=True)
        sine = jnp.sum(jnp.where(place == lx + first + plane, phase_ref[...], 0.0), axis=1, keepdims=True)
        total_re += cosine * real - sine * imag
        total_im += cosine * imag + sine * real
    sums_ref[0, 0] = total_re
    sums_ref[0, 1] = -total_im
    for direction in range(3):
        grid = acc_ref[direction * 2 * count : (direction + 1) * 2 * count, :]
        real, imag = anti(*paired(grid, count))
        sums_ref[direction + 1, 0] = real
        sums_ref[direction + 1, 1] = imag
    for half in range(halves):
        rim_lhs_ref[half] = lhs_ref[half]


def gram(low, high, u, phases, tables, count, tiles, planes, lx, groups, slots, empty):
    spots = tiles * planes
    pair = 2
    steps = planes * (tiles // pair)
    return pl.pallas_call(
        partial(gram_kernel, count, tiles, planes, lx, groups, slots, empty),
        in_specs=[vspec()] * 8,
        out_specs=[vspec()] * 3,
        out_shape=[
            jax.ShapeDtypeStruct((OPS, 2, count, count), F32),
            jax.ShapeDtypeStruct((tiles // pair, 3 * pair, 2 * count, LANES), BF16),
            jax.ShapeDtypeStruct((1, LANES), jnp.int32),
        ],
        scratch_shapes=[
            VMEM((steps, 3 * pair, 2 * count, LANES), BF16),
            VMEM((2, 3 * pair, 6 * count, LANES), BF16),
            VMEM((6 * count, 2 * count), F32),
            VMEM((planes, 2 * count, 2 * count), F32),
            VMEM((GROUP * spots, GROUP * spots), BF16),
        ],
        compiler_params=limit(26),
        cost_estimate=cost(8 * 10**9, 5 * 10**6),
        name="gram",
    )(low, high, u, phases, *tables)


def edge_kernel(count, rows, cores, low_ref, high_ref, lhs_ref, sums_ref, keep_ref, send_ref, tot_ref):
    total = None
    for half in range(low_ref.shape[0]):
        sides = [joined([ref[half, k] for k in range(ref.shape[1])]) for ref in (low_ref, high_ref, lhs_ref)]
        got = nt_dot(jnp.concatenate(sides[:2], axis=0), sides[2])
        total = got if total is None else total + got
    reals, imags = [], []
    at = 0
    for size in (lead_count(count), count - lead_count(count)):
        mid, end = at + size, at + 2 * size
        reals.append(total[at:mid, :count] + total[mid:end, count:])
        imags.append(total[at:mid, count:] - total[mid:end, :count])
        at = end
    real, imag = jnp.concatenate(reals, axis=0), jnp.concatenate(imags, axis=0)
    tot_ref[0] = 0.5 * (real - real.T)
    tot_ref[1] = 0.5 * (imag + imag.T)
    mine = lax.axis_index("space") & (cores - 1)
    for chip in range(count // (rows * cores)):
        for which, ref in ((mine, keep_ref), (1 - mine, send_ref)):
            at = pl.multiple_of((chip * cores + which) * rows, rows)
            for op in range(OPS):
                for half in range(2):
                    piece = sums_ref[op, half, pl.ds(at, rows), :]
                    if op == 1:
                        piece = piece + tot_ref[half, pl.ds(at, rows), :]
                    ref[chip, op, half] = piece


def edge(halos, rim_lhs, sums, count, rows, cores):
    shape = jax.ShapeDtypeStruct((count // (rows * cores), OPS, 2, rows, count), F32)
    return pl.pallas_call(
        partial(edge_kernel, count, rows, cores),
        in_specs=[vspec()] * 4,
        out_specs=[vspec(), vspec()],
        out_shape=[shape, shape],
        scratch_shapes=[VMEM((2, count, count), F32)],
        compiler_params=limit(8),
        cost_estimate=cost(10**9, 3 * 10**6),
        name="edge",
    )(*halos, rim_lhs, sums)


def split_sum(block):
    high = block[0:1].astype(BF16)
    low = (block[0:1] - high.astype(F32)).astype(BF16)
    return jnp.concatenate([high, low, block[1:].astype(BF16)], axis=0)


def fold_kernel(chips, cores, keep_ref, got_ref, own_ref, *out_refs):
    me = lax.axis_index("space") // cores
    own_ref[...] = keep_ref[me] + got_ref[me]
    for step in range(1, chips):
        to = me ^ step
        out_refs[step - 1][...] = split_sum(keep_ref[to] + got_ref[to])


def fold(keep, got, cores):
    chips = keep.shape[0]
    shape = keep.shape[1:]
    sent = jax.ShapeDtypeStruct((shape[0] + 1,) + shape[1:], BF16)
    return pl.pallas_call(
        partial(fold_kernel, chips, cores),
        in_specs=[vspec()] * 2,
        out_specs=[vspec()] * chips,
        out_shape=[jax.ShapeDtypeStruct(shape, F32)] + [sent] * (chips - 1),
        compiler_params=limit(4),
        cost_estimate=cost(10**6, 10**6),
        name="fold",
    )(keep, got)


def total_kernel(own_ref, *refs):
    total_ref = refs[-1]
    first = own_ref[0:1]
    rest = own_ref[1:]
    for ref in refs[:-1]:
        first = first + (ref[0:1].astype(F32) + ref[1:2].astype(F32))
        rest = rest + ref[2:].astype(F32)
    total_ref[0:1] = first.astype(BF16)
    total_ref[1:] = rest.astype(BF16)


def total_rows(parts):
    return pl.pallas_call(
        total_kernel,
        in_specs=[vspec()] * len(parts),
        out_specs=vspec(),
        out_shape=jax.ShapeDtypeStruct(parts[0].shape, BF16),
        compiler_params=limit(4),
        cost_estimate=cost(10**6, 10**6),
        name="total",
    )(*parts)


def dress_kernel(groups, slots, taus, rows, count, table_any, per_ref, *refs):
    slab_refs = refs[:groups]
    out_hbm, lhs_ref, prod_ref, stage_ref, table_ref, sems = refs[groups:]
    table_copy = pltpu.make_async_copy(table_any, table_ref, sems.at[groups])
    table_copy.start()
    me = lax.axis_index("tm")
    for step in range(groups):
        group = me ^ step
        for op in range(OPS):
            at = pl.multiple_of((group * OPS + op) * rows, rows)
            lhs_ref[pl.ds(at, rows), 0:count] = slab_refs[step][op, 0]
            lhs_ref[pl.ds(at, rows), count : 2 * count] = slab_refs[step][op, 1]
    left = lhs_ref[...]
    for tau in range(taus):
        real, imag = per_ref[tau, 0], per_ref[tau, 1]
        right = jnp.concatenate([joined([real, imag]), joined([-imag, real])], axis=0)
        got = jnp.dot(left, right, preferred_element_type=F32).astype(BF16)
        for piece in range(groups * OPS):
            for half in range(2):
                prod_ref[tau * groups * OPS + piece, half] = got[
                    piece * rows : (piece + 1) * rows, half * count : (half + 1) * count
                ]
    prod_ref[taus * groups * OPS] = jnp.zeros((2, rows, count), BF16)
    table_copy.wait()
    copies = []
    for group in range(groups):
        for slot in range(slots):
            stage_ref[group, slot] = prod_ref[table_ref[0, group * slots + slot]]
        copies.append(pltpu.make_async_copy(stage_ref.at[group], out_hbm.at[group], sems.at[group]))
        copies[group].start()
    for copy in copies:
        copy.wait()


def dress(table, per, slabs, groups, slots, rows, count):
    taus = per.shape[0]
    shape = (groups, slots, 2, rows, count)
    return pl.pallas_call(
        partial(dress_kernel, groups, slots, taus, rows, count),
        in_specs=[pl.BlockSpec(memory_space=pl.ANY), vspec()] + [vspec()] * groups,
        out_specs=pl.BlockSpec(memory_space=pltpu.HBM),
        out_shape=jax.ShapeDtypeStruct(shape, BF16),
        scratch_shapes=[
            VMEM((groups * OPS * rows, 2 * count), BF16),
            VMEM((taus * groups * OPS + 1, 2, rows, count), BF16),
            VMEM(shape, BF16),
            SMEM(table.shape, jnp.int32),
            pltpu.SemaphoreType.DMA((groups + 1,)),
        ],
        compiler_params=limit(8),
        cost_estimate=cost(10**9, 2 * 10**6),
        name="dress",
    )(table, per, *slabs)


def fast_shards(eigvecs, gauge_links, perambulator, job_owner, job_elemental, job_source, job_spin):
    count = eigvecs.shape[1]
    planes, sites = eigvecs.shape[4], eigvecs.shape[5]
    tiles = sites // LANES
    space_size = lax.axis_size("space")
    groups = lax.axis_size("tm")
    lx = planes * space_size
    rows = count // space_size
    slots = 3 * ((JOB_DEV + groups - 1) // groups)
    cores = 2

    def tiled(field):
        head = field.shape[:-2]
        order = tuple(range(len(head))) + (len(head) + 1, len(head), len(head) + 2)
        split = field.reshape(head + (planes, tiles, LANES))
        return split.transpose(order).reshape(-1, LANES)

    x = tiled(eigvecs)
    u = tiled(gauge_links)
    angle = 2.0 * math.pi / lx * np.arange(lx)
    phases = jnp.asarray(np.concatenate([np.cos(angle), np.sin(angle)]).astype(np.float32)[None])

    per = perambulator.reshape(-1, 2, count, count)
    empty = per.shape[0] * groups * OPS
    x = pltpu.with_memory_space_constraint(x, pltpu.HBM)
    u = pltpu.with_memory_space_constraint(u, pltpu.HBM)
    up = [(i, (i + 1) % space_size) for i in range(space_size)]
    rim, low, links = rim_plane(x, u, None, count, tiles, planes)
    halos = [lax.ppermute(rim, "space", up)]
    rim, high, u = rim_plane(x, u, links, count, tiles, planes)
    halos.append(lax.ppermute(rim, "space", up))
    tables = [job.reshape(1, -1) for job in (job_owner, job_elemental, job_source, job_spin)]
    sums, rim_lhs, table = gram(
        low, high, u, phases, tables, count, tiles, planes, lx, groups, slots, empty
    )
    keep, send = edge(halos, rim_lhs, sums, count, rows, cores)
    got = lax.ppermute(send, "space", [(i, i ^ 1) for i in range(space_size)])
    parts = fold(keep, got, cores)
    summed = [parts[0]]
    chips = space_size // cores
    for step in range(1, chips):
        summed.append(
            lax.ppermute(parts[step], "space", [(i, i ^ (step * cores)) for i in range(space_size)])
        )
    own = total_rows(summed)
    slabs = [own]
    for step in range(1, groups):
        slabs.append(lax.ppermute(own, "tm", [(i, i ^ step) for i in range(groups)]))
    return dress(table, per, slabs, groups, slots, rows, count)[None]


def passed_along(shard, axis, by):
    count = lax.axis_size(axis)
    return lax.ppermute(shard, axis, [(i, (i + by) % count) for i in range(count)])


def shifted_sites(lattice_field, direction, offset):
    shaped = lattice_field.reshape(lattice_field.shape[:-1] + (LY, LZ))
    rolled = jnp.roll(shaped, -offset, axis=direction - 4)
    return rolled.reshape(lattice_field.shape)


def apply_link(link_field, vectors):
    total_re = None
    total_im = None
    for colour in range(3):
        link_re = link_field[0, :, colour][None]
        link_im = link_field[1, :, colour][None]
        vector_re = vectors[:, 0, colour][:, None]
        vector_im = vectors[:, 1, colour][:, None]
        part_re = link_re * vector_re - link_im * vector_im
        part_im = link_re * vector_im + link_im * vector_re
        if colour == 0:
            total_re, total_im = (part_re, part_im)
        else:
            total_re = total_re + part_re
            total_im = total_im + part_im
    return jnp.stack([total_re, total_im], axis=1)


def stacked_form(vectors):
    vector_count = vectors.shape[0]
    swapped = jnp.concatenate([-vectors[:, 1:2], vectors[:, 0:1]], axis=1)
    return jnp.concatenate(
        [vectors.reshape(vector_count, -1), swapped.reshape(vector_count, -1)], axis=0
    )


def paired_gram(stacked, lattice_field):
    vector_count = lattice_field.shape[0]
    flat_field = lattice_field.astype(jnp.bfloat16).reshape(vector_count, -1)
    product = lax.dot_general(
        stacked, flat_field, (((1,), (1,)), ((), ())), preferred_element_type=jnp.float32
    )
    return product.reshape(2, vector_count, vector_count)


def twisted_field(vectors, xcoord):
    phase_angle = 2.0 * math.pi / (vectors.shape[3] * lax.axis_size("space")) * xcoord
    cosine = jnp.cos(phase_angle)[:, None]
    sine_part = jnp.sin(phase_angle)[:, None]
    real_part = cosine * vectors[:, 0] + sine_part * vectors[:, 1]
    imag_part = cosine * vectors[:, 1] - sine_part * vectors[:, 0]
    return jnp.stack([real_part, imag_part], axis=1)


def antihermitian(paired):
    return 0.5 * jnp.stack([paired[0] - paired[0].T, paired[1] + paired[1].T], axis=0)


def plain_shards(eigvecs, gauge_links, perambulator, job_owner, job_elemental, job_source, job_spin):
    slice_count = eigvecs.shape[0]
    vector_count = eigvecs.shape[1]
    planes = eigvecs.shape[4]
    space_size = lax.axis_size("space")
    group_count = lax.axis_size("tm")
    row_count = vector_count // space_size
    capacity = 3 * ((JOB_DEV + group_count - 1) // group_count)
    xcoord = (lax.axis_index("space") * planes + jnp.arange(planes, dtype=jnp.int32)).astype(
        jnp.float32
    )
    upper_plane = passed_along(eigvecs[:, :, :, :, 0:1], "space", -1)
    low_vectors = eigvecs[0]
    vectors = low_vectors.astype(jnp.float32)
    stacked = stacked_form(low_vectors)
    results = [paired_gram(stacked, twisted_field(vectors, xcoord))]
    for direction in (1, 2, 3):
        link_field = gauge_links[0, direction - 1]
        if direction == 1:
            upper_rim = upper_plane[0].astype(jnp.float32)
            above_field = jnp.concatenate([vectors[:, :, :, 1:], upper_rim], axis=3)
        else:
            above_field = shifted_sites(vectors, direction, 1)
        forward = apply_link(link_field, above_field)
        results.append(antihermitian(paired_gram(stacked, forward)))
    partial_list = [jnp.stack(results, axis=0)]
    partial_value = jnp.stack(partial_list, axis=0)
    summed = lax.psum(partial_value, "space")
    own_rows = lax.dynamic_slice_in_dim(summed, lax.axis_index("space") * row_count, row_count, 3)
    slab_table = own_rows.astype(jnp.bfloat16).reshape(
        slice_count * OPS, 2 * row_count * vector_count
    )
    owners = job_owner[:, 0].reshape(group_count, -1)
    elements = job_elemental.reshape(group_count, -1)
    position = jnp.arange(owners.shape[1], dtype=jnp.int32)
    earlier = position[None, :] < position[:, None]
    same_owner = owners[:, :, None] == owners[:, None, :]
    slot_rank = jnp.sum(jnp.where(same_owner & earlier[None], 1, 0), axis=2).astype(jnp.int32)
    own_group = lax.axis_index("tm")
    slot_count = group_count * capacity
    live_jobs = owners == own_group
    slot_match = live_jobs[:, None, :] & (
        slot_rank[:, None, :] == jnp.arange(capacity, dtype=jnp.int32)[None, :, None]
    )
    sender_owners = lax.dynamic_index_in_dim(owners, own_group, 0, keepdims=False)
    sender_ranks = lax.dynamic_index_in_dim(slot_rank, own_group, 0, keepdims=False)
    sender_elements = lax.dynamic_index_in_dim(elements, own_group, 0, keepdims=False)
    slot_ids = sender_owners * capacity + sender_ranks
    slot_hot = (jnp.arange(slot_count, dtype=jnp.int32)[:, None] == slot_ids[None, :]).astype(
        jnp.float32
    )
    elem_hot = (
        sender_elements[:, None] == jnp.arange(slice_count * OPS, dtype=jnp.int32)[None, :]
    ).astype(jnp.float32)
    picker = jnp.dot(slot_hot, elem_hot, precision=lax.Precision.HIGHEST).astype(jnp.bfloat16)
    outgoing = jnp.dot(picker, slab_table, preferred_element_type=jnp.float32).astype(jnp.bfloat16)
    outgoing = outgoing.reshape(group_count, capacity, 2, row_count, vector_count)
    received = lax.all_to_all(outgoing, "tm", split_axis=0, concat_axis=0, tiled=True)
    block_index = job_source.reshape(group_count, -1) * SPIN + job_spin.reshape(group_count, -1)
    tau_index = jnp.sum(jnp.where(slot_match, block_index[:, None, :], 0), axis=2)
    blocks = perambulator.reshape(-1, 2 * vector_count, vector_count)
    chosen = jnp.take(blocks, tau_index.reshape(-1), axis=0)
    slab_rows = received.reshape(slot_count, 2, row_count, vector_count)
    real_rows = jnp.concatenate([slab_rows[:, 0], -slab_rows[:, 1]], axis=-1)
    imag_rows = jnp.concatenate([slab_rows[:, 1], slab_rows[:, 0]], axis=-1)
    left_side = jnp.stack([real_rows, imag_rows], axis=1).reshape(
        slot_count, 2 * row_count, 2 * vector_count
    )
    dressed = lax.dot_general(
        left_side, chosen, (((2,), (1,)), ((0,), (0,))), preferred_element_type=jnp.float32
    )
    return dressed.astype(jnp.bfloat16).reshape(
        1, group_count, capacity, 2, row_count, vector_count
    )


def shards(*args):
    eigvecs = args[0]
    count, planes, sites = eigvecs.shape[1], eigvecs.shape[4], eigvecs.shape[5]
    space_size, groups = lax.axis_size("space"), lax.axis_size("tm")
    whole_tiles = sites % (2 * LANES) == 0 and count == LANES and planes * (sites // LANES) == GROUP
    fits = groups * 3 * ((JOB_DEV + groups - 1) // groups) < LANES
    powers = space_size & (space_size - 1) == 0 and groups & (groups - 1) == 0
    small = space_size * GROUP == count and groups <= 8 and args[3].shape[0] <= LANES
    if whole_tiles and fits and powers and small and eigvecs.shape[0] == 1:
        return fast_shards(*args)
    return plain_shards(*args)


def solution(mesh):
    return jax.shard_map(
        shards,
        mesh=mesh,
        in_specs=(
            P("tm", None, None, None, "space", None),
            P("tm", None, None, None, None, "space", None),
            P("tm", None, None, None, None),
            P(),
            P(),
            P(),
            P(),
        ),
        out_specs=P("tm", None, None, None, "space", None),
        check_vma=False,
    )
```

```python
import math
from functools import partial

import numpy as np
import jax
import jax.numpy as jnp
from jax import lax
from jax.experimental import pallas as pl
from jax.experimental.pallas import tpu as pltpu
from jax.sharding import PartitionSpec as P

LY = 16
LZ = 32
OPS = 4
SPIN = 4
JOB_DEV = 24
LANES = 128
GROUP = 16
NARROW = (1, 2)
F32 = jnp.float32
BF16 = jnp.bfloat16
VMEM = pltpu.VMEM
SMEM = pltpu.SMEM


def vspec():
    return pl.BlockSpec(memory_space=VMEM)


def cost(flops, moved):
    return pl.CostEstimate(flops=flops, bytes_accessed=moved, transcendentals=0)


def limit(mebibytes):
    return pltpu.CompilerParams(vmem_limit_bytes=mebibytes * 2**20)


def pick_matrix(rows, cols, source_of):
    row = lax.broadcasted_iota(jnp.int32, (rows, cols), 0)
    col = lax.broadcasted_iota(jnp.int32, (rows, cols), 1)
    return jnp.where(col == source_of(row), 1.0, 0.0).astype(BF16)


def joined(pieces):
    return jnp.concatenate(pieces, axis=1)


def nt_dot(left, right):
    return lax.dot_general(left, right, (((1,), (1,)), ((), ())), preferred_element_type=F32)


def rim_kernel(tiles, planes, start, leads, x_hbm, u_hbm, *refs):
    if leads:
        out_ref, x_ref, link_ref, u_ref, pick_ref, sems = refs
    else:
        link_ref, out_ref, x_ref, u_ref, pick_ref, sems = refs
    spots = tiles * planes
    pair = 2
    part_count = out_ref.shape[2] // 2
    chunk = GROUP * 6 * spots
    chunks = part_count // GROUP
    rows_of = [pl.ds(g * chunk, chunk) for g in range(chunks)]
    copies = [
        pltpu.make_async_copy(x_hbm.at[pl.ds((start + g) * chunk, chunk)], x_ref.at[rows], sems.at[g])
        for g, rows in enumerate(rows_of)
    ]
    link_copy = pltpu.make_async_copy(u_hbm.at[pl.ds(0, u_ref.shape[0])], u_ref, sems.at[chunks])
    for copy in [link_copy] + copies if leads else copies + [link_copy]:
        copy.start()

    def source(row):
        return (row & (GROUP - 1)) * spots + (row // GROUP) * planes + planes - 1

    pick_ref[...] = pick_matrix(tiles * GROUP, GROUP * spots, source)
    if leads:
        link_copy.wait()
        for tile in range(tiles):
            flat = adjoint(load_rows(u_ref, 0, tile * planes + planes - 1, spots))
            for k, link in enumerate(flat):
                link_ref[tile, k] = link
    chosen = pick_ref[...]
    for g in range(chunks):
        copies[g].wait()
        block = x_ref[g * chunk : (g + 1) * chunk, :].reshape(GROUP, 6, spots, LANES)
        taken = []
        for part in range(0, 6, 2):
            rows = joined([block[:, part + k].reshape(GROUP * spots, LANES) for k in range(2)])
            got = jnp.dot(chosen, rows, preferred_element_type=F32)
            taken += [got[:, :LANES], got[:, LANES:]]
        for tile in range(tiles):
            links = [[[link_ref[tile, (p * 3 + r) * 3 + c] for c in range(3)] for r in range(3)] for p in range(3)]
            outs = []
            for eight in (0, 8):
                at = tile * GROUP + eight
                vec = [part[at : at + 8] for part in taken]
                outs.append(link_product(links, vec[:3], vec[3:]))
            for half in range(2):
                row = half * part_count + g * GROUP
                for colour in range(3):
                    both = jnp.concatenate([outs[0][half][colour], outs[1][half][colour]], axis=0)
                    out_ref[tile // pair, (tile % pair) * 3 + colour, row : row + GROUP] = both.astype(BF16)
    if not leads:
        link_copy.wait()


def lead_count(count):
    return count * 3 // (8 * GROUP) * GROUP


def rim_plane(x, u, links, count, tiles, planes):
    spots = tiles * planes
    pair = 2
    leads = links is None
    part_count = lead_count(count) if leads else count - lead_count(count)
    chunks = part_count // GROUP
    hbm = pl.BlockSpec(memory_space=pltpu.HBM)
    out_shape = [
        jax.ShapeDtypeStruct((tiles // pair, 3 * pair, 2 * part_count, LANES), BF16),
        jax.ShapeDtypeStruct((part_count * 6 * spots, LANES), BF16),
    ]
    scratch = [
        VMEM((tiles * GROUP, GROUP * spots), BF16),
        pltpu.SemaphoreType.DMA((chunks + 1,)),
    ]
    if leads:
        out_shape.append(jax.ShapeDtypeStruct((tiles, 27, 8, LANES), F32))
        scratch = [VMEM((18 * spots, LANES), F32)] + scratch
    else:
        out_shape.append(jax.ShapeDtypeStruct(u.shape, F32))
    return pl.pallas_call(
        partial(rim_kernel, tiles, planes, 0 if leads else lead_count(count) // GROUP, leads),
        in_specs=[hbm, hbm] + ([] if leads else [vspec()]),
        out_specs=[vspec()] * 3,
        out_shape=out_shape,
        scratch_shapes=scratch,
        compiler_params=limit(6),
        cost_estimate=cost(10**8, 2 * 10**6),
        name="rim" if leads else "rest",
    )(x, u, *([] if leads else [links]))


def link_product(links, vec_re, vec_im):
    plus = [vec_re[c] + vec_im[c] for c in range(3)]
    outs_re, outs_im = [], []
    for row in range(3):
        link_re, link_less, link_more = links[0][row], links[1][row], links[2][row]
        one = link_re[0] * plus[0] + link_re[1] * plus[1] + link_re[2] * plus[2]
        two = link_less[0] * vec_re[0] + link_less[1] * vec_re[1] + link_less[2] * vec_re[2]
        three = link_more[0] * vec_im[0] + link_more[1] * vec_im[1] + link_more[2] * vec_im[2]
        outs_re.append(one - three)
        outs_im.append(one + two)
    return outs_re, outs_im


def narrow_product(links, vec_re, vec_im):
    real, imag = links
    outs_re, outs_im = [], []
    for row in range(3):
        ones = [real[row][c] * vec_re[c] - imag[row][c] * vec_im[c] for c in range(3)]
        twos = [real[row][c] * vec_im[c] + imag[row][c] * vec_re[c] for c in range(3)]
        outs_re.append(ones[0] + ones[1] + ones[2])
        outs_im.append(twos[0] + twos[1] + twos[2])
    return outs_re, outs_im


def narrow_links(u_ref, direction, spot, spots):
    def one(part, row, col):
        at = (((direction * 2 + part) * 3 + row) * 3 + col) * spots + spot
        return jnp.broadcast_to(u_ref[pl.ds(at, 1), :], (GROUP, LANES)).astype(BF16)

    return [[[one(part, row, col) for col in range(3)] for row in range(3)] for part in range(2)]


def load_rows(u_ref, direction, spot, spots):
    def one(part, row, col):
        at = (((direction * 2 + part) * 3 + row) * 3 + col) * spots + spot
        return jnp.broadcast_to(u_ref[pl.ds(at, 1), :], (8, LANES))

    return [[[one(part, row, col) for col in range(3)] for row in range(3)] for part in range(2)]


def load_links(u_ref, direction, spot, spots):
    real, imag = load_rows(u_ref, direction, spot, spots)
    less = [[imag[row][col] - real[row][col] for col in range(3)] for row in range(3)]
    more = [[imag[row][col] + real[row][col] for col in range(3)] for row in range(3)]
    return real, less, more


def adjoint(grid):
    real, imag = grid
    order = [(row, col) for row in range(3) for col in range(3)]
    return (
        [real[col][row] for row, col in order]
        + [-imag[col][row] - real[col][row] for row, col in order]
        + [real[col][row] - imag[col][row] for row, col in order]
    )


def fill_table(groups, slots, empty, owner_ref, elem_ref, source_ref, spin_ref, table_ref):
    total = owner_ref.shape[1]
    jobs = total // groups
    row = lax.broadcasted_iota(jnp.int32, (total, total), 0)
    col = lax.broadcasted_iota(jnp.int32, (total, total), 1)

    def group_of(index):
        return sum((index >= group * jobs).astype(jnp.int32) for group in range(1, groups))

    live = jnp.where(owner_ref[...] == lax.axis_index("tm"), 1.0, 0.0)
    product = source_ref[...] * (SPIN * groups * OPS) + spin_ref[...] * (groups * OPS) + elem_ref[...]

    def column(mask, values):
        wide = jnp.broadcast_to(values.astype(F32), (total, total))
        return jnp.sum(jnp.where(mask, wide, 0.0), axis=1, keepdims=True)

    rank = column((col < row) & (group_of(col) == group_of(row)), live)
    alive = column(col == row, live)
    value = column(col == row, product)
    at_row = lax.broadcasted_iota(jnp.int32, (total, LANES), 0)
    at_col = lax.broadcasted_iota(jnp.int32, (total, LANES), 1)
    group = group_of(at_row).astype(F32)
    place = jnp.where(alive > 0.5, group * slots + rank, -1.0)
    found = at_col.astype(F32) == place
    picked = jnp.sum(jnp.where(found, value + group * OPS - empty, 0.0), axis=0, keepdims=True)
    table_ref[...] = (picked + empty).astype(jnp.int32)


def paired(grid, count):
    real = grid[:count, :count] + grid[count:, count:]
    imag = grid[count:, :count] - grid[:count, count:]
    return real, imag


def anti(real, imag):
    return 0.5 * (real.T - real), 0.5 * (imag.T + imag)


def gram_kernel(
    count, tiles, planes, lx, groups, slots, empty,
    low_ref, high_ref, u_ref, phase_ref, owner_ref, elem_ref, source_ref, spin_ref,
    sums_ref, rim_lhs_ref, table_ref,
    lhs_ref, op_ref, acc_ref, g_ref, pick_ref,
):
    spots = tiles * planes
    pair = 2
    halves = tiles // pair
    steps = planes * halves

    def source(row):
        spot = row // GROUP
        return (row & (GROUP - 1)) * spots + (spot % tiles) * planes + spot // tiles

    pick_ref[...] = pick_matrix(GROUP * spots, GROUP * spots, source)
    acc_ref[...] = jnp.zeros_like(acc_ref)
    g_ref[...] = jnp.zeros_like(g_ref)

    chosen = pick_ref[...]
    for at in range(0, count, GROUP):
        lead = lead_count(count)
        x_ref, near = (low_ref, at) if at < lead else (high_ref, at - lead)
        block = x_ref[near * 6 * spots : (near + GROUP) * 6 * spots, :].reshape(GROUP, 6, spots, LANES)
        for first in range(0, 6, 2):
            rows = jnp.concatenate(
                [block[:, first + k].reshape(GROUP * spots, LANES) for k in range(2)], axis=1
            )
            taken = jnp.dot(chosen, rows, preferred_element_type=F32)
            for k in range(2):
                part = first + k
                half, colour = part // 3, part % 3
                for spot in range(spots):
                    piece = taken[spot * GROUP : (spot + 1) * GROUP, k * LANES : (k + 1) * LANES]
                    plane, tile = spot // tiles, spot % tiles
                    lhs_ref[
                        plane * halves + tile // pair,
                        (tile % pair) * 3 + colour,
                        half * count + at : half * count + at + GROUP,
                    ] = piece.astype(BF16)

    lane = lax.broadcasted_iota(jnp.int32, (GROUP, LANES), 1)
    wraps = (lane & (LZ - 1)) == LZ - 1
    spills = lane < LZ

    def elementwise(step, slot, directions):
        plane = step // halves
        half_tile = step % halves
        for sub in range(pair):
            tile = half_tile * pair + sub
            ahead = step if sub + 1 < pair else plane * halves + (half_tile + 1) % halves
            for direction in directions:
                narrow = direction in NARROW
                links = (narrow_links if narrow else load_links)(
                    u_ref, direction, tile * planes + plane, spots
                )
                for at in range(0, count, GROUP):

                    def part(where, turn, k):
                        row = k // 3 * count + at
                        return lhs_ref[where, turn * 3 + k % 3, row : row + GROUP]

                    if direction == 0:
                        vec = [part(step + halves, sub, k) for k in range(6)]
                    elif direction == 1:
                        vec = [
                            pltpu.roll(
                                jnp.where(spills, part(ahead, (sub + 1) % pair, k), part(step, sub, k)), LANES - LZ, 1
                            )
                            for k in range(6)
                        ]
                    else:
                        vec = [
                            jnp.where(
                                wraps,
                                pltpu.roll(part(step, sub, k), LZ - 1, 1),
                                pltpu.roll(part(step, sub, k), LANES - 1, 1),
                            )
                            for k in range(6)
                        ]
                    if narrow:
                        outs = narrow_product(links, vec[:3], vec[3:])
                    else:
                        wide = [piece.astype(F32) for piece in vec]
                        pieces = [[piece[eight : eight + 8] for piece in wide] for eight in (0, 8)]
                        low, high = [link_product(links, piece[:3], piece[3:]) for piece in pieces]
                        outs = [
                            [
                                jnp.concatenate([low[half][colour], high[half][colour]], axis=0).astype(BF16)
                                for colour in range(3)
                            ]
                            for half in range(2)
                        ]
                    for half in range(2):
                        row = (direction * 2 + half) * count + at
                        for colour in range(3):
                            op_ref[slot, sub * 3 + colour, row : row + GROUP] = outs[half][colour]

    def multiply(step, slot, directions):
        fixed = joined([lhs_ref[step, k] for k in range(3 * pair)])
        low = min(directions) * 2 * count
        high = (max(directions) + 1) * 2 * count
        moving = joined([op_ref[slot, k, low:high] for k in range(3 * pair)])
        got = nt_dot(jnp.concatenate([fixed, moving], axis=0), fixed)
        g_ref[step // halves] += got[: 2 * count]
        acc_ref[low:high, :] += got[2 * count :]

    every, side = (0, 1, 2), (1, 2)
    inner = steps - halves
    elementwise(inner, 0, side)
    for step in range(inner + 1, steps):
        multiply(step - 1, (step - 1) & 1, side)
        elementwise(step, step & 1, side)
    multiply(steps - 1, (steps - 1) & 1, side)
    elementwise(0, 0, every)

    for step in range(1, inner):
        multiply(step - 1, (step - 1) & 1, every)
        elementwise(step, step & 1, every)
    multiply(inner - 1, (inner - 1) & 1, every)
    fill_table(groups, slots, empty, owner_ref, elem_ref, source_ref, spin_ref, table_ref)

    first = lax.axis_index("space") * planes
    place = lax.broadcasted_iota(jnp.int32, phase_ref.shape, 1)
    total_re = jnp.zeros((count, count), F32)
    total_im = jnp.zeros((count, count), F32)
    for plane in range(planes):
        real, imag = paired(g_ref[plane], count)
        cosine = jnp.sum(jnp.where(place == first + plane, phase_ref[...], 0.0), axis=1, keepdims=True)
        sine = jnp.sum(jnp.where(place == lx + first + plane, phase_ref[...], 0.0), axis=1, keepdims=True)
        total_re += cosine * real - sine * imag
        total_im += cosine * imag + sine * real
    sums_ref[0, 0] = total_re
    sums_ref[0, 1] = -total_im
    for direction in range(3):
        grid = acc_ref[direction * 2 * count : (direction + 1) * 2 * count, :]
        real, imag = anti(*paired(grid, count))
        sums_ref[direction + 1, 0] = real
        sums_ref[direction + 1, 1] = imag
    for half in range(halves):
        rim_lhs_ref[half] = lhs_ref[half]


def gram(low, high, u, phases, tables, count, tiles, planes, lx, groups, slots, empty):
    spots = tiles * planes
    pair = 2
    steps = planes * (tiles // pair)
    return pl.pallas_call(
        partial(gram_kernel, count, tiles, planes, lx, groups, slots, empty),
        in_specs=[vspec()] * 8,
        out_specs=[vspec()] * 3,
        out_shape=[
            jax.ShapeDtypeStruct((OPS, 2, count, count), F32),
            jax.ShapeDtypeStruct((tiles // pair, 3 * pair, 2 * count, LANES), BF16),
            jax.ShapeDtypeStruct((1, LANES), jnp.int32),
        ],
        scratch_shapes=[
            VMEM((steps, 3 * pair, 2 * count, LANES), BF16),
            VMEM((2, 3 * pair, 6 * count, LANES), BF16),
            VMEM((6 * count, 2 * count), F32),
            VMEM((planes, 2 * count, 2 * count), F32),
            VMEM((GROUP * spots, GROUP * spots), BF16),
        ],
        compiler_params=limit(26),
        cost_estimate=cost(8 * 10**9, 5 * 10**6),
        name="gram",
    )(low, high, u, phases, *tables)


def edge_kernel(count, rows, cores, low_ref, high_ref, lhs_ref, sums_ref, keep_ref, send_ref, tot_ref):
    total = None
    for half in range(low_ref.shape[0]):
        sides = [joined([ref[half, k] for k in range(ref.shape[1])]) for ref in (low_ref, high_ref, lhs_ref)]
        got = nt_dot(jnp.concatenate(sides[:2], axis=0), sides[2])
        total = got if total is None else total + got
    reals, imags = [], []
    at = 0
    for size in (lead_count(count), count - lead_count(count)):
        mid, end = at + size, at + 2 * size
        reals.append(total[at:mid, :count] + total[mid:end, count:])
        imags.append(total[at:mid, count:] - total[mid:end, :count])
        at = end
    real, imag = jnp.concatenate(reals, axis=0), jnp.concatenate(imags, axis=0)
    tot_ref[0] = 0.5 * (real - real.T)
    tot_ref[1] = 0.5 * (imag + imag.T)
    mine = lax.axis_index("space") & (cores - 1)
    for chip in range(count // (rows * cores)):
        for which, ref in ((mine, keep_ref), (1 - mine, send_ref)):
            at = pl.multiple_of((chip * cores + which) * rows, rows)
            for op in range(OPS):
                for half in range(2):
                    piece = sums_ref[op, half, pl.ds(at, rows), :]
                    if op == 1:
                        piece = piece + tot_ref[half, pl.ds(at, rows), :]
                    ref[chip, op, half] = piece


def edge(halos, rim_lhs, sums, count, rows, cores):
    shape = jax.ShapeDtypeStruct((count // (rows * cores), OPS, 2, rows, count), F32)
    return pl.pallas_call(
        partial(edge_kernel, count, rows, cores),
        in_specs=[vspec()] * 4,
        out_specs=[vspec(), vspec()],
        out_shape=[shape, shape],
        scratch_shapes=[VMEM((2, count, count), F32)],
        compiler_params=limit(8),
        cost_estimate=cost(10**9, 3 * 10**6),
        name="edge",
    )(*halos, rim_lhs, sums)


def split_sum(block):
    high = block[0:1].astype(BF16)
    low = (block[0:1] - high.astype(F32)).astype(BF16)
    return jnp.concatenate([high, low, block[1:].astype(BF16)], axis=0)


def fold_kernel(chips, cores, keep_ref, got_ref, own_ref, *out_refs):
    me = lax.axis_index("space") // cores
    own_ref[...] = keep_ref[me] + got_ref[me]
    for step in range(1, chips):
        to = me ^ step
        out_refs[step - 1][...] = split_sum(keep_ref[to] + got_ref[to])


def fold(keep, got, cores):
    chips = keep.shape[0]
    shape = keep.shape[1:]
    sent = jax.ShapeDtypeStruct((shape[0] + 1,) + shape[1:], BF16)
    return pl.pallas_call(
        partial(fold_kernel, chips, cores),
        in_specs=[vspec()] * 2,
        out_specs=[vspec()] * chips,
        out_shape=[jax.ShapeDtypeStruct(shape, F32)] + [sent] * (chips - 1),
        compiler_params=limit(4),
        cost_estimate=cost(10**6, 10**6),
        name="fold",
    )(keep, got)


def total_kernel(own_ref, *refs):
    total_ref = refs[-1]
    first = own_ref[0:1]
    rest = own_ref[1:]
    for ref in refs[:-1]:
        first = first + (ref[0:1].astype(F32) + ref[1:2].astype(F32))
        rest = rest + ref[2:].astype(F32)
    total_ref[0:1] = first.astype(BF16)
    total_ref[1:] = rest.astype(BF16)


def total_rows(parts):
    return pl.pallas_call(
        total_kernel,
        in_specs=[vspec()] * len(parts),
        out_specs=vspec(),
        out_shape=jax.ShapeDtypeStruct(parts[0].shape, BF16),
        compiler_params=limit(4),
        cost_estimate=cost(10**6, 10**6),
        name="total",
    )(*parts)


def dress_kernel(groups, slots, taus, rows, count, table_any, per_ref, *refs):
    slab_refs = refs[:groups]
    out_hbm, lhs_ref, prod_ref, stage_ref, table_ref, sems = refs[groups:]
    table_copy = pltpu.make_async_copy(table_any, table_ref, sems.at[groups])
    table_copy.start()
    me = lax.axis_index("tm")
    for step in range(groups):
        group = me ^ step
        for op in range(OPS):
            at = pl.multiple_of((group * OPS + op) * rows, rows)
            lhs_ref[pl.ds(at, rows), 0:count] = slab_refs[step][op, 0]
            lhs_ref[pl.ds(at, rows), count : 2 * count] = slab_refs[step][op, 1]
    left = lhs_ref[...]
    for tau in range(taus):
        real, imag = per_ref[tau, 0], per_ref[tau, 1]
        right = jnp.concatenate([joined([real, imag]), joined([-imag, real])], axis=0)
        got = jnp.dot(left, right, preferred_element_type=F32).astype(BF16)
        for piece in range(groups * OPS):
            for half in range(2):
                prod_ref[tau * groups * OPS + piece, half] = got[
                    piece * rows : (piece + 1) * rows, half * count : (half + 1) * count
                ]
    prod_ref[taus * groups * OPS] = jnp.zeros((2, rows, count), BF16)
    table_copy.wait()
    copies = []
    for group in range(groups):
        for slot in range(slots):
            stage_ref[group, slot] = prod_ref[table_ref[0, group * slots + slot]]
        copies.append(pltpu.make_async_copy(stage_ref.at[group], out_hbm.at[group], sems.at[group]))
        copies[group].start()
    for copy in copies:
        copy.wait()


def dress(table, per, slabs, groups, slots, rows, count):
    taus = per.shape[0]
    shape = (groups, slots, 2, rows, count)
    return pl.pallas_call(
        partial(dress_kernel, groups, slots, taus, rows, count),
        in_specs=[pl.BlockSpec(memory_space=pl.ANY), vspec()] + [vspec()] * groups,
        out_specs=pl.BlockSpec(memory_space=pltpu.HBM),
        out_shape=jax.ShapeDtypeStruct(shape, BF16),
        scratch_shapes=[
            VMEM((groups * OPS * rows, 2 * count), BF16),
            VMEM((taus * groups * OPS + 1, 2, rows, count), BF16),
            VMEM(shape, BF16),
            SMEM(table.shape, jnp.int32),
            pltpu.SemaphoreType.DMA((groups + 1,)),
        ],
        compiler_params=limit(8),
        cost_estimate=cost(10**9, 2 * 10**6),
        name="dress",
    )(table, per, *slabs)


def fast_shards(eigvecs, gauge_links, perambulator, job_owner, job_elemental, job_source, job_spin):
    count = eigvecs.shape[1]
    planes, sites = eigvecs.shape[4], eigvecs.shape[5]
    tiles = sites // LANES
    space_size = lax.axis_size("space")
    groups = lax.axis_size("tm")
    lx = planes * space_size
    rows = count // space_size
    slots = 3 * ((JOB_DEV + groups - 1) // groups)
    cores = 2

    def tiled(field):
        head = field.shape[:-2]
        order = tuple(range(len(head))) + (len(head) + 1, len(head), len(head) + 2)
        split = field.reshape(head + (planes, tiles, LANES))
        return split.transpose(order).reshape(-1, LANES)

    x = tiled(eigvecs)
    u = tiled(gauge_links)
    angle = 2.0 * math.pi / lx * np.arange(lx)
    phases = jnp.asarray(np.concatenate([np.cos(angle), np.sin(angle)]).astype(np.float32)[None])

    per = perambulator.reshape(-1, 2, count, count)
    empty = per.shape[0] * groups * OPS
    x = pltpu.with_memory_space_constraint(x, pltpu.HBM)
    u = pltpu.with_memory_space_constraint(u, pltpu.HBM)
    up = [(i, (i + 1) % space_size) for i in range(space_size)]
    rim, low, links = rim_plane(x, u, None, count, tiles, planes)
    halos = [lax.ppermute(rim, "space", up)]
    rim, high, u = rim_plane(x, u, links, count, tiles, planes)
    halos.append(lax.ppermute(rim, "space", up))
    tables = [job.reshape(1, -1) for job in (job_owner, job_elemental, job_source, job_spin)]
    sums, rim_lhs, table = gram(
        low, high, u, phases, tables, count, tiles, planes, lx, groups, slots, empty
    )
    keep, send = edge(halos, rim_lhs, sums, count, rows, cores)
    got = lax.ppermute(send, "space", [(i, i ^ 1) for i in range(space_size)])
    parts = fold(keep, got, cores)
    summed = [parts[0]]
    chips = space_size // cores
    for step in range(1, chips):
        summed.append(
            lax.ppermute(parts[step], "space", [(i, i ^ (step * cores)) for i in range(space_size)])
        )
    own = total_rows(summed)
    moved = {0: own}
    for step in sorted(range(1, groups), key=lambda step: (step & 1 == 0, step)):
        moved[step] = lax.ppermute(own, "tm", [(i, i ^ step) for i in range(groups)])
    slabs = [moved[step] for step in range(groups)]
    return dress(table, per, slabs, groups, slots, rows, count)[None]


def passed_along(shard, axis, by):
    count = lax.axis_size(axis)
    return lax.ppermute(shard, axis, [(i, (i + by) % count) for i in range(count)])


def shifted_sites(lattice_field, direction, offset):
    shaped = lattice_field.reshape(lattice_field.shape[:-1] + (LY, LZ))
    rolled = jnp.roll(shaped, -offset, axis=direction - 4)
    return rolled.reshape(lattice_field.shape)


def apply_link(link_field, vectors):
    total_re = None
    total_im = None
    for colour in range(3):
        link_re = link_field[0, :, colour][None]
        link_im = link_field[1, :, colour][None]
        vector_re = vectors[:, 0, colour][:, None]
        vector_im = vectors[:, 1, colour][:, None]
        part_re = link_re * vector_re - link_im * vector_im
        part_im = link_re * vector_im + link_im * vector_re
        if colour == 0:
            total_re, total_im = (part_re, part_im)
        else:
            total_re = total_re + part_re
            total_im = total_im + part_im
    return jnp.stack([total_re, total_im], axis=1)


def stacked_form(vectors):
    vector_count = vectors.shape[0]
    swapped = jnp.concatenate([-vectors[:, 1:2], vectors[:, 0:1]], axis=1)
    return jnp.concatenate(
        [vectors.reshape(vector_count, -1), swapped.reshape(vector_count, -1)], axis=0
    )


def paired_gram(stacked, lattice_field):
    vector_count = lattice_field.shape[0]
    flat_field = lattice_field.astype(jnp.bfloat16).reshape(vector_count, -1)
    product = lax.dot_general(
        stacked, flat_field, (((1,), (1,)), ((), ())), preferred_element_type=jnp.float32
    )
    return product.reshape(2, vector_count, vector_count)


def twisted_field(vectors, xcoord):
    phase_angle = 2.0 * math.pi / (vectors.shape[3] * lax.axis_size("space")) * xcoord
    cosine = jnp.cos(phase_angle)[:, None]
    sine_part = jnp.sin(phase_angle)[:, None]
    real_part = cosine * vectors[:, 0] + sine_part * vectors[:, 1]
    imag_part = cosine * vectors[:, 1] - sine_part * vectors[:, 0]
    return jnp.stack([real_part, imag_part], axis=1)


def antihermitian(paired):
    return 0.5 * jnp.stack([paired[0] - paired[0].T, paired[1] + paired[1].T], axis=0)


def plain_shards(eigvecs, gauge_links, perambulator, job_owner, job_elemental, job_source, job_spin):
    slice_count = eigvecs.shape[0]
    vector_count = eigvecs.shape[1]
    planes = eigvecs.shape[4]
    space_size = lax.axis_size("space")
    group_count = lax.axis_size("tm")
    row_count = vector_count // space_size
    capacity = 3 * ((JOB_DEV + group_count - 1) // group_count)
    xcoord = (lax.axis_index("space") * planes + jnp.arange(planes, dtype=jnp.int32)).astype(
        jnp.float32
    )
    upper_plane = passed_along(eigvecs[:, :, :, :, 0:1], "space", -1)
    low_vectors = eigvecs[0]
    vectors = low_vectors.astype(jnp.float32)
    stacked = stacked_form(low_vectors)
    results = [paired_gram(stacked, twisted_field(vectors, xcoord))]
    for direction in (1, 2, 3):
        link_field = gauge_links[0, direction - 1]
        if direction == 1:
            upper_rim = upper_plane[0].astype(jnp.float32)
            above_field = jnp.concatenate([vectors[:, :, :, 1:], upper_rim], axis=3)
        else:
            above_field = shifted_sites(vectors, direction, 1)
        forward = apply_link(link_field, above_field)
        results.append(antihermitian(paired_gram(stacked, forward)))
    partial_list = [jnp.stack(results, axis=0)]
    partial_value = jnp.stack(partial_list, axis=0)
    summed = lax.psum(partial_value, "space")
    own_rows = lax.dynamic_slice_in_dim(summed, lax.axis_index("space") * row_count, row_count, 3)
    slab_table = own_rows.astype(jnp.bfloat16).reshape(
        slice_count * OPS, 2 * row_count * vector_count
    )
    owners = job_owner[:, 0].reshape(group_count, -1)
    elements = job_elemental.reshape(group_count, -1)
    position = jnp.arange(owners.shape[1], dtype=jnp.int32)
    earlier = position[None, :] < position[:, None]
    same_owner = owners[:, :, None] == owners[:, None, :]
    slot_rank = jnp.sum(jnp.where(same_owner & earlier[None], 1, 0), axis=2).astype(jnp.int32)
    own_group = lax.axis_index("tm")
    slot_count = group_count * capacity
    live_jobs = owners == own_group
    slot_match = live_jobs[:, None, :] & (
        slot_rank[:, None, :] == jnp.arange(capacity, dtype=jnp.int32)[None, :, None]
    )
    sender_owners = lax.dynamic_index_in_dim(owners, own_group, 0, keepdims=False)
    sender_ranks = lax.dynamic_index_in_dim(slot_rank, own_group, 0, keepdims=False)
    sender_elements = lax.dynamic_index_in_dim(elements, own_group, 0, keepdims=False)
    slot_ids = sender_owners * capacity + sender_ranks
    slot_hot = (jnp.arange(slot_count, dtype=jnp.int32)[:, None] == slot_ids[None, :]).astype(
        jnp.float32
    )
    elem_hot = (
        sender_elements[:, None] == jnp.arange(slice_count * OPS, dtype=jnp.int32)[None, :]
    ).astype(jnp.float32)
    picker = jnp.dot(slot_hot, elem_hot, precision=lax.Precision.HIGHEST).astype(jnp.bfloat16)
    outgoing = jnp.dot(picker, slab_table, preferred_element_type=jnp.float32).astype(jnp.bfloat16)
    outgoing = outgoing.reshape(group_count, capacity, 2, row_count, vector_count)
    received = lax.all_to_all(outgoing, "tm", split_axis=0, concat_axis=0, tiled=True)
    block_index = job_source.reshape(group_count, -1) * SPIN + job_spin.reshape(group_count, -1)
    tau_index = jnp.sum(jnp.where(slot_match, block_index[:, None, :], 0), axis=2)
    blocks = perambulator.reshape(-1, 2 * vector_count, vector_count)
    chosen = jnp.take(blocks, tau_index.reshape(-1), axis=0)
    slab_rows = received.reshape(slot_count, 2, row_count, vector_count)
    real_rows = jnp.concatenate([slab_rows[:, 0], -slab_rows[:, 1]], axis=-1)
    imag_rows = jnp.concatenate([slab_rows[:, 1], slab_rows[:, 0]], axis=-1)
    left_side = jnp.stack([real_rows, imag_rows], axis=1).reshape(
        slot_count, 2 * row_count, 2 * vector_count
    )
    dressed = lax.dot_general(
        left_side, chosen, (((2,), (1,)), ((0,), (0,))), preferred_element_type=jnp.float32
    )
    return dressed.astype(jnp.bfloat16).reshape(
        1, group_count, capacity, 2, row_count, vector_count
    )


def shards(*args):
    eigvecs = args[0]
    count, planes, sites = eigvecs.shape[1], eigvecs.shape[4], eigvecs.shape[5]
    space_size, groups = lax.axis_size("space"), lax.axis_size("tm")
    whole_tiles = sites % (2 * LANES) == 0 and count == LANES and planes * (sites // LANES) == GROUP
    fits = groups * 3 * ((JOB_DEV + groups - 1) // groups) < LANES
    powers = space_size & (space_size - 1) == 0 and groups & (groups - 1) == 0
    small = space_size * GROUP == count and groups <= 8 and args[3].shape[0] <= LANES
    if whole_tiles and fits and powers and small and eigvecs.shape[0] == 1:
        return fast_shards(*args)
    return plain_shards(*args)


def solution(mesh):
    return jax.shard_map(
        shards,
        mesh=mesh,
        in_specs=(
            P("tm", None, None, None, "space", None),
            P("tm", None, None, None, None, "space", None),
            P("tm", None, None, None, None),
            P(),
            P(),
            P(),
            P(),
        ),
        out_specs=P("tm", None, None, None, "space", None),
        check_vma=False,
    )
```
